32 devices in a mesh: ctx: 16 (over z, x, core), wa: 2 (over y).
Axes of the slice: x: 2, y: 2, z: 4, core: 2. Of those that a mesh axis runs over, the one named last changes fastest.
Arguments:
- tokens: bfloat16 [2, 6144, 768], P('wa', 'ctx'), may hold values from -6 to 6
- cotangent: bfloat16 [2, 6144, 768], P('wa', 'ctx'), may hold values from -6 to 6
- lengths: int32 [2, 3], P('wa'), may hold values from 1024 to 3072, as said below
- block_order: int32 [32], replicated, may hold values from 0 to 31, each once
- w_query: float32 [768, 768], P('wa'), may hold values from -0.21875 to 0.21875
- b_query: float32 [768], P('wa'), may hold values from -4 to 4
- w_key: float32 [768, 768], P('wa'), may hold values from -0.21875 to 0.21875
- w_value: float32 [768, 768], P('wa'), may hold values from -0.21875 to 0.21875
- b_value: float32 [768], P('wa'), may hold values from -4 to 4
- w_out: float32 [768, 768], P('wa'), may hold values from -6 to 6
- b_out: float32 [768], P('wa'), may hold values from -4 to 4
- gain_one: float32 [768], P('wa'), may hold values from 0.5 to 1.5
- shift_one: float32 [768], P('wa'), may hold values from -4 to 4
- w_up: float32 [768, 3072], P('wa'), may hold values from -0.21875 to 0.21875
- b_up: float32 [3072], P('wa'), may hold values from -4 to 4
- w_down: float32 [3072, 768], P('wa'), may hold values from -0.109375 to 0.109375
- b_down: float32 [768], P('wa'), may hold values from -4 to 4
- gain_two: float32 [768], P('wa'), may hold values from 0.5 to 1.5
- shift_two: float32 [768], P('wa'), may hold values from -4 to 4
Outputs:
- activations: bfloat16 [2, 6144, 768], P('wa', 'ctx')
- input_grad: bfloat16 [2, 6144, 768], P('wa', 'ctx')
- grad_w_query: float32 [768, 768], P('wa')
- grad_b_query: float32 [768], P('wa')
- grad_w_key: float32 [768, 768], P('wa')
- grad_w_value: float32 [768, 768], P('wa')
- grad_b_value: float32 [768], P('wa')
- grad_w_out: float32 [768, 768], P('wa')
- grad_b_out: float32 [768], P('wa')
- grad_gain_one: float32 [768], P('wa')
- grad_shift_one: float32 [768], P('wa')
- grad_w_up: float32 [768, 3072], P('wa')
- grad_b_up: float32 [3072], P('wa')
- grad_w_down: float32 [3072, 768], P('wa')
- grad_b_down: float32 [768], P('wa')
- grad_gain_two: float32 [768], P('wa')
- grad_shift_two: float32 [768], P('wa')
The draws below stay inside these ranges and needn't reach their ends.
Inputs may be any that keep to these rules, and one draw needn't show every extreme that they name: `lengths`: each slot holds three sequences, each of 1024 tokens or more, one of them exactly 3072; the rest of the slot, 2 tokens or more, is padding. `block_order`: each block number appears once.
All inputs are finite; a program needn't handle non-finite values.
Results may differ from the reference program's by a relative error of at most 0.023.
Values may be sent and summed in bfloat16 or wider, within the bound.
A program may use at most 256 MiB of HBM per device.

```python
import jax
import jax.numpy as jnp
from jax import lax

D = 768
HEADS = 12
HEAD_DIM = 64
FF = 3072
MIN_LEN = 1024
SLOTS = 2
SLOT_LEN = 6144
HALF = 192
N_CTX = 16


def draw_lengths(key, part):
    first_key, second_key = jax.random.split(jax.random.fold_in(key, 7))
    quarter = SLOT_LEN // 4
    others = jax.random.randint(first_key, (SLOTS, 2), MIN_LEN, quarter, dtype=jnp.int32)
    longest = jax.random.randint(second_key, (SLOTS, 1), 0, 3, dtype=jnp.int32)
    places = jnp.arange(3, dtype=jnp.int32)[None, :]
    rank_of = jnp.clip(places - (places > longest).astype(jnp.int32), 0, 1)
    picked = jnp.where(rank_of == 0, others[:, :1], others[:, 1:])
    return jnp.where(places == longest, SLOT_LEN // 2, picked).astype(jnp.int32)


def steps_of(key, extent, pieces, least, largest):
    gain = 1.0
    for axis_at, blocks in pieces:
        heights = jax.random.uniform(jax.random.fold_in(jax.random.fold_in(key, 6), axis_at), (blocks,), jnp.float32, least / len(pieces), largest / len(pieces))
        gain = gain * jnp.repeat(jnp.exp(heights), extent[axis_at] // blocks).reshape((-1,) + (1,) * (len(extent) - 1 - axis_at))
    return gain


def bell_draw(rng, dims, deviation, reach, cuts=(), kind=jnp.bfloat16):
    values = jax.random.normal(rng, dims, jnp.float32) * deviation
    if len(cuts) > 0:
        values = steps_of(rng, dims, cuts, -0.22, 0.18) * values
    return jnp.clip(values, min=-reach, max=reach).astype(kind)


def setup_inputs(seed: int = 0) -> dict:
    splits = jax.random.split(jax.random.key(seed), 20)
    return {
        "tokens": bell_draw(splits[0], (SLOTS, SLOT_LEN, D), 1.0, 6.0, ((0, 2), (1, 16))),
        "cotangent": bell_draw(splits[1], (SLOTS, SLOT_LEN, D), 1.0, 6.0, ((0, 2), (1, 16))),
        "lengths": draw_lengths(jax.random.fold_in(splits[19], 71), 0),
        "block_order": jax.random.permutation(splits[3], 2 * N_CTX).astype(jnp.int32),
        "w_query": bell_draw(splits[4], (D, D), D ** -0.5, 0.21875, ((0, 2),), jnp.float32),
        "b_query": bell_draw(splits[5], (D,), 1.0, 4.0, ((0, 2),), jnp.float32),
        "w_key": bell_draw(splits[6], (D, D), D ** -0.5, 0.21875, ((0, 2),), jnp.float32),
        "w_value": bell_draw(splits[7], (D, D), D ** -0.5, 0.21875, ((0, 2),), jnp.float32),
        "b_value": bell_draw(splits[8], (D,), 0.3, 4.0, ((0, 2),), jnp.float32),
        "w_out": bell_draw(splits[9], (D, D), (max(1, 4 * D // SLOT_LEN)) ** -0.5, 6.0, ((0, 2),), jnp.float32),
        "b_out": bell_draw(splits[10], (D,), 0.3, 4.0, ((0, 2),), jnp.float32),
        "gain_one": jnp.clip(1.0 + 0.1 * jax.random.normal(splits[11], (D,), jnp.float32), 0.5, 1.5),
        "shift_one": bell_draw(splits[12], (D,), 0.3, 4.0, ((0, 2),), jnp.float32),
        "w_up": bell_draw(splits[13], (D, FF), D ** -0.5, 0.21875, ((0, 2),), jnp.float32),
        "b_up": bell_draw(splits[14], (FF,), 0.3, 4.0, ((0, 2),), jnp.float32),
        "w_down": bell_draw(splits[15], (FF, D), FF ** -0.5, 0.109375, ((0, 2),), jnp.float32),
        "b_down": bell_draw(splits[16], (D,), 0.3, 4.0, ((0, 2),), jnp.float32),
        "gain_two": jnp.clip(1.0 + 0.1 * jax.random.normal(splits[17], (D,), jnp.float32), 0.5, 1.5),
        "shift_two": bell_draw(splits[18], (D,), 0.3, 4.0, ((0, 2),), jnp.float32),
    }


@jax.custom_vjp
def low(v):
    return lax.optimization_barrier(v.astype(jnp.bfloat16)).astype(jnp.float32)

@jax.custom_vjp
def low_back(v):
    return v

def low_keep(v):
    return (low(v), None)

def low_pass(kept, grad):
    return (grad,)

def back_keep(v):
    return (v, None)

def back_low(kept, grad):
    return (low(grad),)
low.defvjp(low_keep, low_pass)
low_back.defvjp(back_keep, back_low)
epsilon = 1e-05

def matmul(left, right):
    return jnp.dot(left, right, precision=lax.Precision.HIGHEST, preferred_element_type=jnp.float32)

def layer_norm(hidden, gain_vec, shift_vec):
    centre = hidden - lax.optimization_barrier(jnp.mean(hidden, axis=-1, keepdims=True))
    spread = lax.optimization_barrier(jnp.mean(centre * centre, axis=-1, keepdims=True))
    return centre * lax.rsqrt(spread + epsilon) * gain_vec + shift_vec

def segment_ids(row_ids, block_order, seq_ends, half_len):
    dealt_slot = row_ids // (2 * half_len) * 2 + row_ids // half_len % 2
    table_ids = jnp.arange(block_order.shape[0], dtype=jnp.int32)
    block_ids = lax.optimization_barrier(jnp.sum(jnp.where(dealt_slot[:, None] == table_ids[None, :], block_order[None, :], 0), axis=1)).astype(jnp.int32)
    position = block_ids * half_len + row_ids % half_len
    return lax.optimization_barrier(jnp.sum((position[:, None] >= seq_ends[None, :]).astype(jnp.int32), axis=1)).astype(jnp.int32)

def attend(query_blk, key_proj, value_proj, query_seg, key_seg):
    scores = low_back(jnp.einsum('qhd,khd->hqk', query_blk, key_proj, precision=lax.Precision.HIGHEST))
    mask = query_seg[:, None] == key_seg[None, :]
    expo = jnp.where(mask[None], jnp.exp(scores), 0.0)
    totals = lax.optimization_barrier(jnp.sum(expo, axis=-1))
    summed = low_back(jnp.einsum('hqk,khd->qhd', low(expo), value_proj, precision=lax.Precision.HIGHEST))
    return summed / totals.T[:, :, None]

def layer_forward(x_all, params, segs):
    query_weight, query_bias, key_weight, value_weight, value_bias, out_weight, out_bias, gain_first, shift_first, up_weight, up_bias, down_weight, down_bias, gain_second, shift_second = tuple((low(entry) for entry in params))
    row_block = min(512, SLOT_LEN)
    results = []
    for slot_num in range(SLOTS):
        inputs = x_all[slot_num]
        seg_row = segs[slot_num]
        query_proj = low(low_back((matmul(inputs, query_weight) + query_bias) * 0.125)).reshape(SLOT_LEN, HEADS, HEAD_DIM)
        key_proj = low(low_back(matmul(inputs, key_weight))).reshape(SLOT_LEN, HEADS, HEAD_DIM)
        value_proj = low(low_back(matmul(inputs, value_weight) + value_bias)).reshape(SLOT_LEN, HEADS, HEAD_DIM)

        def block_fn(pair_item, key_proj=key_proj, value_proj=value_proj, seg_row=seg_row):
            return attend(pair_item[0], key_proj, value_proj, pair_item[1], seg_row)
        context = lax.map(jax.checkpoint(block_fn), (query_proj.reshape(SLOT_LEN // row_block, row_block, HEADS, HEAD_DIM), seg_row.reshape(SLOT_LEN // row_block, row_block)))
        context = low(context.reshape(SLOT_LEN, D))
        attn_out = low_back(matmul(context, out_weight) + out_bias)
        norm_one = layer_norm(inputs + attn_out, gain_first, shift_first)
        up_pre = low_back(matmul(low(norm_one), up_weight) + up_bias)
        down_out = low_back(matmul(low(jax.nn.gelu(up_pre, approximate=False)), down_weight) + down_bias)
        results.append(layer_norm(norm_one + down_out, gain_second, shift_second))
    return jnp.stack(results)

def reference(tokens, cotangent, lengths, block_order, w_query, b_query, w_key, w_value, b_value, w_out, b_out, gain_one, shift_one, w_up, b_up, w_down, b_down, gain_two, shift_two):
    row_ids = jnp.arange(SLOT_LEN, dtype=jnp.int32)
    segs = jnp.stack([segment_ids(row_ids, block_order, jnp.cumsum(lengths[slot_num]).astype(jnp.int32), HALF) for slot_num in range(SLOTS)])
    valid = (segs < 3).astype(jnp.float32)
    params = (w_query, b_query, w_key, w_value, b_value, w_out, b_out, gain_one, shift_one, w_up, b_up, w_down, b_down, gain_two, shift_two)

    def wrapped(x_all, param_set):
        return layer_forward(x_all, param_set, segs)
    result, back_fn = jax.vjp(wrapped, tokens.astype(jnp.float32), params)
    grad_x, grad_p = back_fn(cotangent.astype(jnp.float32) * valid[:, :, None])
    return (result.astype(jnp.bfloat16), grad_x.astype(jnp.bfloat16), grad_p[0], grad_p[1], grad_p[2], grad_p[3], grad_p[4], grad_p[5], grad_p[6], grad_p[7], grad_p[8], grad_p[9], grad_p[10], grad_p[11], grad_p[12], grad_p[13], grad_p[14])
```

```python
from functools import partial

import jax
import jax.numpy as jnp
from jax import lax
from jax.experimental import pallas as pl
from jax.experimental.pallas import tpu as pltpu
from jax.sharding import PartitionSpec as P

HEADS = 12
HEAD_DIM = 64
LANES = 128
TILE = 512
FAR = -(2.0**40)
VMEM_BYTES = 60 << 20

low_type = jnp.bfloat16
epsilon = 1e-05


def dot_nt(left, right):
    return lax.dot_general(
        left, right, (((1,), (1,)), ((), ())), preferred_element_type=jnp.float32
    )


def dot_nn(left, right):
    return lax.dot_general(
        left, right, (((1,), (0,)), ((), ())), preferred_element_type=jnp.float32
    )


def layer_norm(hidden, gain_vec, shift_vec):
    centre = hidden - jnp.mean(hidden, axis=-1, keepdims=True)
    spread = jnp.mean(centre * centre, axis=-1, keepdims=True)
    return centre * lax.rsqrt(spread + epsilon) * gain_vec + shift_vec


def segment_of(position, seq_ends):
    return jnp.sum((position[:, None] >= seq_ends[None, :]).astype(jnp.int32), axis=1)


def owner_of(head, count):
    return head * count // HEADS


def greet_all(count, me):
    barrier = pltpu.get_barrier_semaphore()

    def greet(step, _):
        other = lax.rem(me + step, count)
        pl.semaphore_signal(
            barrier, inc=1, device_id={"ctx": other}, device_id_type=pl.DeviceIdType.MESH
        )
        return 0

    lax.fori_loop(1, count, greet, 0)
    pl.semaphore_wait(barrier, count - 1)


def to_heads_kernel(count, send_ref, recv_ref, send_sem, recv_sem, own_sem):
    me = lax.axis_index("ctx")
    greet_all(count, me)
    first = me * HEADS // count + 1

    def copy_for(head, source, owner):
        return pltpu.make_async_remote_copy(
            src_ref=send_ref.at[head],
            dst_ref=recv_ref.at[source],
            send_sem=send_sem.at[head],
            recv_sem=recv_sem.at[source],
            device_id={"ctx": owner},
            device_id_type=pl.DeviceIdType.MESH,
        )

    def own_copy(head):
        return pltpu.make_async_copy(send_ref.at[head], recv_ref.at[me], own_sem)

    def begin(step, _):
        head = lax.rem(first + step, HEADS)
        owner = owner_of(head, count)

        @pl.when(owner != me)
        def _():
            copy_for(head, me, owner).start()

        @pl.when(owner == me)
        def _():
            own_copy(head).start()

        return 0

    lax.fori_loop(0, HEADS, begin, 0)

    def finish(head, _):
        owner = owner_of(head, count)

        @pl.when(owner != me)
        def _():
            copy_for(head, me, owner).wait_send()

        @pl.when(owner == me)
        def _():
            own_copy(head).wait()

            def arrive(source, _):
                @pl.when(source != me)
                def _():
                    copy_for(head, source, owner).wait_recv()

                return 0

            lax.fori_loop(0, count, arrive, 0)

        return 0

    lax.fori_loop(0, HEADS, finish, 0)


def to_heads(send, count, collective_id):
    rows = send.shape[1]
    return pl.pallas_call(
        partial(to_heads_kernel, count),
        out_shape=jax.ShapeDtypeStruct((count, rows, LANES), low_type),
        in_specs=[pl.BlockSpec(memory_space=pltpu.VMEM)],
        out_specs=pl.BlockSpec(memory_space=pltpu.VMEM),
        scratch_shapes=[
            pltpu.SemaphoreType.DMA((HEADS,)),
            pltpu.SemaphoreType.DMA((count,)),
            pltpu.SemaphoreType.DMA,
        ],
        compiler_params=pltpu.CompilerParams(
            collective_id=collective_id, has_side_effects=True, vmem_limit_bytes=VMEM_BYTES
        ),
        cost_estimate=pl.CostEstimate(
            flops=rows * 40_000_000, bytes_accessed=send.size * 4, transcendentals=0
        ),
        name=f"to_heads_{rows}",
    )(send)


def to_rows_kernel(count, send_ref, recv_ref, send_sem, recv_sem, own_sem):
    me = lax.axis_index("ctx")
    greet_all(count, me)

    def copy_for(head, target):
        return pltpu.make_async_remote_copy(
            src_ref=send_ref.at[target],
            dst_ref=recv_ref.at[head],
            send_sem=send_sem.at[target],
            recv_sem=recv_sem.at[head],
            device_id={"ctx": target},
            device_id_type=pl.DeviceIdType.MESH,
        )

    def own_copy(head):
        return pltpu.make_async_copy(send_ref.at[me], recv_ref.at[head], own_sem)

    def begin(head, _):
        @pl.when(owner_of(head, count) == me)
        def _():
            own_copy(head).start()

            def push(step, _):
                copy_for(head, lax.rem(me + step, count)).start()
                return 0

            lax.fori_loop(1, count, push, 0)

        return 0

    lax.fori_loop(0, HEADS, begin, 0)

    def finish(head, _):
        @pl.when(owner_of(head, count) == me)
        def _():
            own_copy(head).wait()

            def leave(step, _):
                copy_for(head, lax.rem(me + step, count)).wait_send()
                return 0

            lax.fori_loop(1, count, leave, 0)

        @pl.when(owner_of(head, count) != me)
        def _():
            copy_for(head, me).wait_recv()

        return 0

    lax.fori_loop(0, HEADS, finish, 0)


def to_rows(send, count, collective_id):
    rows = send.shape[1]
    return pl.pallas_call(
        partial(to_rows_kernel, count),
        out_shape=jax.ShapeDtypeStruct((HEADS, rows, LANES), low_type),
        in_specs=[pl.BlockSpec(memory_space=pltpu.VMEM)],
        out_specs=pl.BlockSpec(memory_space=pltpu.VMEM),
        scratch_shapes=[
            pltpu.SemaphoreType.DMA((count,)),
            pltpu.SemaphoreType.DMA((HEADS,)),
            pltpu.SemaphoreType.DMA,
        ],
        compiler_params=pltpu.CompilerParams(
            collective_id=collective_id, has_side_effects=True, vmem_limit_bytes=VMEM_BYTES
        ),
        cost_estimate=pl.CostEstimate(
            flops=rows * 40_000_000, bytes_accessed=send.size * 4, transcendentals=0
        ),
        name=f"to_rows_{rows}",
    )(send)


def project_kernel(x_ref, wq_ref, wkv_ref, bq_ref, bkv_ref, out_ref):
    rows = x_ref.shape[0]
    half = rows // 2
    step = 4
    for base in range(0, HEADS, step):
        cols = slice(base * LANES, (base + step) * LANES)
        both = (dot_nn(x_ref[...], wkv_ref[:, cols]) + bkv_ref[:, cols]).astype(low_type)
        for at in range(step):
            out_ref[base + at, 0:rows, :] = both[:, at * LANES : (at + 1) * LANES]
        cols = slice(base * HEAD_DIM, (base + step) * HEAD_DIM)
        query = ((dot_nn(x_ref[...], wq_ref[:, cols]) + bq_ref[:, cols]) * 0.125).astype(low_type)
        for at in range(step):
            lanes = slice(at * HEAD_DIM, (at + 1) * HEAD_DIM)
            out_ref[base + at, rows : rows + half, :] = jnp.concatenate(
                [query[:half, lanes], query[half:, lanes]], axis=1
            )


def project(x, wq, wkv, bq, bkv):
    rows = x.shape[0]
    vmem = pl.BlockSpec(memory_space=pltpu.VMEM)
    return pl.pallas_call(
        project_kernel,
        out_shape=jax.ShapeDtypeStruct((HEADS, rows + rows // 2, LANES), low_type),
        in_specs=[vmem] * 5,
        out_specs=vmem,
        compiler_params=pltpu.CompilerParams(vmem_limit_bytes=VMEM_BYTES),
        name="project",
    )(x, wq, wkv, bq, bkv)


def tile_range(meta_ref, first, last, total):
    end_a, end_b, end_c = meta_ref[0], meta_ref[1], meta_ref[2]
    low = jnp.where(
        first >= end_c, end_c, jnp.where(first >= end_b, end_b, jnp.where(first >= end_a, end_a, 0))
    )
    high = jnp.where(
        last >= end_c,
        total,
        jnp.where(last >= end_b, end_c, jnp.where(last >= end_a, end_b, end_a)),
    )
    return low // TILE, (high + TILE - 1) // TILE


def attend_kernel(meta_ref, order_ref, recv_ref, out_ref, qa_ref, ka_ref, va_ref, sum_ref):
    count = recv_ref.shape[0]
    half = recv_ref.shape[1] // 3
    total = qa_ref.shape[0]

    @pl.when(meta_ref[3] == 1)
    def _():
        lane = lax.broadcasted_iota(jnp.int32, (half, LANES), 1)
        lower = lane < HEAD_DIM
        row = lax.broadcasted_iota(jnp.int32, (half, LANES), 0)

        def place(source, _):
            query = recv_ref[source, 2 * half :, :].astype(jnp.float32)
            for part in range(2):
                first = pl.multiple_of(order_ref[2 * source + part] * half, half)
                position = first + row
                segment = (
                    (position >= meta_ref[0]).astype(jnp.int32)
                    + (position >= meta_ref[1]).astype(jnp.int32)
                    + (position >= meta_ref[2]).astype(jnp.int32)
                )
                mine = (lane - HEAD_DIM) == segment
                other = (lane < HEAD_DIM + 4) & (~mine)
                pair = recv_ref[source, part * half : (part + 1) * half, :].astype(jnp.float32)
                if part == 1:
                    query = pltpu.roll(query, HEAD_DIM, 1)
                mark_k = jnp.where(
                    other, FAR, jnp.where((lane >= HEAD_DIM + 4) & (lane < HEAD_DIM + 7), 1.0, 0.0)
                )
                rows = pl.ds(first, half)
                qa_ref[rows, :] = jnp.where(lower, query, jnp.where(mine, 1.0, 0.0)).astype(low_type)
                ka_ref[rows, :] = jnp.where(lower, pair, mark_k).astype(low_type)
                va_ref[rows, :] = jnp.where(lower, 1.0, pair).astype(low_type)
            return 0

        lax.fori_loop(0, count, place, 0)

        def query_step(index, _):
            first = pl.multiple_of(index * TILE, TILE)
            rows = pl.ds(first, TILE)
            begin, end = tile_range(meta_ref, first, first + TILE - 1, total)
            query = qa_ref[rows, :]
            sum_ref[rows, :] = jnp.zeros((TILE, LANES), jnp.float32)

            def key_step(key_index, _):
                keys = pl.ds(pl.multiple_of(key_index * TILE, TILE), TILE)
                expo = jnp.exp(dot_nt(query, ka_ref[keys, :])).astype(low_type)
                sum_ref[rows, :] += dot_nn(expo, va_ref[keys, :])
                return 0

            lax.fori_loop(begin, end, key_step, 0)
            return 0

        lax.fori_loop(0, total // TILE, query_step, 0)

        def give(source, _):
            parts = []
            for part in range(2):
                first = pl.multiple_of(order_ref[2 * source + part] * half, half)
                block = sum_ref[pl.ds(first, half), :]
                parts.append((block, pltpu.roll(block, HEAD_DIM, 1)))
            top = jnp.where(lower, parts[0][1], parts[1][0])
            bottom = jnp.where(lower, parts[0][0], parts[1][1])
            out_ref[source] = (top / bottom).astype(low_type)
            return 0

        lax.fori_loop(0, count, give, 0)


def attend(meta, order, recv):
    count, rows, _ = recv.shape
    total = count * rows * 2 // 3
    vmem = pl.BlockSpec(memory_space=pltpu.VMEM)
    smem = pl.BlockSpec(memory_space=pltpu.SMEM)
    whole = jax.ShapeDtypeStruct((total, LANES), low_type)
    return pl.pallas_call(
        attend_kernel,
        out_shape=(
            jax.ShapeDtypeStruct((count, rows // 3, LANES), low_type),
            whole,
            whole,
            whole,
            jax.ShapeDtypeStruct((total, LANES), jnp.float32),
        ),
        in_specs=[smem, smem, vmem],
        out_specs=(vmem,) * 5,
        compiler_params=pltpu.CompilerParams(vmem_limit_bytes=VMEM_BYTES),
        cost_estimate=pl.CostEstimate(
            flops=total * total * LANES * 8, bytes_accessed=total * LANES * 12, transcendentals=0
        ),
        name="attend",
    )(meta, order, recv)


def split_three(value):
    first = value.astype(low_type).astype(jnp.float32)
    rest = value - first
    second = rest.astype(low_type).astype(jnp.float32)
    return first, second, rest - second


def attend_back_kernel(
    meta_ref,
    order_ref,
    recv_ref,
    qa_ref,
    ka_ref,
    va_ref,
    sum_ref,
    out_ref,
    qb_ref,
    da_ref,
    kt_ref,
    dkv_ref,
    dq_ref,
    acc_ref,
):
    count = recv_ref.shape[0]
    half = recv_ref.shape[1]
    total = qa_ref.shape[0]

    @pl.when(meta_ref[3] == 1)
    def _():
        lane = lax.broadcasted_iota(jnp.int32, (half, LANES), 1)
        lower = lane < HEAD_DIM

        def place(source, _):
            given = recv_ref[source].astype(jnp.float32)
            for part in range(2):
                first = pl.multiple_of(order_ref[2 * source + part] * half, half)
                rows = pl.ds(first, half)
                block = sum_ref[rows, :]
                turned = pltpu.roll(block, HEAD_DIM, 1)
                d_context = pltpu.roll(given, HEAD_DIM, 1) if part == 0 else given
                product = jnp.where(lower, 0.0, d_context * (block / turned))
                minus = -jnp.sum(product, axis=1, keepdims=True)
                one, two, three = split_three(minus)
                mark = jnp.where(
                    lane == 0, one, jnp.where(lane == 1, two, jnp.where(lane == 2, three, 0.0))
                )
                da_ref[rows, :] = jnp.where(lower, mark, d_context).astype(low_type)
                one, two, three = split_three(-jnp.log(turned))
                at = lane - (HEAD_DIM + 4)
                mark = jnp.where(at == 0, one, jnp.where(at == 1, two, three))
                query = qa_ref[rows, :].astype(jnp.float32)
                qb_ref[rows, :] = jnp.where((at >= 0) & (at < 3), mark, query).astype(low_type)
            return 0

        lax.fori_loop(0, count, place, 0)

        def prepare(index, _):
            rows = pl.ds(pl.multiple_of(index * TILE, TILE), TILE)
            kt_ref[:, rows] = jnp.transpose(ka_ref[rows, :])[:HEAD_DIM, :]
            dkv_ref[rows, :] = jnp.zeros((TILE, LANES), jnp.float32)
            return 0

        lax.fori_loop(0, total // TILE, prepare, 0)

        lower_tile = lax.broadcasted_iota(jnp.int32, (TILE, LANES), 1) < HEAD_DIM

        def query_step(index, _):
            first = pl.multiple_of(index * TILE, TILE)
            rows = pl.ds(first, TILE)
            begin, end = tile_range(meta_ref, first, first + TILE - 1, total)
            query = qb_ref[rows, :]
            given = da_ref[rows, :]
            query_only = jnp.where(lower_tile, query.astype(jnp.float32), 0.0).astype(low_type)
            given_only = jnp.where(lower_tile, 0.0, given.astype(jnp.float32)).astype(low_type)
            acc_ref[...] = jnp.zeros_like(acc_ref)

            def key_step(key_index, _):
                keys = pl.ds(pl.multiple_of(key_index * TILE, TILE), TILE)
                prob = jnp.exp(dot_nt(ka_ref[keys, :], query))
                d_scores = (prob * dot_nt(va_ref[keys, :], given)).astype(low_type)
                dkv_ref[keys, :] += dot_nn(d_scores, query_only) + dot_nn(
                    prob.astype(low_type), given_only
                )
                acc_ref[...] += dot_nn(kt_ref[:, keys], d_scores)
                return 0

            lax.fori_loop(begin, end, key_step, 0)
            dq_ref[rows, :] = jnp.transpose(acc_ref[...])
            return 0

        lax.fori_loop(0, total // TILE, query_step, 0)

        def give(source, _):
            queries = []
            for part in range(2):
                first = pl.multiple_of(order_ref[2 * source + part] * half, half)
                rows = pl.ds(first, half)
                out_ref[source, part * half : (part + 1) * half, :] = dkv_ref[rows, :].astype(low_type)
                queries.append(dq_ref[rows, :])
            out_ref[source, 2 * half :, :] = jnp.concatenate(queries, axis=1).astype(low_type)
            return 0

        lax.fori_loop(0, count, give, 0)


def attend_back(meta, order, recv, qa, ka, va, sums):
    count, half, _ = recv.shape
    total = qa.shape[0]
    vmem = pl.BlockSpec(memory_space=pltpu.VMEM)
    smem = pl.BlockSpec(memory_space=pltpu.SMEM)
    return pl.pallas_call(
        attend_back_kernel,
        out_shape=jax.ShapeDtypeStruct((count, 3 * half, LANES), low_type),
        in_specs=[smem, smem] + [vmem] * 5,
        out_specs=vmem,
        scratch_shapes=[
            pltpu.VMEM((total, LANES), low_type),
            pltpu.VMEM((total, LANES), low_type),
            pltpu.VMEM((HEAD_DIM, total), low_type),
            pltpu.VMEM((total, LANES), jnp.float32),
            pltpu.VMEM((total, HEAD_DIM), jnp.float32),
            pltpu.VMEM((HEAD_DIM, TILE), jnp.float32),
        ],
        compiler_params=pltpu.CompilerParams(vmem_limit_bytes=VMEM_BYTES),
        cost_estimate=pl.CostEstimate(
            flops=total * total * LANES * 16, bytes_accessed=total * LANES * 16, transcendentals=0
        ),
        name="attend_back",
    )(meta, order, recv, qa, ka, va, sums)


def pack_columns(vectors, rows):
    columns = jnp.stack([vec.astype(low_type) for vec in vectors], axis=1)
    return jnp.pad(columns, ((0, 0), (0, LANES - len(vectors))))


def column_sums(terms):
    block = jnp.stack([jnp.sum(term, axis=0) for term in terms], axis=1).astype(low_type)
    return jnp.pad(block, ((0, 0), (0, LANES - len(terms))))


def rows_of_columns(block, wanted):
    pick = jnp.eye(LANES, 8, dtype=low_type)
    return jnp.einsum("fk,kj->jf", block, pick, preferred_element_type=jnp.float32)[:wanted]


def reduce_shards(grad):
    part = lax.psum_scatter(
        grad.astype(low_type), ("wa", "ctx"), scatter_dimension=0, tiled=True
    )
    return lax.all_gather(part, "ctx", axis=0, tiled=True)


def body(
    count,
    tokens,
    cotangent,
    lengths,
    block_order,
    w_query,
    b_query,
    w_key,
    w_value,
    b_value,
    w_out,
    b_out,
    gain_one,
    shift_one,
    w_up,
    b_up,
    w_down,
    b_down,
    gain_two,
    shift_two,
):
    inputs = tokens[0]
    tok_rows, width = inputs.shape
    wide = w_up.shape[1]
    half = tok_rows // 2
    shard = w_query.shape[0]
    me = lax.axis_index("ctx")
    seq_ends = jnp.cumsum(lengths[0])
    own_blocks = lax.dynamic_slice(block_order, (2 * me,), (2,))
    position = (own_blocks[:, None] * half + jnp.arange(half, dtype=jnp.int32)[None, :]).reshape(-1)
    own_seg = segment_of(position, seq_ends)
    owns = jnp.any(me == jnp.arange(HEADS, dtype=jnp.int32) * count // HEADS).astype(jnp.int32)
    meta = jnp.concatenate([seq_ends.astype(jnp.int32), owns[None]])

    def gather_rows(shard_block):
        return lax.all_gather(shard_block, "wa", axis=0, tiled=True)

    pair = jnp.stack(
        [
            w_key.astype(low_type).reshape(shard, HEADS, HEAD_DIM),
            w_value.astype(low_type).reshape(shard, HEADS, HEAD_DIM),
        ],
        axis=2,
    ).reshape(shard, 2 * width)
    vectors = pack_columns(
        [b_query, b_value, b_out, gain_one, shift_one, gain_two, shift_two, b_down], shard
    )
    first_pack = gather_rows(
        jnp.concatenate([w_query.astype(low_type), pair, vectors], axis=1)
    )
    query_weight = first_pack[:, :width]
    pair_weight = first_pack[:, width : 3 * width]
    vector_rows = rows_of_columns(first_pack[:, 3 * width :], 8)
    query_bias, value_bias, out_bias, gain_first, shift_first, gain_second, shift_second, down_bias = (
        vector_rows[index] for index in range(8)
    )
    pair_bias = jnp.stack(
        [jnp.zeros((HEADS, HEAD_DIM), jnp.float32), value_bias.reshape(HEADS, HEAD_DIM)], axis=1
    ).reshape(1, 2 * width)

    out_weight = gather_rows(w_out.astype(low_type))
    up_weight = gather_rows(w_up.astype(low_type))
    down_pack = gather_rows(
        jnp.concatenate([w_down.astype(low_type), pack_columns([b_up], 4 * shard)], axis=1)
    )
    down_weight = down_pack[:, :width]
    up_bias = rows_of_columns(down_pack[:, width:], 1)[0]

    packed = project(inputs, query_weight, pair_weight, query_bias[None, :], pair_bias)
    at_head = to_heads(packed, count, 0)
    context_out, qa, ka, va, sums = attend(meta, block_order, at_head)
    context_in = to_rows(context_out, count, 1)
    context_low = (
        context_in.reshape(HEADS, half, 2, HEAD_DIM).transpose(2, 1, 0, 3).reshape(tok_rows, width)
    )

    attn_out = jnp.dot(context_low, out_weight, preferred_element_type=jnp.float32) + out_bias
    h_one = inputs.astype(jnp.float32) + attn_out
    norm_one, norm_one_back = jax.vjp(layer_norm, h_one, gain_first, shift_first)
    norm_low = norm_one.astype(low_type)
    up_pre = jnp.dot(norm_low, up_weight, preferred_element_type=jnp.float32) + up_bias
    gelu_out, gelu_back = jax.vjp(partial(jax.nn.gelu, approximate=False), up_pre)
    gelu_low = gelu_out.astype(low_type)
    down_out = jnp.dot(gelu_low, down_weight, preferred_element_type=jnp.float32) + down_bias
    h_two = norm_one + down_out
    result, norm_two_back = jax.vjp(layer_norm, h_two, gain_second, shift_second)
    activations = result.astype(low_type)[None]
    valid = (own_seg < 3).astype(jnp.float32)
    g_out = cotangent[0].astype(jnp.float32) * valid[:, None]
    d_htwo, grad_gain_second, grad_shift_second = norm_two_back(g_out)
    d_down = d_htwo.astype(low_type)
    d_gelu = jnp.einsum("td,fd->tf", d_down, down_weight, preferred_element_type=jnp.float32)
    (d_uppre,) = gelu_back(d_gelu)
    d_up = d_uppre.astype(low_type)
    d_yone = d_htwo + jnp.einsum("tf,df->td", d_up, up_weight, preferred_element_type=jnp.float32)
    d_hone, grad_gain_first, grad_shift_first = norm_one_back(d_yone)
    d_attn = d_hone.astype(low_type)
    d_context = jnp.einsum("td,cd->tc", d_attn, out_weight, preferred_element_type=jnp.float32)
    context_back = (
        d_context.astype(low_type)
        .reshape(2, half, HEADS, HEAD_DIM)
        .transpose(2, 1, 0, 3)
        .reshape(HEADS, half, LANES)
    )

    grad_wdown = jnp.einsum("tf,td->fd", gelu_low, d_down, preferred_element_type=jnp.float32)
    grad_wup = jnp.einsum("td,tf->df", norm_low, d_up, preferred_element_type=jnp.float32)
    grad_wout = jnp.einsum("tc,td->cd", context_low, d_attn, preferred_element_type=jnp.float32)
    down_block = jnp.concatenate(
        [grad_wdown.astype(low_type), column_sums([d_up.astype(jnp.float32)])], axis=1
    )
    vec_block = jnp.stack(
        [
            jnp.sum(d_attn.astype(jnp.float32), axis=0),
            grad_gain_first,
            grad_shift_first,
            jnp.sum(d_down.astype(jnp.float32), axis=0),
            grad_gain_second,
            grad_shift_second,
        ],
        axis=1,
    ).astype(low_type)
    out_block = jnp.concatenate(
        [grad_wout.astype(low_type), jnp.pad(vec_block, ((0, 0), (0, LANES - 6)))], axis=1
    )
    up_block = grad_wup.astype(low_type)
    context_back, down_block, out_block, up_block = lax.optimization_barrier(
        (context_back, down_block, out_block, up_block)
    )
    up_sum = reduce_shards(up_block)
    down_sum = reduce_shards(down_block)
    out_sum = reduce_shards(out_block)

    back_at_head = to_heads(context_back, count, 2)
    grads_out = attend_back(meta, block_order, back_at_head, qa, ka, va, sums)
    grads_in = to_rows(grads_out, count, 3)

    d_pair = grads_in[:, :tok_rows, :].transpose(1, 0, 2).reshape(tok_rows, 2 * width)
    d_queries = (
        grads_in[:, tok_rows:, :]
        .reshape(HEADS, half, 2, HEAD_DIM)
        .transpose(2, 1, 0, 3)
        .reshape(tok_rows, width)
        * jnp.asarray(0.125, low_type)
    )
    d_all = jnp.concatenate([d_queries, d_pair], axis=1)
    grad_all = jnp.einsum("tc,td->cd", inputs, d_all, preferred_element_type=jnp.float32)
    d_values = d_pair.reshape(tok_rows, HEADS, 2, HEAD_DIM)[:, :, 1, :].reshape(tok_rows, width)
    last_block = jnp.concatenate(
        [
            grad_all.astype(low_type),
            column_sums([d_queries.astype(jnp.float32), d_values.astype(jnp.float32)]),
        ],
        axis=1,
    )
    last_sum = reduce_shards(last_block)
    d_input = (
        d_hone
        + jnp.einsum("td,cd->tc", d_queries, query_weight, preferred_element_type=jnp.float32)
        + jnp.einsum("td,cd->tc", d_pair, pair_weight, preferred_element_type=jnp.float32)
    )
    input_grad = d_input.astype(low_type)[None]

    wide_grad = last_sum.astype(jnp.float32)
    pair_grad = wide_grad[:, width : 3 * width].reshape(shard, HEADS, 2, HEAD_DIM)
    out_grad = out_sum.astype(jnp.float32)
    down_grad = down_sum.astype(jnp.float32)
    return (
        activations,
        input_grad,
        wide_grad[:, :width],
        wide_grad[:, 3 * width],
        pair_grad[:, :, 0, :].reshape(shard, width),
        pair_grad[:, :, 1, :].reshape(shard, width),
        wide_grad[:, 3 * width + 1],
        out_grad[:, :width],
        out_grad[:, width],
        out_grad[:, width + 1],
        out_grad[:, width + 2],
        up_sum.astype(jnp.float32),
        down_grad[:, width],
        down_grad[:, :width],
        out_grad[:, width + 3],
        out_grad[:, width + 4],
        out_grad[:, width + 5],
    )


def solution(mesh):
    placed = (
        P("wa", "ctx", None),
        P("wa", "ctx", None),
        P("wa", None),
        P(),
        P("wa", None),
        P("wa"),
        P("wa", None),
        P("wa", None),
        P("wa"),
        P("wa", None),
        P("wa"),
        P("wa"),
        P("wa"),
        P("wa", None),
        P("wa"),
        P("wa", None),
        P("wa"),
        P("wa"),
        P("wa"),
    )
    return jax.shard_map(
        partial(body, mesh.shape["ctx"]),
        mesh=mesh,
        in_specs=placed,
        out_specs=(
            P("wa", "ctx", None),
            P("wa", "ctx", None),
            P("wa", None),
            P("wa"),
            P("wa", None),
            P("wa", None),
            P("wa"),
            P("wa", None),
            P("wa"),
            P("wa"),
            P("wa"),
            P("wa", None),
            P("wa"),
            P("wa", None),
            P("wa"),
            P("wa"),
            P("wa"),
        ),
        check_vma=False,
    )
```

```python
from functools import partial

import jax
import jax.numpy as jnp
from jax import lax
from jax.experimental import pallas as pl
from jax.experimental.pallas import tpu as pltpu
from jax.sharding import PartitionSpec as P

HEADS = 12
HEAD_DIM = 64
LANES = 128
TILE = 512
FAR = -(2.0**40)
VMEM_BYTES = 60 << 20

low_type = jnp.bfloat16
epsilon = 1e-05


def dot_nt(left, right):
    return lax.dot_general(
        left, right, (((1,), (1,)), ((), ())), preferred_element_type=jnp.float32
    )


def dot_nn(left, right):
    return lax.dot_general(
        left, right, (((1,), (0,)), ((), ())), preferred_element_type=jnp.float32
    )


def layer_norm(hidden, gain_vec, shift_vec):
    centre = hidden - jnp.mean(hidden, axis=-1, keepdims=True)
    spread = jnp.mean(centre * centre, axis=-1, keepdims=True)
    return centre * lax.rsqrt(spread + epsilon) * gain_vec + shift_vec


def segment_of(position, seq_ends):
    return jnp.sum((position[:, None] >= seq_ends[None, :]).astype(jnp.int32), axis=1)


def owner_of(head, count):
    return head * count // HEADS


def greet_all(count, me):
    barrier = pltpu.get_barrier_semaphore()

    def greet(step, _):
        other = lax.rem(me + step, count)
        pl.semaphore_signal(
            barrier, inc=1, device_id={"ctx": other}, device_id_type=pl.DeviceIdType.MESH
        )
        return 0

    lax.fori_loop(1, count, greet, 0)
    pl.semaphore_wait(barrier, count - 1)


def to_heads_kernel(count, send_ref, recv_ref, send_sem, recv_sem, own_sem):
    me = lax.axis_index("ctx")
    greet_all(count, me)
    first = me * HEADS // count + 1

    def copy_for(head, source, owner):
        return pltpu.make_async_remote_copy(
            src_ref=send_ref.at[head],
            dst_ref=recv_ref.at[source],
            send_sem=send_sem.at[head],
            recv_sem=recv_sem.at[source],
            device_id={"ctx": owner},
            device_id_type=pl.DeviceIdType.MESH,
        )

    def own_copy(head):
        return pltpu.make_async_copy(send_ref.at[head], recv_ref.at[me], own_sem)

    def begin(step, _):
        head = lax.rem(first + step, HEADS)
        owner = owner_of(head, count)

        @pl.when(owner != me)
        def _():
            copy_for(head, me, owner).start()

        @pl.when(owner == me)
        def _():
            own_copy(head).start()

        return 0

    lax.fori_loop(0, HEADS, begin, 0)

    def finish(head, _):
        owner = owner_of(head, count)

        @pl.when(owner != me)
        def _():
            copy_for(head, me, owner).wait_send()

        @pl.when(owner == me)
        def _():
            own_copy(head).wait()

            def arrive(source, _):
                @pl.when(source != me)
                def _():
                    copy_for(head, source, owner).wait_recv()

                return 0

            lax.fori_loop(0, count, arrive, 0)

        return 0

    lax.fori_loop(0, HEADS, finish, 0)


def to_heads(send, count, collective_id):
    rows = send.shape[1]
    return pl.pallas_call(
        partial(to_heads_kernel, count),
        out_shape=jax.ShapeDtypeStruct((count, rows, LANES), low_type),
        in_specs=[pl.BlockSpec(memory_space=pltpu.VMEM)],
        out_specs=pl.BlockSpec(memory_space=pltpu.VMEM),
        scratch_shapes=[
            pltpu.SemaphoreType.DMA((HEADS,)),
            pltpu.SemaphoreType.DMA((count,)),
            pltpu.SemaphoreType.DMA,
        ],
        compiler_params=pltpu.CompilerParams(
            collective_id=collective_id, has_side_effects=True, vmem_limit_bytes=VMEM_BYTES
        ),
        cost_estimate=pl.CostEstimate(
            flops=rows * 40_000_000, bytes_accessed=send.size * 4, transcendentals=0
        ),
        name=f"to_heads_{rows}",
    )(send)


def to_rows_kernel(count, send_ref, recv_ref, send_sem, recv_sem, own_sem):
    me = lax.axis_index("ctx")
    greet_all(count, me)

    def copy_for(head, target):
        return pltpu.make_async_remote_copy(
            src_ref=send_ref.at[target],
            dst_ref=recv_ref.at[head],
            send_sem=send_sem.at[target],
            recv_sem=recv_sem.at[head],
            device_id={"ctx": target},
            device_id_type=pl.DeviceIdType.MESH,
        )

    def own_copy(head):
        return pltpu.make_async_copy(send_ref.at[me], recv_ref.at[head], own_sem)

    def begin(head, _):
        @pl.when(owner_of(head, count) == me)
        def _():
            own_copy(head).start()

            def push(step, _):
                copy_for(head, lax.rem(me + step, count)).start()
                return 0

            lax.fori_loop(1, count, push, 0)

        return 0

    lax.fori_loop(0, HEADS, begin, 0)

    def finish(head, _):
        @pl.when(owner_of(head, count) == me)
        def _():
            own_copy(head).wait()

            def leave(step, _):
                copy_for(head, lax.rem(me + step, count)).wait_send()
                return 0

            lax.fori_loop(1, count, leave, 0)

        @pl.when(owner_of(head, count) != me)
        def _():
            copy_for(head, me).wait_recv()

        return 0

    lax.fori_loop(0, HEADS, finish, 0)


def to_rows(send, count, collective_id):
    rows = send.shape[1]
    return pl.pallas_call(
        partial(to_rows_kernel, count),
        out_shape=jax.ShapeDtypeStruct((HEADS, rows, LANES), low_type),
        in_specs=[pl.BlockSpec(memory_space=pltpu.VMEM)],
        out_specs=pl.BlockSpec(memory_space=pltpu.VMEM),
        scratch_shapes=[
            pltpu.SemaphoreType.DMA((count,)),
            pltpu.SemaphoreType.DMA((HEADS,)),
            pltpu.SemaphoreType.DMA,
        ],
        compiler_params=pltpu.CompilerParams(
            collective_id=collective_id, has_side_effects=True, vmem_limit_bytes=VMEM_BYTES
        ),
        cost_estimate=pl.CostEstimate(
            flops=rows * 40_000_000, bytes_accessed=send.size * 4, transcendentals=0
        ),
        name=f"to_rows_{rows}",
    )(send)


def project_kernel(x_ref, wq_ref, wkv_ref, bq_ref, bkv_ref, out_ref):
    rows = x_ref.shape[0]
    half = rows // 2
    step = 4
    for base in range(0, HEADS, step):
        cols = slice(base * LANES, (base + step) * LANES)
        both = (dot_nn(x_ref[...], wkv_ref[:, cols]) + bkv_ref[:, cols]).astype(low_type)
        for at in range(step):
            out_ref[base + at, 0:rows, :] = both[:, at * LANES : (at + 1) * LANES]
        cols = slice(base * HEAD_DIM, (base + step) * HEAD_DIM)
        query = ((dot_nn(x_ref[...], wq_ref[:, cols]) + bq_ref[:, cols]) * 0.125).astype(low_type)
        for at in range(step):
            lanes = slice(at * HEAD_DIM, (at + 1) * HEAD_DIM)
            out_ref[base + at, rows : rows + half, :] = jnp.concatenate(
                [query[:half, lanes], query[half:, lanes]], axis=1
            )


def project(x, wq, wkv, bq, bkv):
    rows = x.shape[0]
    vmem = pl.BlockSpec(memory_space=pltpu.VMEM)
    return pl.pallas_call(
        project_kernel,
        out_shape=jax.ShapeDtypeStruct((HEADS, rows + rows // 2, LANES), low_type),
        in_specs=[vmem] * 5,
        out_specs=vmem,
        compiler_params=pltpu.CompilerParams(vmem_limit_bytes=VMEM_BYTES),
        name="project",
    )(x, wq, wkv, bq, bkv)


def tile_range(meta_ref, first, last, total):
    end_a, end_b, end_c = meta_ref[0], meta_ref[1], meta_ref[2]
    low = jnp.where(
        first >= end_c, end_c, jnp.where(first >= end_b, end_b, jnp.where(first >= end_a, end_a, 0))
    )
    high = jnp.where(
        last >= end_c,
        total,
        jnp.where(last >= end_b, end_c, jnp.where(last >= end_a, end_b, end_a)),
    )
    return low // TILE, (high + TILE - 1) // TILE


def attend_kernel(meta_ref, order_ref, recv_ref, out_ref, qa_ref, ka_ref, va_ref, sum_ref):
    count = recv_ref.shape[0]
    half = recv_ref.shape[1] // 3
    total = qa_ref.shape[0]

    @pl.when(meta_ref[3] == 1)
    def _():
        lane = lax.broadcasted_iota(jnp.int32, (half, LANES), 1)
        lower = lane < HEAD_DIM
        row = lax.broadcasted_iota(jnp.int32, (half, LANES), 0)

        def place(source, _):
            query = recv_ref[source, 2 * half :, :].astype(jnp.float32)
            for part in range(2):
                first = pl.multiple_of(order_ref[2 * source + part] * half, half)
                position = first + row
                segment = (
                    (position >= meta_ref[0]).astype(jnp.int32)
                    + (position >= meta_ref[1]).astype(jnp.int32)
                    + (position >= meta_ref[2]).astype(jnp.int32)
                )
                mine = (lane - HEAD_DIM) == segment
                other = (lane < HEAD_DIM + 4) & (~mine)
                pair = recv_ref[source, part * half : (part + 1) * half, :].astype(jnp.float32)
                if part == 1:
                    query = pltpu.roll(query, HEAD_DIM, 1)
                mark_k = jnp.where(
                    other, FAR, jnp.where((lane >= HEAD_DIM + 4) & (lane < HEAD_DIM + 7), 1.0, 0.0)
                )
                rows = pl.ds(first, half)
                qa_ref[rows, :] = jnp.where(lower, query, jnp.where(mine, 1.0, 0.0)).astype(low_type)
                ka_ref[rows, :] = jnp.where(lower, pair, mark_k).astype(low_type)
                va_ref[rows, :] = jnp.where(lower, 1.0, pair).astype(low_type)
            return 0

        lax.fori_loop(0, count, place, 0)

        def query_step(index, _):
            first = pl.multiple_of(index * TILE, TILE)
            rows = pl.ds(first, TILE)
            begin, end = tile_range(meta_ref, first, first + TILE - 1, total)
            query = qa_ref[rows, :]
            sum_ref[rows, :] = jnp.zeros((TILE, LANES), jnp.float32)

            def key_step(key_index, _):
                keys = pl.ds(pl.multiple_of(key_index * TILE, TILE), TILE)
                expo = jnp.exp(dot_nt(query, ka_ref[keys, :])).astype(low_type)
                sum_ref[rows, :] += dot_nn(expo, va_ref[keys, :])
                return 0

            lax.fori_loop(begin, end, key_step, 0)
            return 0

        lax.fori_loop(0, total // TILE, query_step, 0)

        def give(source, _):
            parts = []
            for part in range(2):
                first = pl.multiple_of(order_ref[2 * source + part] * half, half)
                block = sum_ref[pl.ds(first, half), :]
                parts.append((block, pltpu.roll(block, HEAD_DIM, 1)))
            top = jnp.where(lower, parts[0][1], parts[1][0])
            bottom = jnp.where(lower, parts[0][0], parts[1][1])
            out_ref[source] = (top / bottom).astype(low_type)
            return 0

        lax.fori_loop(0, count, give, 0)


def attend(meta, order, recv):
    count, rows, _ = recv.shape
    total = count * rows * 2 // 3
    vmem = pl.BlockSpec(memory_space=pltpu.VMEM)
    smem = pl.BlockSpec(memory_space=pltpu.SMEM)
    whole = jax.ShapeDtypeStruct((total, LANES), low_type)
    return pl.pallas_call(
        attend_kernel,
        out_shape=(
            jax.ShapeDtypeStruct((count, rows // 3, LANES), low_type),
            whole,
            whole,
            whole,
            jax.ShapeDtypeStruct((total, LANES), jnp.float32),
        ),
        in_specs=[smem, smem, vmem],
        out_specs=(vmem,) * 5,
        compiler_params=pltpu.CompilerParams(vmem_limit_bytes=VMEM_BYTES),
        cost_estimate=pl.CostEstimate(
            flops=total * total * LANES * 8, bytes_accessed=total * LANES * 12, transcendentals=0
        ),
        name="attend",
    )(meta, order, recv)


def split_three(value):
    first = value.astype(low_type).astype(jnp.float32)
    rest = value - first
    second = rest.astype(low_type).astype(jnp.float32)
    return first, second, rest - second


def attend_back_kernel(
    meta_ref,
    order_ref,
    recv_ref,
    qa_ref,
    ka_ref,
    va_ref,
    sum_ref,
    out_ref,
    qb_ref,
    da_ref,
    kt_ref,
    dkv_ref,
    dq_ref,
    acc_ref,
):
    count = recv_ref.shape[0]
    half = recv_ref.shape[1]
    total = qa_ref.shape[0]

    @pl.when(meta_ref[3] == 1)
    def _():
        lane = lax.broadcasted_iota(jnp.int32, (half, LANES), 1)
        lower = lane < HEAD_DIM

        def place(source, _):
            given = recv_ref[source].astype(jnp.float32)
            for part in range(2):
                first = pl.multiple_of(order_ref[2 * source + part] * half, half)
                rows = pl.ds(first, half)
                block = sum_ref[rows, :]
                turned = pltpu.roll(block, HEAD_DIM, 1)
                d_context = pltpu.roll(given, HEAD_DIM, 1) if part == 0 else given
                product = jnp.where(lower, 0.0, d_context * (block / turned))
                minus = -jnp.sum(product, axis=1, keepdims=True)
                one, two, three = split_three(minus)
                mark = jnp.where(
                    lane == 0, one, jnp.where(lane == 1, two, jnp.where(lane == 2, three, 0.0))
                )
                da_ref[rows, :] = jnp.where(lower, mark, d_context).astype(low_type)
                one, two, three = split_three(-jnp.log(turned))
                at = lane - (HEAD_DIM + 4)
                mark = jnp.where(at == 0, one, jnp.where(at == 1, two, three))
                query = qa_ref[rows, :].astype(jnp.float32)
                qb_ref[rows, :] = jnp.where((at >= 0) & (at < 3), mark, query).astype(low_type)
            return 0

        lax.fori_loop(0, count, place, 0)

        def prepare(index, _):
            rows = pl.ds(pl.multiple_of(index * TILE, TILE), TILE)
            kt_ref[:, rows] = jnp.transpose(ka_ref[rows, :])[:HEAD_DIM, :]
            dkv_ref[rows, :] = jnp.zeros((TILE, LANES), jnp.float32)
            return 0

        lax.fori_loop(0, total // TILE, prepare, 0)

        lower_tile = lax.broadcasted_iota(jnp.int32, (TILE, LANES), 1) < HEAD_DIM

        def query_step(index, _):
            first = pl.multiple_of(index * TILE, TILE)
            rows = pl.ds(first, TILE)
            begin, end = tile_range(meta_ref, first, first + TILE - 1, total)
            query = qb_ref[rows, :]
            given = da_ref[rows, :]
            query_only = jnp.where(lower_tile, query.astype(jnp.float32), 0.0).astype(low_type)
            given_only = jnp.where(lower_tile, 0.0, given.astype(jnp.float32)).astype(low_type)
            acc_ref[...] = jnp.zeros_like(acc_ref)

            def key_step(key_index, _):
                keys = pl.ds(pl.multiple_of(key_index * TILE, TILE), TILE)
                prob = jnp.exp(dot_nt(ka_ref[keys, :], query))
                d_scores = (prob * dot_nt(va_ref[keys, :], given)).astype(low_type)
                dkv_ref[keys, :] += dot_nn(d_scores, query_only) + dot_nn(
                    prob.astype(low_type), given_only
                )
                acc_ref[...] += dot_nn(kt_ref[:, keys], d_scores)
                return 0

            lax.fori_loop(begin, end, key_step, 0)
            dq_ref[rows, :] = jnp.transpose(acc_ref[...])
            return 0

        lax.fori_loop(0, total // TILE, query_step, 0)

        def give(source, _):
            queries = []
            for part in range(2):
                first = pl.multiple_of(order_ref[2 * source + part] * half, half)
                rows = pl.ds(first, half)
                out_ref[source, part * half : (part + 1) * half, :] = dkv_ref[rows, :].astype(low_type)
                queries.append(dq_ref[rows, :])
            out_ref[source, 2 * half :, :] = jnp.concatenate(queries, axis=1).astype(low_type)
            return 0

        lax.fori_loop(0, count, give, 0)


def attend_back(meta, order, recv, qa, ka, va, sums):
    count, half, _ = recv.shape
    total = qa.shape[0]
    vmem = pl.BlockSpec(memory_space=pltpu.VMEM)
    smem = pl.BlockSpec(memory_space=pltpu.SMEM)
    return pl.pallas_call(
        attend_back_kernel,
        out_shape=jax.ShapeDtypeStruct((count, 3 * half, LANES), low_type),
        in_specs=[smem, smem] + [vmem] * 5,
        out_specs=vmem,
        scratch_shapes=[
            pltpu.VMEM((total, LANES), low_type),
            pltpu.VMEM((total, LANES), low_type),
            pltpu.VMEM((HEAD_DIM, total), low_type),
            pltpu.VMEM((total, LANES), jnp.float32),
            pltpu.VMEM((total, HEAD_DIM), jnp.float32),
            pltpu.VMEM((HEAD_DIM, TILE), jnp.float32),
        ],
        compiler_params=pltpu.CompilerParams(vmem_limit_bytes=VMEM_BYTES),
        cost_estimate=pl.CostEstimate(
            flops=total * total * LANES * 16, bytes_accessed=total * LANES * 16, transcendentals=0
        ),
        name="attend_back",
    )(meta, order, recv, qa, ka, va, sums)


PART_ORDERS = (("x", "z", "wa"), ("wa", "x", "z"), ("z", "wa", "x"))
GATHER_ORDERS = (("x", "z"), ("z", "x"), ("z", "x"))
SIZES = {"wa": 2, "x": 2, "z": 4}


class Links:
    def __init__(self):
        me = lax.axis_index("ctx")
        self.at = {
            "core": lax.rem(me, 2),
            "x": lax.rem(me // 2, 2),
            "z": me // 4,
            "wa": lax.axis_index("wa"),
        }

    def peer(self, axis, value):
        at = dict(self.at)
        at[axis] = value
        return {"ctx": at["z"] * 4 + at["x"] * 2 + at["core"], "wa": at["wa"]}


def part_columns(width):
    units = width // 512
    third = units // 4
    second = (units - third) // 2
    first = units - third - second
    bounds = [0, first * 512, (first + second) * 512, width]
    return [(bounds[k], bounds[k + 1]) for k in range(3)]


def grad_sum_kernel(g_ref, out_ref, core_buf, *rest):
    bufs, sems = rest[:9], rest[9:]
    send_sem, recv_sem = sems
    links = Links()
    rows, width = g_ref.shape[3], g_ref.shape[4]
    core, x, z, wa = (links.at[name] for name in ("core", "x", "z", "wa"))
    barrier = pltpu.get_barrier_semaphore()
    peers = [links.peer("core", 1 - core), links.peer("x", 1 - x), links.peer("wa", 1 - wa)]
    peers += [links.peer("z", lax.rem(z + step, 4)) for step in range(1, 4)]
    for peer in peers:
        pl.semaphore_signal(barrier, inc=1, device_id=peer, device_id_type=pl.DeviceIdType.MESH)
    pl.semaphore_wait(barrier, len(peers))
    used = [0]

    def remote(src, dst, peer):
        index = used[0]
        used[0] += 1
        copy = pltpu.make_async_remote_copy(
            src_ref=src,
            dst_ref=dst,
            send_sem=send_sem.at[index],
            recv_sem=recv_sem.at[index],
            device_id=peer,
            device_id_type=pl.DeviceIdType.MESH,
        )
        copy.start()
        return copy

    columns = part_columns(width)

    def z_columns(part, value):
        low, high = columns[part]
        quarter = (high - low) // 4
        return pl.ds(pl.multiple_of(low + value * quarter, LANES), quarter)

    def slab(part, held, axis=None, value=None):
        at = dict(links.at)
        if axis is not None:
            at[axis] = value
            held = held | {axis}
        low, high = columns[part]
        return g_ref.at[
            pl.ds(at["wa"], 1) if "wa" in held else pl.ds(0, 2),
            core,
            pl.ds(at["x"], 1) if "x" in held else pl.ds(0, 2),
            :,
            z_columns(part, at["z"]) if "z" in held else pl.ds(low, high - low),
        ]

    def add_into(target, sources):
        outer, inner, _, _ = target.shape
        for a in range(outer):
            for b in range(inner):

                def add(group, _):
                    some = pl.ds(pl.multiple_of(group * 16, 16), 16)
                    total = target[a, b, some, :].astype(jnp.float32)
                    for source in sources:
                        total = total + source[a, b, some, :].astype(jnp.float32)
                    target[a, b, some, :] = total.astype(low_type)
                    return 0

                lax.fori_loop(0, rows // 16, add, 0)

    core_copies = []
    for part in range(3):
        low, high = columns[part]
        cols = pl.ds(low, high - low)
        core_copies.append(
            remote(
                g_ref.at[:, 1 - core, :, :, cols],
                core_buf.at[:, :, :, cols],
                links.peer("core", 1 - core),
            )
        )

    def begin(part, stage):
        axis = PART_ORDERS[part][stage]
        held = set(PART_ORDERS[part][:stage])
        buf = bufs[part * 3 + stage]
        copies = []
        for step in range(1, SIZES[axis]):
            value = lax.rem(links.at[axis] + step, SIZES[axis])
            copies.append(
                remote(slab(part, held, axis, value), buf.at[step - 1], links.peer(axis, value))
            )
        return copies

    flying = {}
    for part in range(3):
        low, high = columns[part]
        core_copies[part].wait()
        add_into(slab(part, set()), [core_buf.at[:, :, :, pl.ds(low, high - low)]])
        flying[part] = begin(part, 0)
    for stage in range(3):
        for part in range(3):
            axis = PART_ORDERS[part][stage]
            for copy in flying[part]:
                copy.wait()
            buf = bufs[part * 3 + stage]
            add_into(
                slab(part, set(PART_ORDERS[part][: stage + 1])),
                [buf.at[step] for step in range(SIZES[axis] - 1)],
            )
            if stage < 2:
                flying[part] = begin(part, stage + 1)

    def out_slab(part, held):
        low, high = columns[part]
        return out_ref.at[
            core,
            pl.ds(x, 1) if "x" in held else pl.ds(0, 2),
            :,
            z_columns(part, z) if "z" in held else pl.ds(low, high - low),
        ]

    def spread(part, stage):
        axis = GATHER_ORDERS[part][stage]
        block = out_slab(part, set(GATHER_ORDERS[part][stage:]))
        return [
            remote(block, block, links.peer(axis, lax.rem(links.at[axis] + step, SIZES[axis])))
            for step in range(1, SIZES[axis])
        ]

    for part in range(3):
        out_slab(part, {"x", "z"})[...] = slab(part, {"wa", "x", "z"})[0]
        flying[part] = spread(part, 0)
    for stage in range(2):
        for part in range(3):
            for copy in flying[part]:
                copy.wait()
            if stage == 0:
                flying[part] = spread(part, 1)
            else:
                block = out_slab(part, set())
                flying[part] = [remote(block, block, links.peer("core", 1 - core))]
    for part in range(3):
        for copy in flying[part]:
            copy.wait()


def grad_sum(grad, collective_id):
    rows, width = grad.shape
    piece = rows // 8
    columns = part_columns(width)
    bufs = []
    for part in range(3):
        shape = {"wa": 2, "x": 2, "z": columns[part][1] - columns[part][0]}
        for axis in PART_ORDERS[part]:
            shape[axis] //= SIZES[axis]
            bufs.append(
                pltpu.VMEM((SIZES[axis] - 1, shape["wa"], shape["x"], piece, shape["z"]), low_type)
            )
    vmem = pl.BlockSpec(memory_space=pltpu.VMEM)
    total = pl.pallas_call(
        grad_sum_kernel,
        out_shape=jax.ShapeDtypeStruct((2, 2, piece, width), low_type),
        in_specs=[vmem],
        out_specs=vmem,
        scratch_shapes=[
            pltpu.VMEM((2, 2, piece, width), low_type),
            *bufs,
            pltpu.SemaphoreType.DMA((40,)),
            pltpu.SemaphoreType.DMA((40,)),
        ],
        compiler_params=pltpu.CompilerParams(
            collective_id=collective_id, has_side_effects=True, vmem_limit_bytes=VMEM_BYTES
        ),
        cost_estimate=pl.CostEstimate(
            flops=width * 15_000_000, bytes_accessed=grad.size * 4, transcendentals=0
        ),
        name=f"grad_sum_{width}",
    )(grad.reshape(2, 2, 2, piece, width))
    return total.reshape(rows // 2, width)


def pack_columns(vectors, rows):
    columns = jnp.stack([vec.astype(low_type) for vec in vectors], axis=1)
    return jnp.pad(columns, ((0, 0), (0, LANES - len(vectors))))


def column_sums(terms):
    block = jnp.stack([jnp.sum(term, axis=0) for term in terms], axis=1).astype(low_type)
    return jnp.pad(block, ((0, 0), (0, LANES - len(terms))))


def rows_of_columns(block, wanted):
    pick = jnp.eye(LANES, 8, dtype=low_type)
    return jnp.einsum("fk,kj->jf", block, pick, preferred_element_type=jnp.float32)[:wanted]


def reduce_shards(grad):
    part = lax.psum_scatter(
        grad.astype(low_type), ("wa", "ctx"), scatter_dimension=0, tiled=True
    )
    return lax.all_gather(part, "ctx", axis=0, tiled=True)


def body(
    count,
    tokens,
    cotangent,
    lengths,
    block_order,
    w_query,
    b_query,
    w_key,
    w_value,
    b_value,
    w_out,
    b_out,
    gain_one,
    shift_one,
    w_up,
    b_up,
    w_down,
    b_down,
    gain_two,
    shift_two,
):
    inputs = tokens[0]
    tok_rows, width = inputs.shape
    wide = w_up.shape[1]
    half = tok_rows // 2
    shard = w_query.shape[0]
    direct = count == 16 and width == 2 * shard and shard % 64 == 0 and wide == 4 * width
    me = lax.axis_index("ctx")
    seq_ends = jnp.cumsum(lengths[0])
    own_blocks = lax.dynamic_slice(block_order, (2 * me,), (2,))
    position = (own_blocks[:, None] * half + jnp.arange(half, dtype=jnp.int32)[None, :]).reshape(-1)
    own_seg = segment_of(position, seq_ends)
    owns = jnp.any(me == jnp.arange(HEADS, dtype=jnp.int32) * count // HEADS).astype(jnp.int32)
    meta = jnp.concatenate([seq_ends.astype(jnp.int32), owns[None]])

    def gather_rows(shard_block):
        return lax.all_gather(shard_block, "wa", axis=0, tiled=True)

    pair = jnp.stack(
        [
            w_key.astype(low_type).reshape(shard, HEADS, HEAD_DIM),
            w_value.astype(low_type).reshape(shard, HEADS, HEAD_DIM),
        ],
        axis=2,
    ).reshape(shard, 2 * width)
    vectors = pack_columns(
        [b_query, b_value, b_out, gain_one, shift_one, gain_two, shift_two, b_down], shard
    )
    first_pack = gather_rows(
        jnp.concatenate([w_query.astype(low_type), pair, vectors], axis=1)
    )
    query_weight = first_pack[:, :width]
    pair_weight = first_pack[:, width : 3 * width]
    vector_rows = rows_of_columns(first_pack[:, 3 * width :], 8)
    query_bias, value_bias, out_bias, gain_first, shift_first, gain_second, shift_second, down_bias = (
        vector_rows[index] for index in range(8)
    )
    pair_bias = jnp.stack(
        [jnp.zeros((HEADS, HEAD_DIM), jnp.float32), value_bias.reshape(HEADS, HEAD_DIM)], axis=1
    ).reshape(1, 2 * width)

    out_weight = gather_rows(w_out.astype(low_type))
    up_weight = gather_rows(w_up.astype(low_type))
    down_pack = gather_rows(
        jnp.concatenate([w_down.astype(low_type), pack_columns([b_up], 4 * shard)], axis=1)
    )
    down_weight = down_pack[:, :width]
    up_bias = rows_of_columns(down_pack[:, width:], 1)[0]

    packed = project(inputs, query_weight, pair_weight, query_bias[None, :], pair_bias)
    at_head = to_heads(packed, count, 0)
    context_out, qa, ka, va, sums = attend(meta, block_order, at_head)
    context_in = to_rows(context_out, count, 1)
    context_low = (
        context_in.reshape(HEADS, half, 2, HEAD_DIM).transpose(2, 1, 0, 3).reshape(tok_rows, width)
    )

    attn_out = jnp.dot(context_low, out_weight, preferred_element_type=jnp.float32) + out_bias
    h_one = inputs.astype(jnp.float32) + attn_out
    norm_one, norm_one_back = jax.vjp(layer_norm, h_one, gain_first, shift_first)
    norm_low = norm_one.astype(low_type)
    up_pre = jnp.dot(norm_low, up_weight, preferred_element_type=jnp.float32) + up_bias
    gelu_out, gelu_back = jax.vjp(partial(jax.nn.gelu, approximate=False), up_pre)
    gelu_low = gelu_out.astype(low_type)
    down_out = jnp.dot(gelu_low, down_weight, preferred_element_type=jnp.float32) + down_bias
    h_two = norm_one + down_out
    result, norm_two_back = jax.vjp(layer_norm, h_two, gain_second, shift_second)
    activations = result.astype(low_type)[None]
    valid = (own_seg < 3).astype(jnp.float32)
    g_out = cotangent[0].astype(jnp.float32) * valid[:, None]
    d_htwo, grad_gain_second, grad_shift_second = norm_two_back(g_out)
    d_down = d_htwo.astype(low_type)
    d_gelu = jnp.einsum("td,fd->tf", d_down, down_weight, preferred_element_type=jnp.float32)
    (d_uppre,) = gelu_back(d_gelu)
    d_up = d_uppre.astype(low_type)
    d_yone = d_htwo + jnp.einsum("tf,df->td", d_up, up_weight, preferred_element_type=jnp.float32)
    d_hone, grad_gain_first, grad_shift_first = norm_one_back(d_yone)
    d_attn = d_hone.astype(low_type)
    d_context = jnp.einsum("td,cd->tc", d_attn, out_weight, preferred_element_type=jnp.float32)
    context_back = (
        d_context.astype(low_type)
        .reshape(2, half, HEADS, HEAD_DIM)
        .transpose(2, 1, 0, 3)
        .reshape(HEADS, half, LANES)
    )

    grad_wdown = jnp.einsum("tf,td->fd", gelu_low, d_down, preferred_element_type=jnp.float32)
    grad_wup = jnp.einsum("td,tf->df", norm_low, d_up, preferred_element_type=jnp.float32)
    grad_wout = jnp.einsum("tc,td->cd", context_low, d_attn, preferred_element_type=jnp.float32)
    down_block = jnp.concatenate(
        [grad_wdown.astype(low_type), column_sums([d_up.astype(jnp.float32)])], axis=1
    )
    vec_block = jnp.stack(
        [
            jnp.sum(d_attn.astype(jnp.float32), axis=0),
            grad_gain_first,
            grad_shift_first,
            jnp.sum(d_down.astype(jnp.float32), axis=0),
            grad_gain_second,
            grad_shift_second,
        ],
        axis=1,
    ).astype(low_type)
    out_block = jnp.concatenate(
        [grad_wout.astype(low_type), jnp.pad(vec_block, ((0, 0), (0, LANES - 6)))], axis=1
    )
    up_block = grad_wup.astype(low_type)
    context_back, down_block, out_block, up_block = lax.optimization_barrier(
        (context_back, down_block, out_block, up_block)
    )
    back_at_head = to_heads(context_back, count, 2)
    grads_out = attend_back(meta, block_order, back_at_head, qa, ka, va, sums)
    grads_in = to_rows(grads_out, count, 3)

    d_pair = grads_in[:, :tok_rows, :].transpose(1, 0, 2).reshape(tok_rows, 2 * width)
    d_queries = (
        grads_in[:, tok_rows:, :]
        .reshape(HEADS, half, 2, HEAD_DIM)
        .transpose(2, 1, 0, 3)
        .reshape(tok_rows, width)
        * jnp.asarray(0.125, low_type)
    )
    d_all = jnp.concatenate([d_queries, d_pair], axis=1)
    grad_all = jnp.einsum("tc,td->cd", inputs, d_all, preferred_element_type=jnp.float32)
    d_values = d_pair.reshape(tok_rows, HEADS, 2, HEAD_DIM)[:, :, 1, :].reshape(tok_rows, width)
    last_block = jnp.concatenate(
        [
            grad_all.astype(low_type),
            column_sums([d_queries.astype(jnp.float32), d_values.astype(jnp.float32)]),
        ],
        axis=1,
    )
    if direct:
        fold = (2, 4, shard, width + LANES)
        wide_block = jnp.concatenate(
            [
                up_block,
                down_block.reshape(fold).transpose(0, 2, 1, 3).reshape(2 * shard, -1),
                out_block,
                last_block,
            ],
            axis=1,
        )
        unused = -wide_block.shape[1] % 512
        wide_sum = grad_sum(jnp.pad(wide_block, ((0, 0), (0, unused))), 4)
        edges = [0]
        for piece in (wide, 4 * (width + LANES), width + LANES, 3 * width + LANES):
            edges.append(edges[-1] + piece)
        up_sum, down_sum, out_sum, last_sum = (
            wide_sum[:, edges[k] : edges[k + 1]] for k in range(4)
        )
        down_sum = down_sum.reshape(shard, 4, -1).transpose(1, 0, 2).reshape(4 * shard, -1)
    else:
        up_sum, down_sum, out_sum, last_sum = (
            reduce_shards(block) for block in (up_block, down_block, out_block, last_block)
        )
    d_input = (
        d_hone
        + jnp.einsum("td,cd->tc", d_queries, query_weight, preferred_element_type=jnp.float32)
        + jnp.einsum("td,cd->tc", d_pair, pair_weight, preferred_element_type=jnp.float32)
    )
    input_grad = d_input.astype(low_type)[None]

    wide_grad = last_sum.astype(jnp.float32)
    pair_grad = wide_grad[:, width : 3 * width].reshape(shard, HEADS, 2, HEAD_DIM)
    out_grad = out_sum.astype(jnp.float32)
    down_grad = down_sum.astype(jnp.float32)
    return (
        activations,
        input_grad,
        wide_grad[:, :width],
        wide_grad[:, 3 * width],
        pair_grad[:, :, 0, :].reshape(shard, width),
        pair_grad[:, :, 1, :].reshape(shard, width),
        wide_grad[:, 3 * width + 1],
        out_grad[:, :width],
        out_grad[:, width],
        out_grad[:, width + 1],
        out_grad[:, width + 2],
        up_sum.astype(jnp.float32),
        down_grad[:, width],
        down_grad[:, :width],
        out_grad[:, width + 3],
        out_grad[:, width + 4],
        out_grad[:, width + 5],
    )


def solution(mesh):
    placed = (
        P("wa", "ctx", None),
        P("wa", "ctx", None),
        P("wa", None),
        P(),
        P("wa", None),
        P("wa"),
        P("wa", None),
        P("wa", None),
        P("wa"),
        P("wa", None),
        P("wa"),
        P("wa"),
        P("wa"),
        P("wa", None),
        P("wa"),
        P("wa", None),
        P("wa"),
        P("wa"),
        P("wa"),
    )
    return jax.shard_map(
        partial(body, mesh.shape["ctx"]),
        mesh=mesh,
        in_specs=placed,
        out_specs=(
            P("wa", "ctx", None),
            P("wa", "ctx", None),
            P("wa", None),
            P("wa"),
            P("wa", None),
            P("wa", None),
            P("wa"),
            P("wa", None),
            P("wa"),
            P("wa"),
            P("wa"),
            P("wa", None),
            P("wa"),
            P("wa", None),
            P("wa"),
            P("wa"),
            P("wa"),
        ),
        check_vma=False,
    )
```

```python
from functools import partial

import jax
import jax.numpy as jnp
from jax import lax
from jax.experimental import pallas as pl
from jax.experimental.pallas import tpu as pltpu
from jax.sharding import PartitionSpec as P

HEADS = 12
HEAD_DIM = 64
LANES = 128
TILE = 512
FAR = -(2.0**40)
VMEM_BYTES = 60 << 20

low_type = jnp.bfloat16
epsilon = 1e-05


def dot_nt(left, right):
    return lax.dot_general(
        left, right, (((1,), (1,)), ((), ())), preferred_element_type=jnp.float32
    )


def dot_nn(left, right):
    return lax.dot_general(
        left, right, (((1,), (0,)), ((), ())), preferred_element_type=jnp.float32
    )


def layer_norm(hidden, gain_vec, shift_vec):
    centre = hidden - jnp.mean(hidden, axis=-1, keepdims=True)
    spread = jnp.mean(centre * centre, axis=-1, keepdims=True)
    return centre * lax.rsqrt(spread + epsilon) * gain_vec + shift_vec


def segment_of(position, seq_ends):
    return jnp.sum((position[:, None] >= seq_ends[None, :]).astype(jnp.int32), axis=1)


def owner_of(head, count):
    return head * count // HEADS


def greet_all(count, me):
    barrier = pltpu.get_barrier_semaphore()

    def greet(step, _):
        other = lax.rem(me + step, count)
        pl.semaphore_signal(
            barrier, inc=1, device_id={"ctx": other}, device_id_type=pl.DeviceIdType.MESH
        )
        return 0

    lax.fori_loop(1, count, greet, 0)
    pl.semaphore_wait(barrier, count - 1)


def to_heads_kernel(count, send_ref, recv_ref, send_sem, recv_sem, own_sem):
    me = lax.axis_index("ctx")
    greet_all(count, me)
    first = me * HEADS // count + 1

    def copy_for(head, source, owner):
        return pltpu.make_async_remote_copy(
            src_ref=send_ref.at[head],
            dst_ref=recv_ref.at[source],
            send_sem=send_sem.at[head],
            recv_sem=recv_sem.at[source],
            device_id={"ctx": owner},
            device_id_type=pl.DeviceIdType.MESH,
        )

    def own_copy(head):
        return pltpu.make_async_copy(send_ref.at[head], recv_ref.at[me], own_sem)

    def begin(step, _):
        head = lax.rem(first + step, HEADS)
        owner = owner_of(head, count)

        @pl.when(owner != me)
        def _():
            copy_for(head, me, owner).start()

        @pl.when(owner == me)
        def _():
            own_copy(head).start()

        return 0

    lax.fori_loop(0, HEADS, begin, 0)

    def finish(head, _):
        owner = owner_of(head, count)

        @pl.when(owner != me)
        def _():
            copy_for(head, me, owner).wait_send()

        @pl.when(owner == me)
        def _():
            own_copy(head).wait()

            def arrive(source, _):
                @pl.when(source != me)
                def _():
                    copy_for(head, source, owner).wait_recv()

                return 0

            lax.fori_loop(0, count, arrive, 0)

        return 0

    lax.fori_loop(0, HEADS, finish, 0)


def to_heads(send, count, collective_id):
    rows = send.shape[1]
    return pl.pallas_call(
        partial(to_heads_kernel, count),
        out_shape=jax.ShapeDtypeStruct((count, rows, LANES), low_type),
        in_specs=[pl.BlockSpec(memory_space=pltpu.VMEM)],
        out_specs=pl.BlockSpec(memory_space=pltpu.VMEM),
        scratch_shapes=[
            pltpu.SemaphoreType.DMA((HEADS,)),
            pltpu.SemaphoreType.DMA((count,)),
            pltpu.SemaphoreType.DMA,
        ],
        compiler_params=pltpu.CompilerParams(
            collective_id=collective_id, has_side_effects=True, vmem_limit_bytes=VMEM_BYTES
        ),
        cost_estimate=pl.CostEstimate(
            flops=rows * 250_000_000, bytes_accessed=send.size * 4, transcendentals=0
        ),
        name=f"to_heads_{rows}",
    )(send)


def to_rows_kernel(count, send_ref, recv_ref, send_sem, recv_sem, own_sem):
    me = lax.axis_index("ctx")
    greet_all(count, me)

    def copy_for(head, target):
        return pltpu.make_async_remote_copy(
            src_ref=send_ref.at[target],
            dst_ref=recv_ref.at[head],
            send_sem=send_sem.at[target],
            recv_sem=recv_sem.at[head],
            device_id={"ctx": target},
            device_id_type=pl.DeviceIdType.MESH,
        )

    def own_copy(head):
        return pltpu.make_async_copy(send_ref.at[me], recv_ref.at[head], own_sem)

    def begin(head, _):
        @pl.when(owner_of(head, count) == me)
        def _():
            own_copy(head).start()

            def push(step, _):
                copy_for(head, lax.rem(me + step, count)).start()
                return 0

            lax.fori_loop(1, count, push, 0)

        return 0

    lax.fori_loop(0, HEADS, begin, 0)

    def finish(head, _):
        @pl.when(owner_of(head, count) == me)
        def _():
            own_copy(head).wait()

            def leave(step, _):
                copy_for(head, lax.rem(me + step, count)).wait_send()
                return 0

            lax.fori_loop(1, count, leave, 0)

        @pl.when(owner_of(head, count) != me)
        def _():
            copy_for(head, me).wait_recv()

        return 0

    lax.fori_loop(0, HEADS, finish, 0)


def to_rows(send, count, collective_id):
    rows = send.shape[1]
    return pl.pallas_call(
        partial(to_rows_kernel, count),
        out_shape=jax.ShapeDtypeStruct((HEADS, rows, LANES), low_type),
        in_specs=[pl.BlockSpec(memory_space=pltpu.VMEM)],
        out_specs=pl.BlockSpec(memory_space=pltpu.VMEM),
        scratch_shapes=[
            pltpu.SemaphoreType.DMA((count,)),
            pltpu.SemaphoreType.DMA((HEADS,)),
            pltpu.SemaphoreType.DMA,
        ],
        compiler_params=pltpu.CompilerParams(
            collective_id=collective_id, has_side_effects=True, vmem_limit_bytes=VMEM_BYTES
        ),
        cost_estimate=pl.CostEstimate(
            flops=rows * 250_000_000, bytes_accessed=send.size * 4, transcendentals=0
        ),
        name=f"to_rows_{rows}",
    )(send)


def project_kernel(x_ref, wq_ref, wkv_ref, bq_ref, bkv_ref, out_ref):
    rows = x_ref.shape[0]
    half = rows // 2
    step = 4
    for base in range(0, HEADS, step):
        cols = slice(base * LANES, (base + step) * LANES)
        both = (dot_nn(x_ref[...], wkv_ref[:, cols]) + bkv_ref[:, cols]).astype(low_type)
        for at in range(step):
            out_ref[base + at, 0:rows, :] = both[:, at * LANES : (at + 1) * LANES]
        cols = slice(base * HEAD_DIM, (base + step) * HEAD_DIM)
        query = ((dot_nn(x_ref[...], wq_ref[:, cols]) + bq_ref[:, cols]) * 0.125).astype(low_type)
        for at in range(step):
            lanes = slice(at * HEAD_DIM, (at + 1) * HEAD_DIM)
            out_ref[base + at, rows : rows + half, :] = jnp.concatenate(
                [query[:half, lanes], query[half:, lanes]], axis=1
            )


def project(x, wq, wkv, bq, bkv):
    rows = x.shape[0]
    vmem = pl.BlockSpec(memory_space=pltpu.VMEM)
    return pl.pallas_call(
        project_kernel,
        out_shape=jax.ShapeDtypeStruct((HEADS, rows + rows // 2, LANES), low_type),
        in_specs=[vmem] * 5,
        out_specs=vmem,
        compiler_params=pltpu.CompilerParams(vmem_limit_bytes=VMEM_BYTES),
        name="project",
    )(x, wq, wkv, bq, bkv)


def tile_range(meta_ref, first, last, total):
    end_a, end_b, end_c = meta_ref[0], meta_ref[1], meta_ref[2]
    low = jnp.where(
        first >= end_c, end_c, jnp.where(first >= end_b, end_b, jnp.where(first >= end_a, end_a, 0))
    )
    high = jnp.where(
        last >= end_c,
        total,
        jnp.where(last >= end_b, end_c, jnp.where(last >= end_a, end_b, end_a)),
    )
    return low // TILE, (high + TILE - 1) // TILE


def attend_kernel(meta_ref, order_ref, recv_ref, out_ref, qa_ref, ka_ref, va_ref, sum_ref):
    count = recv_ref.shape[0]
    half = recv_ref.shape[1] // 3
    total = qa_ref.shape[0]

    @pl.when(meta_ref[3] == 1)
    def _():
        lane = lax.broadcasted_iota(jnp.int32, (half, LANES), 1)
        lower = lane < HEAD_DIM
        row = lax.broadcasted_iota(jnp.int32, (half, LANES), 0)

        def place(source, _):
            query = recv_ref[source, 2 * half :, :].astype(jnp.float32)
            for part in range(2):
                first = pl.multiple_of(order_ref[2 * source + part] * half, half)
                position = first + row
                segment = (
                    (position >= meta_ref[0]).astype(jnp.int32)
                    + (position >= meta_ref[1]).astype(jnp.int32)
                    + (position >= meta_ref[2]).astype(jnp.int32)
                )
                mine = (lane - HEAD_DIM) == segment
                other = (lane < HEAD_DIM + 4) & (~mine)
                pair = recv_ref[source, part * half : (part + 1) * half, :].astype(jnp.float32)
                if part == 1:
                    query = pltpu.roll(query, HEAD_DIM, 1)
                mark_k = jnp.where(
                    other, FAR, jnp.where((lane >= HEAD_DIM + 4) & (lane < HEAD_DIM + 7), 1.0, 0.0)
                )
                rows = pl.ds(first, half)
                qa_ref[rows, :] = jnp.where(lower, query, jnp.where(mine, 1.0, 0.0)).astype(low_type)
                ka_ref[rows, :] = jnp.where(lower, pair, mark_k).astype(low_type)
                va_ref[rows, :] = jnp.where(lower, 1.0, pair).astype(low_type)
            return 0

        lax.fori_loop(0, count, place, 0)

        def query_step(index, _):
            first = pl.multiple_of(index * TILE, TILE)
            rows = pl.ds(first, TILE)
            begin, end = tile_range(meta_ref, first, first + TILE - 1, total)
            query = qa_ref[rows, :]
            sum_ref[rows, :] = jnp.zeros((TILE, LANES), jnp.float32)

            def key_step(key_index, _):
                keys = pl.ds(pl.multiple_of(key_index * TILE, TILE), TILE)
                expo = jnp.exp(dot_nt(query, ka_ref[keys, :])).astype(low_type)
                sum_ref[rows, :] += dot_nn(expo, va_ref[keys, :])
                return 0

            lax.fori_loop(begin, end, key_step, 0)
            return 0

        lax.fori_loop(0, total // TILE, query_step, 0)

        def give(source, _):
            parts = []
            for part in range(2):
                first = pl.multiple_of(order_ref[2 * source + part] * half, half)
                block = sum_ref[pl.ds(first, half), :]
                parts.append((block, pltpu.roll(block, HEAD_DIM, 1)))
            top = jnp.where(lower, parts[0][1], parts[1][0])
            bottom = jnp.where(lower, parts[0][0], parts[1][1])
            out_ref[source] = (top / bottom).astype(low_type)
            return 0

        lax.fori_loop(0, count, give, 0)


def attend(meta, order, recv):
    count, rows, _ = recv.shape
    total = count * rows * 2 // 3
    vmem = pl.BlockSpec(memory_space=pltpu.VMEM)
    smem = pl.BlockSpec(memory_space=pltpu.SMEM)
    whole = jax.ShapeDtypeStruct((total, LANES), low_type)
    return pl.pallas_call(
        attend_kernel,
        out_shape=(
            jax.ShapeDtypeStruct((count, rows // 3, LANES), low_type),
            whole,
            whole,
            whole,
            jax.ShapeDtypeStruct((total, LANES), jnp.float32),
        ),
        in_specs=[smem, smem, vmem],
        out_specs=(vmem,) * 5,
        compiler_params=pltpu.CompilerParams(vmem_limit_bytes=VMEM_BYTES),
        cost_estimate=pl.CostEstimate(
            flops=total * total * LANES * 8, bytes_accessed=total * LANES * 12, transcendentals=0
        ),
        name="attend",
    )(meta, order, recv)


def split_three(value):
    first = value.astype(low_type).astype(jnp.float32)
    rest = value - first
    second = rest.astype(low_type).astype(jnp.float32)
    return first, second, rest - second


def attend_back_kernel(
    meta_ref,
    order_ref,
    recv_ref,
    qa_ref,
    ka_ref,
    va_ref,
    sum_ref,
    out_ref,
    qb_ref,
    da_ref,
    kt_ref,
    dkv_ref,
    dq_ref,
    acc_ref,
):
    count = recv_ref.shape[0]
    half = recv_ref.shape[1]
    total = qa_ref.shape[0]

    @pl.when(meta_ref[3] == 1)
    def _():
        lane = lax.broadcasted_iota(jnp.int32, (half, LANES), 1)
        lower = lane < HEAD_DIM

        def place(source, _):
            given = recv_ref[source].astype(jnp.float32)
            for part in range(2):
                first = pl.multiple_of(order_ref[2 * source + part] * half, half)
                rows = pl.ds(first, half)
                block = sum_ref[rows, :]
                turned = pltpu.roll(block, HEAD_DIM, 1)
                d_context = pltpu.roll(given, HEAD_DIM, 1) if part == 0 else given
                product = jnp.where(lower, 0.0, d_context * (block / turned))
                minus = -jnp.sum(product, axis=1, keepdims=True)
                one, two, three = split_three(minus)
                mark = jnp.where(
                    lane == 0, one, jnp.where(lane == 1, two, jnp.where(lane == 2, three, 0.0))
                )
                da_ref[rows, :] = jnp.where(lower, mark, d_context).astype(low_type)
                one, two, three = split_three(-jnp.log(turned))
                at = lane - (HEAD_DIM + 4)
                mark = jnp.where(at == 0, one, jnp.where(at == 1, two, three))
                query = qa_ref[rows, :].astype(jnp.float32)
                qb_ref[rows, :] = jnp.where((at >= 0) & (at < 3), mark, query).astype(low_type)
            return 0

        lax.fori_loop(0, count, place, 0)

        def prepare(index, _):
            rows = pl.ds(pl.multiple_of(index * TILE, TILE), TILE)
            kt_ref[:, rows] = jnp.transpose(ka_ref[rows, :])[:HEAD_DIM, :]
            dkv_ref[rows, :] = jnp.zeros((TILE, LANES), jnp.float32)
            return 0

        lax.fori_loop(0, total // TILE, prepare, 0)

        lower_tile = lax.broadcasted_iota(jnp.int32, (TILE, LANES), 1) < HEAD_DIM

        def query_step(index, _):
            first = pl.multiple_of(index * TILE, TILE)
            rows = pl.ds(first, TILE)
            begin, end = tile_range(meta_ref, first, first + TILE - 1, total)
            query = qb_ref[rows, :]
            given = da_ref[rows, :]
            query_only = jnp.where(lower_tile, query.astype(jnp.float32), 0.0).astype(low_type)
            given_only = jnp.where(lower_tile, 0.0, given.astype(jnp.float32)).astype(low_type)
            acc_ref[...] = jnp.zeros_like(acc_ref)

            def key_step(key_index, _):
                keys = pl.ds(pl.multiple_of(key_index * TILE, TILE), TILE)
                prob = jnp.exp(dot_nt(ka_ref[keys, :], query))
                d_scores = (prob * dot_nt(va_ref[keys, :], given)).astype(low_type)
                dkv_ref[keys, :] += dot_nn(d_scores, query_only) + dot_nn(
                    prob.astype(low_type), given_only
                )
                acc_ref[...] += dot_nn(kt_ref[:, keys], d_scores)
                return 0

            lax.fori_loop(begin, end, key_step, 0)
            dq_ref[rows, :] = jnp.transpose(acc_ref[...])
            return 0

        lax.fori_loop(0, total // TILE, query_step, 0)

        def give(source, _):
            queries = []
            for part in range(2):
                first = pl.multiple_of(order_ref[2 * source + part] * half, half)
                rows = pl.ds(first, half)
                out_ref[source, part * half : (part + 1) * half, :] = dkv_ref[rows, :].astype(low_type)
                queries.append(dq_ref[rows, :])
            out_ref[source, 2 * half :, :] = jnp.concatenate(queries, axis=1).astype(low_type)
            return 0

        lax.fori_loop(0, count, give, 0)


def attend_back(meta, order, recv, qa, ka, va, sums):
    count, half, _ = recv.shape
    total = qa.shape[0]
    vmem = pl.BlockSpec(memory_space=pltpu.VMEM)
    smem = pl.BlockSpec(memory_space=pltpu.SMEM)
    return pl.pallas_call(
        attend_back_kernel,
        out_shape=jax.ShapeDtypeStruct((count, 3 * half, LANES), low_type),
        in_specs=[smem, smem] + [vmem] * 5,
        out_specs=vmem,
        scratch_shapes=[
            pltpu.VMEM((total, LANES), low_type),
            pltpu.VMEM((total, LANES), low_type),
            pltpu.VMEM((HEAD_DIM, total), low_type),
            pltpu.VMEM((total, LANES), jnp.float32),
            pltpu.VMEM((total, HEAD_DIM), jnp.float32),
            pltpu.VMEM((HEAD_DIM, TILE), jnp.float32),
        ],
        compiler_params=pltpu.CompilerParams(vmem_limit_bytes=VMEM_BYTES),
        cost_estimate=pl.CostEstimate(
            flops=total * total * LANES * 16, bytes_accessed=total * LANES * 16, transcendentals=0
        ),
        name="attend_back",
    )(meta, order, recv, qa, ka, va, sums)


PART_ORDERS = (("x", "z", "wa"), ("wa", "x", "z"), ("z", "wa", "x"))
GATHER_ORDERS = (("x", "z"), ("z", "x"), ("z", "x"))
SIZES = {"wa": 2, "x": 2, "z": 4}


class Links:
    def __init__(self):
        me = lax.axis_index("ctx")
        self.at = {
            "core": lax.rem(me, 2),
            "x": lax.rem(me // 2, 2),
            "z": me // 4,
            "wa": lax.axis_index("wa"),
        }

    def peer(self, axis, value):
        at = dict(self.at)
        at[axis] = value
        return {"ctx": at["z"] * 4 + at["x"] * 2 + at["core"], "wa": at["wa"]}


def splits_rows(piece):
    return piece % 64 == 0


def grad_sum_kernel(*refs):
    g_refs, out_refs, core_bufs, bufs = refs[:3], refs[3:6], refs[6:9], refs[9:18]
    send_sem, recv_sem = refs[18:]
    links = Links()
    core, x, z, wa = (links.at[name] for name in ("core", "x", "z", "wa"))
    barrier = pltpu.get_barrier_semaphore()
    peers = [links.peer("core", 1 - core), links.peer("x", 1 - x), links.peer("wa", 1 - wa)]
    peers += [links.peer("z", lax.rem(z + step, 4)) for step in range(1, 4)]
    for peer in peers:
        pl.semaphore_signal(barrier, inc=1, device_id=peer, device_id_type=pl.DeviceIdType.MESH)
    pl.semaphore_wait(barrier, len(peers))
    used = [0]

    def remote(src, dst, peer):
        index = used[0]
        used[0] += 1
        copy = pltpu.make_async_remote_copy(
            src_ref=src,
            dst_ref=dst,
            send_sem=send_sem.at[index],
            recv_sem=recv_sem.at[index],
            device_id=peer,
            device_id_type=pl.DeviceIdType.MESH,
        )
        copy.start()
        return copy

    def z_share(ref, value):
        piece, width = ref.shape[-2:]
        if value is None:
            return slice(None), slice(None)
        if splits_rows(piece):
            return pl.ds(pl.multiple_of(value * (piece // 4), 16), piece // 4), slice(None)
        return slice(None), pl.ds(pl.multiple_of(value * (width // 4), LANES), width // 4)

    def slab(part, held, axis=None, value=None):
        at = dict(links.at)
        if axis is not None:
            at[axis] = value
            held = held | {axis}
        return g_refs[part].at[
            pl.ds(at["wa"], 1) if "wa" in held else pl.ds(0, 2),
            core,
            pl.ds(at["x"], 1) if "x" in held else pl.ds(0, 2),
            *z_share(g_refs[part], at["z"] if "z" in held else None),
        ]

    def add_into(target, sources):
        outer, inner, rows, _ = target.shape
        for a in range(outer):
            for b in range(inner):

                def add(group, _):
                    some = pl.ds(pl.multiple_of(group * 16, 16), 16)
                    total = target[a, b, some, :].astype(jnp.float32)
                    for source in sources:
                        total = total + source[a, b, some, :].astype(jnp.float32)
                    target[a, b, some, :] = total.astype(low_type)
                    return 0

                lax.fori_loop(0, rows // 16, add, 0)

    core_copies = [
        remote(g_refs[part].at[:, 1 - core], core_bufs[part], links.peer("core", 1 - core))
        for part in range(3)
    ]

    def begin(part, stage):
        axis = PART_ORDERS[part][stage]
        held = set(PART_ORDERS[part][:stage])
        buf = bufs[part * 3 + stage]
        copies = []
        for step in range(1, SIZES[axis]):
            value = lax.rem(links.at[axis] + step, SIZES[axis])
            copies.append(
                remote(slab(part, held, axis, value), buf.at[step - 1], links.peer(axis, value))
            )
        return copies

    flying = {}
    for part in range(3):
        core_copies[part].wait()
        add_into(slab(part, set()), [core_bufs[part]])
        flying[part] = begin(part, 0)
    for stage in range(3):
        for part in range(3):
            axis = PART_ORDERS[part][stage]
            for copy in flying[part]:
                copy.wait()
            buf = bufs[part * 3 + stage]
            add_into(
                slab(part, set(PART_ORDERS[part][: stage + 1])),
                [buf.at[step] for step in range(SIZES[axis] - 1)],
            )
            if stage < 2:
                flying[part] = begin(part, stage + 1)

    def out_slab(part, held):
        return out_refs[part].at[
            core,
            pl.ds(x, 1) if "x" in held else pl.ds(0, 2),
            *z_share(out_refs[part], z if "z" in held else None),
        ]

    def spread(part, stage):
        axis = GATHER_ORDERS[part][stage]
        block = out_slab(part, set(GATHER_ORDERS[part][stage:]))
        return [
            remote(block, block, links.peer(axis, lax.rem(links.at[axis] + step, SIZES[axis])))
            for step in range(1, SIZES[axis])
        ]

    for part in range(3):
        out_slab(part, {"x", "z"})[...] = slab(part, {"wa", "x", "z"})[0]
        flying[part] = spread(part, 0)
    for stage in range(2):
        for part in range(3):
            for copy in flying[part]:
                copy.wait()
            if stage == 0:
                flying[part] = spread(part, 1)
            else:
                block = out_slab(part, set())
                flying[part] = [remote(block, block, links.peer("core", 1 - core))]
    for part in range(3):
        for copy in flying[part]:
            copy.wait()


def grad_sum(grads, collective_id):
    bufs, core_bufs, outs, given = [], [], [], []
    for part, grad in enumerate(grads):
        rows, width = grad.shape
        piece = rows // 8
        shape = {"wa": 2, "x": 2, "z": 4}
        for axis in PART_ORDERS[part]:
            shape[axis] //= SIZES[axis]
            share = (
                (piece * shape["z"] // 4, width)
                if splits_rows(piece)
                else (piece, width * shape["z"] // 4)
            )
            bufs.append(
                pltpu.VMEM((SIZES[axis] - 1, shape["wa"], shape["x"], *share), low_type)
            )
        core_bufs.append(pltpu.VMEM((2, 2, piece, width), low_type))
        outs.append(jax.ShapeDtypeStruct((2, 2, piece, width), low_type))
        given.append(grad.reshape(2, 2, 2, piece, width))
    vmem = pl.BlockSpec(memory_space=pltpu.VMEM)
    size = sum(grad.size for grad in grads)
    sums = pl.pallas_call(
        grad_sum_kernel,
        out_shape=tuple(outs),
        in_specs=[vmem] * 3,
        out_specs=(vmem,) * 3,
        scratch_shapes=[
            *core_bufs,
            *bufs,
            pltpu.SemaphoreType.DMA((40,)),
            pltpu.SemaphoreType.DMA((40,)),
        ],
        compiler_params=pltpu.CompilerParams(
            collective_id=collective_id, has_side_effects=True, vmem_limit_bytes=VMEM_BYTES
        ),
        cost_estimate=pl.CostEstimate(
            flops=size * 20_000, bytes_accessed=size * 4, transcendentals=0
        ),
        name="grad_sum",
    )(*given)
    return [part.reshape(-1, part.shape[-1]) for part in sums]


def pack_columns(vectors, rows):
    columns = jnp.stack([vec.astype(low_type) for vec in vectors], axis=1)
    return jnp.pad(columns, ((0, 0), (0, LANES - len(vectors))))


def column_sums(terms, lanes):
    block = jnp.stack([jnp.sum(term, axis=0) for term in terms], axis=1).astype(low_type)
    return jnp.pad(block, ((0, 0), (0, lanes - len(terms))))


def rows_of_columns(block, wanted):
    pick = jnp.eye(LANES, 8, dtype=low_type)
    return jnp.einsum("fk,kj->jf", block, pick, preferred_element_type=jnp.float32)[:wanted]


def reduce_shards(grad):
    part = lax.psum_scatter(
        grad.astype(low_type), ("wa", "ctx"), scatter_dimension=0, tiled=True
    )
    return lax.all_gather(part, "ctx", axis=0, tiled=True)


def body(
    count,
    tokens,
    cotangent,
    lengths,
    block_order,
    w_query,
    b_query,
    w_key,
    w_value,
    b_value,
    w_out,
    b_out,
    gain_one,
    shift_one,
    w_up,
    b_up,
    w_down,
    b_down,
    gain_two,
    shift_two,
):
    inputs = tokens[0]
    tok_rows, width = inputs.shape
    wide = w_up.shape[1]
    half = tok_rows // 2
    shard = w_query.shape[0]
    direct = count == 16 and width == 2 * shard and shard % 64 == 0 and wide == 4 * width
    me = lax.axis_index("ctx")
    seq_ends = jnp.cumsum(lengths[0])
    own_blocks = lax.dynamic_slice(block_order, (2 * me,), (2,))
    position = (own_blocks[:, None] * half + jnp.arange(half, dtype=jnp.int32)[None, :]).reshape(-1)
    own_seg = segment_of(position, seq_ends)
    owns = jnp.any(me == jnp.arange(HEADS, dtype=jnp.int32) * count // HEADS).astype(jnp.int32)
    meta = jnp.concatenate([seq_ends.astype(jnp.int32), owns[None]])

    core = me % 2
    wa = lax.axis_index("wa")

    def fetch_half(shard_block, after=None):
        if not direct:
            return None
        if after is not None:
            shard_block, _ = lax.optimization_barrier((shard_block, after))
        size, columns = shard_block.shape
        part = lax.dynamic_slice(shard_block, (core * (size // 2), 0), (size // 2, columns))
        return lax.ppermute(part, "wa", [(0, 1), (1, 0)])

    def gather_rows(shard_block, fetched):
        if not direct:
            return lax.all_gather(shard_block, "wa", axis=0, tiled=True)
        size, columns = shard_block.shape
        swapped = lax.ppermute(fetched, "ctx", [(k, k ^ 1) for k in range(count)])
        other = (1 - wa) * size
        whole = jnp.zeros((2 * size, columns), shard_block.dtype)
        whole = lax.dynamic_update_slice(whole, shard_block, (wa * size, 0))
        whole = lax.dynamic_update_slice(whole, fetched, (other + core * (size // 2), 0))
        return lax.dynamic_update_slice(whole, swapped, (other + (1 - core) * (size // 2), 0))

    pair = jnp.stack(
        [
            w_key.astype(low_type).reshape(shard, HEADS, HEAD_DIM),
            w_value.astype(low_type).reshape(shard, HEADS, HEAD_DIM),
        ],
        axis=2,
    ).reshape(shard, 2 * width)
    vectors = pack_columns(
        [b_query, b_value, b_out, gain_one, shift_one, gain_two, shift_two, b_down], shard
    )
    first_shard = jnp.concatenate([w_query.astype(low_type), pair, vectors], axis=1)
    fetched = fetch_half(first_shard)
    later_shards = (
        w_out.astype(low_type),
        w_up.astype(low_type),
        jnp.concatenate([w_down.astype(low_type), pack_columns([b_up], 4 * shard)], axis=1),
    )
    later_fetched = tuple(fetch_half(block, fetched) for block in later_shards)
    first_pack = gather_rows(first_shard, fetched)
    query_weight = first_pack[:, :width]
    pair_weight = first_pack[:, width : 3 * width]
    vector_rows = rows_of_columns(first_pack[:, 3 * width :], 8)
    query_bias, value_bias, out_bias, gain_first, shift_first, gain_second, shift_second, down_bias = (
        vector_rows[index] for index in range(8)
    )
    pair_bias = jnp.stack(
        [jnp.zeros((HEADS, HEAD_DIM), jnp.float32), value_bias.reshape(HEADS, HEAD_DIM)], axis=1
    ).reshape(1, 2 * width)

    packed = project(inputs, query_weight, pair_weight, query_bias[None, :], pair_bias)
    at_head = to_heads(packed, count, 0)
    context_out, qa, ka, va, sums = attend(meta, block_order, at_head)
    context_out, later_fetched = lax.optimization_barrier((context_out, later_fetched))
    out_weight, up_weight, down_pack = (
        gather_rows(block, half_block) for block, half_block in zip(later_shards, later_fetched)
    )
    down_weight = down_pack[:, :width]
    up_bias = rows_of_columns(down_pack[:, width:], 1)[0]
    context_in = to_rows(context_out, count, 1)
    context_low = (
        context_in.reshape(HEADS, half, 2, HEAD_DIM).transpose(2, 1, 0, 3).reshape(tok_rows, width)
    )

    attn_out = jnp.dot(context_low, out_weight, preferred_element_type=jnp.float32) + out_bias
    h_one = inputs.astype(jnp.float32) + attn_out
    norm_one, norm_one_back = jax.vjp(layer_norm, h_one, gain_first, shift_first)
    norm_low = norm_one.astype(low_type)
    up_pre = jnp.dot(norm_low, up_weight, preferred_element_type=jnp.float32) + up_bias
    gelu_out, gelu_back = jax.vjp(partial(jax.nn.gelu, approximate=False), up_pre)
    gelu_low = gelu_out.astype(low_type)
    down_out = jnp.dot(gelu_low, down_weight, preferred_element_type=jnp.float32) + down_bias
    h_two = norm_one + down_out
    result, norm_two_back = jax.vjp(layer_norm, h_two, gain_second, shift_second)
    activations = result.astype(low_type)[None]
    valid = (own_seg < 3).astype(jnp.float32)
    g_out = cotangent[0].astype(jnp.float32) * valid[:, None]
    d_htwo, grad_gain_second, grad_shift_second = norm_two_back(g_out)
    d_down = d_htwo.astype(low_type)
    d_gelu = jnp.einsum("td,fd->tf", d_down, down_weight, preferred_element_type=jnp.float32)
    (d_uppre,) = gelu_back(d_gelu)
    d_up = d_uppre.astype(low_type)
    d_yone = d_htwo + jnp.einsum("tf,df->td", d_up, up_weight, preferred_element_type=jnp.float32)
    d_hone, grad_gain_first, grad_shift_first = norm_one_back(d_yone)
    d_attn = d_hone.astype(low_type)
    d_context = jnp.einsum("td,cd->tc", d_attn, out_weight, preferred_element_type=jnp.float32)
    context_back = (
        d_context.astype(low_type)
        .reshape(2, half, HEADS, HEAD_DIM)
        .transpose(2, 1, 0, 3)
        .reshape(HEADS, half, LANES)
    )

    grad_wdown = jnp.einsum("tf,td->fd", gelu_low, d_down, preferred_element_type=jnp.float32)
    grad_wup = jnp.einsum("td,tf->df", norm_low, d_up, preferred_element_type=jnp.float32)
    grad_wout = jnp.einsum("tc,td->cd", context_low, d_attn, preferred_element_type=jnp.float32)
    up_bias_sums = jnp.sum(d_up.astype(jnp.float32), axis=0)
    lanes = 2 * LANES
    vec_block = jnp.concatenate(
        [
            jnp.stack(
                [
                    jnp.sum(d_attn.astype(jnp.float32), axis=0),
                    grad_gain_first,
                    grad_shift_first,
                    jnp.sum(d_down.astype(jnp.float32), axis=0),
                    grad_gain_second,
                    grad_shift_second,
                ],
                axis=1,
            ),
            up_bias_sums.reshape(width // shard, 4, shard).transpose(0, 2, 1).reshape(width, 4),
        ],
        axis=1,
    ).astype(low_type)
    out_block = jnp.concatenate(
        [grad_wout.astype(low_type), jnp.pad(vec_block, ((0, 0), (0, lanes - 10)))], axis=1
    )
    up_block = grad_wup.astype(low_type)
    down_block = grad_wdown.astype(low_type)
    context_back, down_block, out_block, up_block = lax.optimization_barrier(
        (context_back, down_block, out_block, up_block)
    )
    up_sum = reduce_shards(up_block)

    back_at_head = to_heads(context_back, count, 2)
    grads_out = attend_back(meta, block_order, back_at_head, qa, ka, va, sums)
    grads_in = to_rows(grads_out, count, 3)

    d_pair = grads_in[:, :tok_rows, :].transpose(1, 0, 2).reshape(tok_rows, 2 * width)
    d_queries = (
        grads_in[:, tok_rows:, :]
        .reshape(HEADS, half, 2, HEAD_DIM)
        .transpose(2, 1, 0, 3)
        .reshape(tok_rows, width)
        * jnp.asarray(0.125, low_type)
    )
    d_all = jnp.concatenate([d_queries, d_pair], axis=1)
    grad_all = jnp.einsum("tc,td->cd", inputs, d_all, preferred_element_type=jnp.float32)
    d_values = d_pair.reshape(tok_rows, HEADS, 2, HEAD_DIM)[:, :, 1, :].reshape(tok_rows, width)
    last_block = jnp.concatenate(
        [
            grad_all.astype(low_type),
            column_sums([d_queries.astype(jnp.float32), d_values.astype(jnp.float32)], lanes),
        ],
        axis=1,
    )
    if direct:
        down_sum, last_sum, out_sum = grad_sum((down_block, last_block, out_block), 4)
    else:
        down_sum, last_sum, out_sum = (
            reduce_shards(block) for block in (down_block, last_block, out_block)
        )
    d_input = (
        d_hone
        + jnp.einsum("td,cd->tc", d_queries, query_weight, preferred_element_type=jnp.float32)
        + jnp.einsum("td,cd->tc", d_pair, pair_weight, preferred_element_type=jnp.float32)
    )
    input_grad = d_input.astype(low_type)[None]

    wide_grad = last_sum.astype(jnp.float32)
    pair_grad = wide_grad[:, width : 3 * width].reshape(shard, HEADS, 2, HEAD_DIM)
    out_grad = out_sum.astype(jnp.float32)
    return (
        activations,
        input_grad,
        wide_grad[:, :width],
        wide_grad[:, 3 * width],
        pair_grad[:, :, 0, :].reshape(shard, width),
        pair_grad[:, :, 1, :].reshape(shard, width),
        wide_grad[:, 3 * width + 1],
        out_grad[:, :width],
        out_grad[:, width],
        out_grad[:, width + 1],
        out_grad[:, width + 2],
        up_sum.astype(jnp.float32),
        out_grad[:, width + 6 : width + 10].T.reshape(-1),
        down_sum.astype(jnp.float32),
        out_grad[:, width + 3],
        out_grad[:, width + 4],
        out_grad[:, width + 5],
    )


def solution(mesh):
    placed = (
        P("wa", "ctx", None),
        P("wa", "ctx", None),
        P("wa", None),
        P(),
        P("wa", None),
        P("wa"),
        P("wa", None),
        P("wa", None),
        P("wa"),
        P("wa", None),
        P("wa"),
        P("wa"),
        P("wa"),
        P("wa", None),
        P("wa"),
        P("wa", None),
        P("wa"),
        P("wa"),
        P("wa"),
    )
    return jax.shard_map(
        partial(body, mesh.shape["ctx"]),
        mesh=mesh,
        in_specs=placed,
        out_specs=(
            P("wa", "ctx", None),
            P("wa", "ctx", None),
            P("wa", None),
            P("wa"),
            P("wa", None),
            P("wa", None),
            P("wa"),
            P("wa", None),
            P("wa"),
            P("wa"),
            P("wa"),
            P("wa", None),
            P("wa"),
            P("wa", None),
            P("wa"),
            P("wa"),
            P("wa"),
        ),
        check_vma=False,
    )
```

```python
from functools import partial

import jax
import jax.numpy as jnp
from jax import lax
from jax.experimental import pallas as pl
from jax.experimental.pallas import tpu as pltpu
from jax.sharding import PartitionSpec as P

HEADS = 12
HEAD_DIM = 64
LANES = 128
TILE = 512
FAR = -(2.0**40)
VMEM_BYTES = 60 << 20

low_type = jnp.bfloat16
epsilon = 1e-05


def dot_nt(left, right):
    return lax.dot_general(
        left, right, (((1,), (1,)), ((), ())), preferred_element_type=jnp.float32
    )


def dot_nn(left, right):
    return lax.dot_general(
        left, right, (((1,), (0,)), ((), ())), preferred_element_type=jnp.float32
    )


def layer_norm(hidden, gain_vec, shift_vec):
    centre = hidden - jnp.mean(hidden, axis=-1, keepdims=True)
    spread = jnp.mean(centre * centre, axis=-1, keepdims=True)
    return centre * lax.rsqrt(spread + epsilon) * gain_vec + shift_vec


def segment_of(position, seq_ends):
    return jnp.sum((position[:, None] >= seq_ends[None, :]).astype(jnp.int32), axis=1)


def owner_of(head, count):
    return head * count // HEADS


def greet_all(count, me):
    barrier = pltpu.get_barrier_semaphore()

    def greet(step, _):
        other = lax.rem(me + step, count)
        pl.semaphore_signal(
            barrier, inc=1, device_id={"ctx": other}, device_id_type=pl.DeviceIdType.MESH
        )
        return 0

    lax.fori_loop(1, count, greet, 0)
    pl.semaphore_wait(barrier, count - 1)


def to_heads_kernel(count, send_ref, recv_ref, send_sem, recv_sem, own_sem):
    me = lax.axis_index("ctx")
    greet_all(count, me)
    first = me * HEADS // count + 1

    def copy_for(head, source, owner):
        return pltpu.make_async_remote_copy(
            src_ref=send_ref.at[head],
            dst_ref=recv_ref.at[source],
            send_sem=send_sem.at[head],
            recv_sem=recv_sem.at[source],
            device_id={"ctx": owner},
            device_id_type=pl.DeviceIdType.MESH,
        )

    def own_copy(head):
        return pltpu.make_async_copy(send_ref.at[head], recv_ref.at[me], own_sem)

    def begin(step, _):
        head = lax.rem(first + step, HEADS)
        owner = owner_of(head, count)

        @pl.when(owner != me)
        def _():
            copy_for(head, me, owner).start()

        @pl.when(owner == me)
        def _():
            own_copy(head).start()

        return 0

    lax.fori_loop(0, HEADS, begin, 0)

    def finish(head, _):
        owner = owner_of(head, count)

        @pl.when(owner != me)
        def _():
            copy_for(head, me, owner).wait_send()

        @pl.when(owner == me)
        def _():
            own_copy(head).wait()

            def arrive(source, _):
                @pl.when(source != me)
                def _():
                    copy_for(head, source, owner).wait_recv()

                return 0

            lax.fori_loop(0, count, arrive, 0)

        return 0

    lax.fori_loop(0, HEADS, finish, 0)


def to_heads(send, count, collective_id):
    rows = send.shape[1]
    return pl.pallas_call(
        partial(to_heads_kernel, count),
        out_shape=jax.ShapeDtypeStruct((count, rows, LANES), low_type),
        in_specs=[pl.BlockSpec(memory_space=pltpu.VMEM)],
        out_specs=pl.BlockSpec(memory_space=pltpu.VMEM),
        scratch_shapes=[
            pltpu.SemaphoreType.DMA((HEADS,)),
            pltpu.SemaphoreType.DMA((count,)),
            pltpu.SemaphoreType.DMA,
        ],
        compiler_params=pltpu.CompilerParams(
            collective_id=collective_id, has_side_effects=True, vmem_limit_bytes=VMEM_BYTES
        ),
        cost_estimate=pl.CostEstimate(
            flops=rows * 250_000_000, bytes_accessed=send.size * 4, transcendentals=0
        ),
        name=f"to_heads_{rows}",
    )(send)


def to_rows_kernel(count, send_ref, recv_ref, send_sem, recv_sem, own_sem):
    me = lax.axis_index("ctx")
    greet_all(count, me)

    def copy_for(head, target):
        return pltpu.make_async_remote_copy(
            src_ref=send_ref.at[target],
            dst_ref=recv_ref.at[head],
            send_sem=send_sem.at[target],
            recv_sem=recv_sem.at[head],
            device_id={"ctx": target},
            device_id_type=pl.DeviceIdType.MESH,
        )

    def own_copy(head):
        return pltpu.make_async_copy(send_ref.at[me], recv_ref.at[head], own_sem)

    def begin(head, _):
        @pl.when(owner_of(head, count) == me)
        def _():
            own_copy(head).start()

            def push(step, _):
                copy_for(head, lax.rem(me + step, count)).start()
                return 0

            lax.fori_loop(1, count, push, 0)

        return 0

    lax.fori_loop(0, HEADS, begin, 0)

    def finish(head, _):
        @pl.when(owner_of(head, count) == me)
        def _():
            own_copy(head).wait()

            def leave(step, _):
                copy_for(head, lax.rem(me + step, count)).wait_send()
                return 0

            lax.fori_loop(1, count, leave, 0)

        @pl.when(owner_of(head, count) != me)
        def _():
            copy_for(head, me).wait_recv()

        return 0

    lax.fori_loop(0, HEADS, finish, 0)


def to_rows(send, count, collective_id):
    rows = send.shape[1]
    return pl.pallas_call(
        partial(to_rows_kernel, count),
        out_shape=jax.ShapeDtypeStruct((HEADS, rows, LANES), low_type),
        in_specs=[pl.BlockSpec(memory_space=pltpu.VMEM)],
        out_specs=pl.BlockSpec(memory_space=pltpu.VMEM),
        scratch_shapes=[
            pltpu.SemaphoreType.DMA((count,)),
            pltpu.SemaphoreType.DMA((HEADS,)),
            pltpu.SemaphoreType.DMA,
        ],
        compiler_params=pltpu.CompilerParams(
            collective_id=collective_id, has_side_effects=True, vmem_limit_bytes=VMEM_BYTES
        ),
        cost_estimate=pl.CostEstimate(
            flops=rows * 250_000_000, bytes_accessed=send.size * 4, transcendentals=0
        ),
        name=f"to_rows_{rows}",
    )(send)


def project_kernel(x_ref, wq_ref, wkv_ref, bq_ref, bkv_ref, out_ref):
    rows = x_ref.shape[0]
    half = rows // 2
    step = 4
    for base in range(0, HEADS, step):
        cols = slice(base * LANES, (base + step) * LANES)
        both = (dot_nn(x_ref[...], wkv_ref[:, cols]) + bkv_ref[:, cols]).astype(low_type)
        for at in range(step):
            out_ref[base + at, 0:rows, :] = both[:, at * LANES : (at + 1) * LANES]
        cols = slice(base * HEAD_DIM, (base + step) * HEAD_DIM)
        query = ((dot_nn(x_ref[...], wq_ref[:, cols]) + bq_ref[:, cols]) * 0.125).astype(low_type)
        for at in range(step):
            lanes = slice(at * HEAD_DIM, (at + 1) * HEAD_DIM)
            out_ref[base + at, rows : rows + half, :] = jnp.concatenate(
                [query[:half, lanes], query[half:, lanes]], axis=1
            )


def project(x, wq, wkv, bq, bkv):
    rows = x.shape[0]
    vmem = pl.BlockSpec(memory_space=pltpu.VMEM)
    return pl.pallas_call(
        project_kernel,
        out_shape=jax.ShapeDtypeStruct((HEADS, rows + rows // 2, LANES), low_type),
        in_specs=[vmem] * 5,
        out_specs=vmem,
        compiler_params=pltpu.CompilerParams(vmem_limit_bytes=VMEM_BYTES),
        name="project",
    )(x, wq, wkv, bq, bkv)


def tile_range(meta_ref, first, last, total):
    end_a, end_b, end_c = meta_ref[0], meta_ref[1], meta_ref[2]
    low = jnp.where(
        first >= end_c, end_c, jnp.where(first >= end_b, end_b, jnp.where(first >= end_a, end_a, 0))
    )
    high = jnp.where(
        last >= end_c,
        total,
        jnp.where(last >= end_b, end_c, jnp.where(last >= end_a, end_b, end_a)),
    )
    return low // TILE, (high + TILE - 1) // TILE


def attend_kernel(meta_ref, order_ref, recv_ref, out_ref, qa_ref, ka_ref, va_ref, sum_ref):
    count = recv_ref.shape[0]
    half = recv_ref.shape[1] // 3
    total = qa_ref.shape[0]

    @pl.when(meta_ref[3] == 1)
    def _():
        lane = lax.broadcasted_iota(jnp.int32, (half, LANES), 1)
        lower = lane < HEAD_DIM
        row = lax.broadcasted_iota(jnp.int32, (half, LANES), 0)

        def place(source, _):
            query = recv_ref[source, 2 * half :, :].astype(jnp.float32)
            for part in range(2):
                first = pl.multiple_of(order_ref[2 * source + part] * half, half)
                position = first + row
                segment = (
                    (position >= meta_ref[0]).astype(jnp.int32)
                    + (position >= meta_ref[1]).astype(jnp.int32)
                    + (position >= meta_ref[2]).astype(jnp.int32)
                )
                mine = (lane - HEAD_DIM) == segment
                other = (lane < HEAD_DIM + 4) & (~mine)
                pair = recv_ref[source, part * half : (part + 1) * half, :].astype(jnp.float32)
                if part == 1:
                    query = pltpu.roll(query, HEAD_DIM, 1)
                mark_k = jnp.where(
                    other, FAR, jnp.where((lane >= HEAD_DIM + 4) & (lane < HEAD_DIM + 7), 1.0, 0.0)
                )
                rows = pl.ds(first, half)
                qa_ref[rows, :] = jnp.where(lower, query, jnp.where(mine, 1.0, 0.0)).astype(low_type)
                ka_ref[rows, :] = jnp.where(lower, pair, mark_k).astype(low_type)
                va_ref[rows, :] = jnp.where(lower, 1.0, pair).astype(low_type)
            return 0

        lax.fori_loop(0, count, place, 0)

        def query_step(index, _):
            first = pl.multiple_of(index * TILE, TILE)
            rows = pl.ds(first, TILE)
            begin, end = tile_range(meta_ref, first, first + TILE - 1, total)
            query = qa_ref[rows, :]
            sum_ref[rows, :] = jnp.zeros((TILE, LANES), jnp.float32)

            def key_step(key_index, _):
                keys = pl.ds(pl.multiple_of(key_index * TILE, TILE), TILE)
                expo = jnp.exp(dot_nt(query, ka_ref[keys, :])).astype(low_type)
                sum_ref[rows, :] += dot_nn(expo, va_ref[keys, :])
                return 0

            lax.fori_loop(begin, end, key_step, 0)
            return 0

        lax.fori_loop(0, total // TILE, query_step, 0)

        def give(source, _):
            parts = []
            for part in range(2):
                first = pl.multiple_of(order_ref[2 * source + part] * half, half)
                block = sum_ref[pl.ds(first, half), :]
                parts.append((block, pltpu.roll(block, HEAD_DIM, 1)))
            top = jnp.where(lower, parts[0][1], parts[1][0])
            bottom = jnp.where(lower, parts[0][0], parts[1][1])
            out_ref[source] = (top / bottom).astype(low_type)
            return 0

        lax.fori_loop(0, count, give, 0)


def attend(meta, order, recv):
    count, rows, _ = recv.shape
    total = count * rows * 2 // 3
    vmem = pl.BlockSpec(memory_space=pltpu.VMEM)
    smem = pl.BlockSpec(memory_space=pltpu.SMEM)
    whole = jax.ShapeDtypeStruct((total, LANES), low_type)
    return pl.pallas_call(
        attend_kernel,
        out_shape=(
            jax.ShapeDtypeStruct((count, rows // 3, LANES), low_type),
            whole,
            whole,
            whole,
            jax.ShapeDtypeStruct((total, LANES), jnp.float32),
        ),
        in_specs=[smem, smem, vmem],
        out_specs=(vmem,) * 5,
        compiler_params=pltpu.CompilerParams(vmem_limit_bytes=VMEM_BYTES),
        cost_estimate=pl.CostEstimate(
            flops=total * total * LANES * 8, bytes_accessed=total * LANES * 12, transcendentals=0
        ),
        name="attend",
    )(meta, order, recv)


def split_three(value):
    first = value.astype(low_type).astype(jnp.float32)
    rest = value - first
    second = rest.astype(low_type).astype(jnp.float32)
    return first, second, rest - second


def attend_back_kernel(
    meta_ref,
    order_ref,
    recv_ref,
    qa_ref,
    ka_ref,
    va_ref,
    sum_ref,
    out_ref,
    qb_ref,
    da_ref,
    kt_ref,
    dkv_ref,
    dq_ref,
    acc_ref,
):
    count = recv_ref.shape[0]
    half = recv_ref.shape[1]
    total = qa_ref.shape[0]

    @pl.when(meta_ref[3] == 1)
    def _():
        lane = lax.broadcasted_iota(jnp.int32, (half, LANES), 1)
        lower = lane < HEAD_DIM

        def place(source, _):
            given = recv_ref[source].astype(jnp.float32)
            for part in range(2):
                first = pl.multiple_of(order_ref[2 * source + part] * half, half)
                rows = pl.ds(first, half)
                block = sum_ref[rows, :]
                turned = pltpu.roll(block, HEAD_DIM, 1)
                d_context = pltpu.roll(given, HEAD_DIM, 1) if part == 0 else given
                product = jnp.where(lower, 0.0, d_context * (block / turned))
                minus = -jnp.sum(product, axis=1, keepdims=True)
                one, two, three = split_three(minus)
                mark = jnp.where(
                    lane == 0, one, jnp.where(lane == 1, two, jnp.where(lane == 2, three, 0.0))
                )
                da_ref[rows, :] = jnp.where(lower, mark, d_context).astype(low_type)
                one, two, three = split_three(-jnp.log(turned))
                at = lane - (HEAD_DIM + 4)
                mark = jnp.where(at == 0, one, jnp.where(at == 1, two, three))
                query = qa_ref[rows, :].astype(jnp.float32)
                qb_ref[rows, :] = jnp.where((at >= 0) & (at < 3), mark, query).astype(low_type)
            return 0

        lax.fori_loop(0, count, place, 0)

        def prepare(index, _):
            rows = pl.ds(pl.multiple_of(index * TILE, TILE), TILE)
            kt_ref[:, rows] = jnp.transpose(ka_ref[rows, :])[:HEAD_DIM, :]
            dkv_ref[rows, :] = jnp.zeros((TILE, LANES), jnp.float32)
            return 0

        lax.fori_loop(0, total // TILE, prepare, 0)

        lower_tile = lax.broadcasted_iota(jnp.int32, (TILE, LANES), 1) < HEAD_DIM

        def query_step(index, _):
            first = pl.multiple_of(index * TILE, TILE)
            rows = pl.ds(first, TILE)
            begin, end = tile_range(meta_ref, first, first + TILE - 1, total)
            query = qb_ref[rows, :]
            given = da_ref[rows, :]
            query_only = jnp.where(lower_tile, query.astype(jnp.float32), 0.0).astype(low_type)
            given_only = jnp.where(lower_tile, 0.0, given.astype(jnp.float32)).astype(low_type)
            acc_ref[...] = jnp.zeros_like(acc_ref)

            def key_step(key_index, _):
                keys = pl.ds(pl.multiple_of(key_index * TILE, TILE), TILE)
                prob = jnp.exp(dot_nt(ka_ref[keys, :], query))
                d_scores = (prob * dot_nt(va_ref[keys, :], given)).astype(low_type)
                dkv_ref[keys, :] += dot_nn(d_scores, query_only) + dot_nn(
                    prob.astype(low_type), given_only
                )
                acc_ref[...] += dot_nn(kt_ref[:, keys], d_scores)
                return 0

            lax.fori_loop(begin, end, key_step, 0)
            dq_ref[rows, :] = jnp.transpose(acc_ref[...])
            return 0

        lax.fori_loop(0, total // TILE, query_step, 0)

        def give(source, _):
            queries = []
            for part in range(2):
                first = pl.multiple_of(order_ref[2 * source + part] * half, half)
                rows = pl.ds(first, half)
                out_ref[source, part * half : (part + 1) * half, :] = dkv_ref[rows, :].astype(low_type)
                queries.append(dq_ref[rows, :])
            out_ref[source, 2 * half :, :] = jnp.concatenate(queries, axis=1).astype(low_type)
            return 0

        lax.fori_loop(0, count, give, 0)


def attend_back(meta, order, recv, qa, ka, va, sums):
    count, half, _ = recv.shape
    total = qa.shape[0]
    vmem = pl.BlockSpec(memory_space=pltpu.VMEM)
    smem = pl.BlockSpec(memory_space=pltpu.SMEM)
    return pl.pallas_call(
        attend_back_kernel,
        out_shape=jax.ShapeDtypeStruct((count, 3 * half, LANES), low_type),
        in_specs=[smem, smem] + [vmem] * 5,
        out_specs=vmem,
        scratch_shapes=[
            pltpu.VMEM((total, LANES), low_type),
            pltpu.VMEM((total, LANES), low_type),
            pltpu.VMEM((HEAD_DIM, total), low_type),
            pltpu.VMEM((total, LANES), jnp.float32),
            pltpu.VMEM((total, HEAD_DIM), jnp.float32),
            pltpu.VMEM((HEAD_DIM, TILE), jnp.float32),
        ],
        compiler_params=pltpu.CompilerParams(vmem_limit_bytes=VMEM_BYTES),
        cost_estimate=pl.CostEstimate(
            flops=total * total * LANES * 16, bytes_accessed=total * LANES * 16, transcendentals=0
        ),
        name="attend_back",
    )(meta, order, recv, qa, ka, va, sums)


PART_ORDERS = (("x", "z"), ("z", "x"), ("wa", "x", "z"), ("z", "wa", "x"))
GATHER_ORDERS = (("z", "x"), ("z", "x"), ("z", "x"), ("z", "x"))
PARTS = 4
EARLY = 2
STAGES = sum(len(order) for order in PART_ORDERS)
SIZES = {"wa": 2, "x": 2, "z": 4}


class Links:
    def __init__(self):
        me = lax.axis_index("ctx")
        self.at = {
            "core": lax.rem(me, 2),
            "x": lax.rem(me // 2, 2),
            "z": me // 4,
            "wa": lax.axis_index("wa"),
        }

    def peer(self, axis, value):
        at = dict(self.at)
        at[axis] = value
        return {"ctx": at["z"] * 4 + at["x"] * 2 + at["core"], "wa": at["wa"]}


def splits_rows(piece):
    return piece % 64 == 0


def grad_sum_kernel(*refs):
    refs = list(refs)
    sizes = (PARTS, PARTS, PARTS - EARLY, STAGES)
    g_refs, out_refs, core_bufs, bufs = (
        [refs.pop(0) for _ in range(number)] for number in sizes
    )
    core_bufs = [None] * EARLY + core_bufs
    send_sem, recv_sem = refs
    links = Links()
    core, x, z, wa = (links.at[name] for name in ("core", "x", "z", "wa"))
    barrier = pltpu.get_barrier_semaphore()
    peers = [links.peer("core", 1 - core), links.peer("x", 1 - x), links.peer("wa", 1 - wa)]
    peers += [links.peer("z", lax.rem(z + step, 4)) for step in range(1, 4)]
    for peer in peers:
        pl.semaphore_signal(barrier, inc=1, device_id=peer, device_id_type=pl.DeviceIdType.MESH)
    pl.semaphore_wait(barrier, len(peers))
    used = [0]

    def remote(src, dst, peer):
        index = used[0]
        used[0] += 1
        copy = pltpu.make_async_remote_copy(
            src_ref=src,
            dst_ref=dst,
            send_sem=send_sem.at[index],
            recv_sem=recv_sem.at[index],
            device_id=peer,
            device_id_type=pl.DeviceIdType.MESH,
        )
        copy.start()
        return copy

    def z_share(ref, value):
        piece, width = ref.shape[-2:]
        if value is None:
            return slice(None), slice(None)
        if splits_rows(piece):
            return pl.ds(pl.multiple_of(value * (piece // 4), 16), piece // 4), slice(None)
        return slice(None), pl.ds(pl.multiple_of(value * (width // 4), LANES), width // 4)

    def slab(part, held, axis=None, value=None):
        at = dict(links.at)
        if axis is not None:
            at[axis] = value
            held = held | {axis}
        return g_refs[part].at[
            pl.ds(0, 1) if part < EARLY else pl.ds(at["wa"], 1) if "wa" in held else pl.ds(0, 2),
            0 if part < EARLY else core,
            pl.ds(at["x"], 1) if "x" in held else pl.ds(0, 2),
            *z_share(g_refs[part], at["z"] if "z" in held else None),
        ]

    def add_into(target, sources):
        outer, inner, rows, _ = target.shape
        for a in range(outer):
            for b in range(inner):

                def add(group, _):
                    some = pl.ds(pl.multiple_of(group * 16, 16), 16)
                    total = target[a, b, some, :].astype(jnp.float32)
                    for source in sources:
                        total = total + source[a, b, some, :].astype(jnp.float32)
                    target[a, b, some, :] = total.astype(low_type)
                    return 0

                lax.fori_loop(0, rows // 16, add, 0)

    core_copies = [
        remote(g_refs[part].at[:, 1 - core], core_bufs[part], links.peer("core", 1 - core))
        if part >= EARLY
        else None
        for part in range(PARTS)
    ]
    first_buf = [sum(len(order) for order in PART_ORDERS[:part]) for part in range(PARTS)]

    def begin(part, stage):
        axis = PART_ORDERS[part][stage]
        held = set(PART_ORDERS[part][:stage])
        buf = bufs[first_buf[part] + stage]
        copies = []
        for step in range(1, SIZES[axis]):
            value = lax.rem(links.at[axis] + step, SIZES[axis])
            copies.append(
                remote(slab(part, held, axis, value), buf.at[step - 1], links.peer(axis, value))
            )
        return copies

    flying = {}
    for part in range(PARTS):
        if part >= EARLY:
            core_copies[part].wait()
            add_into(slab(part, set()), [core_bufs[part]])
        flying[part] = begin(part, 0)
    for stage in range(3):
        for part in range(PARTS):
            order = PART_ORDERS[part]
            if stage >= len(order):
                continue
            for copy in flying[part]:
                copy.wait()
            buf = bufs[first_buf[part] + stage]
            add_into(
                slab(part, set(order[: stage + 1])),
                [buf.at[step] for step in range(SIZES[order[stage]] - 1)],
            )
            flying[part] = begin(part, stage + 1) if stage + 1 < len(order) else None

    def out_slab(part, held):
        return out_refs[part].at[
            core,
            pl.ds(x, 1) if "x" in held else pl.ds(0, 2),
            *z_share(out_refs[part], z if "z" in held else None),
        ]

    def spread(part, stage):
        axis = GATHER_ORDERS[part][stage]
        block = out_slab(part, set(GATHER_ORDERS[part][stage:]))
        return [
            remote(block, block, links.peer(axis, lax.rem(links.at[axis] + step, SIZES[axis])))
            for step in range(1, SIZES[axis])
        ]

    for part in range(PARTS):
        out_slab(part, {"x", "z"})[...] = slab(part, {"wa", "x", "z"})[0]
        flying[part] = spread(part, 0)
    for stage in range(2):
        for part in range(PARTS):
            for copy in flying[part]:
                copy.wait()
            if stage == 0:
                flying[part] = spread(part, 1)
            else:
                block = out_slab(part, set())
                flying[part] = [remote(block, block, links.peer("core", 1 - core))]
    for part in range(PARTS):
        for copy in flying[part]:
            copy.wait()


def grad_sum(grads, collective_id):
    bufs, core_bufs, outs, given = [], [], [], []
    for part, grad in enumerate(grads):
        rows, width = grad.shape
        early = part < EARLY
        piece = rows // 2 if early else rows // 8
        shape = {"wa": 1 if early else 2, "x": 2, "z": 4}
        for axis in PART_ORDERS[part]:
            shape[axis] //= SIZES[axis]
            share = (
                (piece * shape["z"] // 4, width)
                if splits_rows(piece)
                else (piece, width * shape["z"] // 4)
            )
            bufs.append(
                pltpu.VMEM((SIZES[axis] - 1, shape["wa"], shape["x"], *share), low_type)
            )
        if not early:
            core_bufs.append(pltpu.VMEM((2, 2, piece, width), low_type))
        outs.append(jax.ShapeDtypeStruct((2, 2, piece, width), low_type))
        lead = (1, 1) if early else (2, 2)
        given.append(grad.reshape(*lead, 2, piece, width))
    vmem = pl.BlockSpec(memory_space=pltpu.VMEM)
    size = sum(grad.size for grad in grads)
    sums = pl.pallas_call(
        grad_sum_kernel,
        out_shape=tuple(outs),
        in_specs=[vmem] * PARTS,
        out_specs=(vmem,) * PARTS,
        scratch_shapes=[
            *core_bufs,
            *bufs,
            pltpu.SemaphoreType.DMA((48,)),
            pltpu.SemaphoreType.DMA((48,)),
        ],
        compiler_params=pltpu.CompilerParams(
            collective_id=collective_id, has_side_effects=True, vmem_limit_bytes=VMEM_BYTES
        ),
        cost_estimate=pl.CostEstimate(
            flops=size * 20_000, bytes_accessed=size * 4, transcendentals=0
        ),
        name="grad_sum",
    )(*given)
    return [part.reshape(-1, part.shape[-1]) for part in sums]


def pack_columns(vectors, rows):
    columns = jnp.stack([vec.astype(low_type) for vec in vectors], axis=1)
    return jnp.pad(columns, ((0, 0), (0, LANES - len(vectors))))


def column_sums(terms, lanes):
    block = jnp.stack([jnp.sum(term, axis=0) for term in terms], axis=1).astype(low_type)
    return jnp.pad(block, ((0, 0), (0, lanes - len(terms))))


def rows_of_columns(block, wanted):
    pick = jnp.eye(LANES, 8, dtype=low_type)
    return jnp.einsum("fk,kj->jf", block, pick, preferred_element_type=jnp.float32)[:wanted]


def reduce_shards(grad):
    part = lax.psum_scatter(
        grad.astype(low_type), ("wa", "ctx"), scatter_dimension=0, tiled=True
    )
    return lax.all_gather(part, "ctx", axis=0, tiled=True)


def body(
    count,
    tokens,
    cotangent,
    lengths,
    block_order,
    w_query,
    b_query,
    w_key,
    w_value,
    b_value,
    w_out,
    b_out,
    gain_one,
    shift_one,
    w_up,
    b_up,
    w_down,
    b_down,
    gain_two,
    shift_two,
):
    inputs = tokens[0]
    tok_rows, width = inputs.shape
    wide = w_up.shape[1]
    half = tok_rows // 2
    shard = w_query.shape[0]
    direct = count == 16 and width == 2 * shard and shard % 64 == 0 and wide == 4 * width
    me = lax.axis_index("ctx")
    seq_ends = jnp.cumsum(lengths[0])
    own_blocks = lax.dynamic_slice(block_order, (2 * me,), (2,))
    position = (own_blocks[:, None] * half + jnp.arange(half, dtype=jnp.int32)[None, :]).reshape(-1)
    own_seg = segment_of(position, seq_ends)
    owns = jnp.any(me == jnp.arange(HEADS, dtype=jnp.int32) * count // HEADS).astype(jnp.int32)
    meta = jnp.concatenate([seq_ends.astype(jnp.int32), owns[None]])

    core = me % 2
    wa = lax.axis_index("wa")

    def fetch_half(shard_block, after=None):
        if not direct:
            return None
        if after is not None:
            shard_block, _ = lax.optimization_barrier((shard_block, after))
        size, columns = shard_block.shape
        part = lax.dynamic_slice(shard_block, (core * (size // 2), 0), (size // 2, columns))
        return lax.ppermute(part, "wa", [(0, 1), (1, 0)])

    def gather_rows(shard_block, fetched):
        if not direct:
            return lax.all_gather(shard_block, "wa", axis=0, tiled=True)
        size, columns = shard_block.shape
        swapped = lax.ppermute(fetched, "ctx", [(k, k ^ 1) for k in range(count)])
        other = (1 - wa) * size
        whole = jnp.zeros((2 * size, columns), shard_block.dtype)
        whole = lax.dynamic_update_slice(whole, shard_block, (wa * size, 0))
        whole = lax.dynamic_update_slice(whole, fetched, (other + core * (size // 2), 0))
        return lax.dynamic_update_slice(whole, swapped, (other + (1 - core) * (size // 2), 0))

    pair = jnp.stack(
        [
            w_key.astype(low_type).reshape(shard, HEADS, HEAD_DIM),
            w_value.astype(low_type).reshape(shard, HEADS, HEAD_DIM),
        ],
        axis=2,
    ).reshape(shard, 2 * width)
    vectors = pack_columns(
        [b_query, b_value, b_out, gain_one, shift_one, gain_two, shift_two, b_down], shard
    )
    first_shard = jnp.concatenate([w_query.astype(low_type), pair, vectors], axis=1)
    fetched = fetch_half(first_shard)
    later_shards = (
        w_out.astype(low_type),
        w_up.astype(low_type),
        jnp.concatenate([w_down.astype(low_type), pack_columns([b_up], 4 * shard)], axis=1),
    )
    later_fetched = tuple(fetch_half(block, fetched) for block in later_shards)
    first_pack = gather_rows(first_shard, fetched)
    query_weight = first_pack[:, :width]
    pair_weight = first_pack[:, width : 3 * width]
    vector_rows = rows_of_columns(first_pack[:, 3 * width :], 8)
    query_bias, value_bias, out_bias, gain_first, shift_first, gain_second, shift_second, down_bias = (
        vector_rows[index] for index in range(8)
    )
    pair_bias = jnp.stack(
        [jnp.zeros((HEADS, HEAD_DIM), jnp.float32), value_bias.reshape(HEADS, HEAD_DIM)], axis=1
    ).reshape(1, 2 * width)

    packed = project(inputs, query_weight, pair_weight, query_bias[None, :], pair_bias)
    at_head = to_heads(packed, count, 0)
    context_out, qa, ka, va, sums = attend(meta, block_order, at_head)
    context_out, later_fetched = lax.optimization_barrier((context_out, later_fetched))
    out_weight, up_weight, down_pack = (
        gather_rows(block, half_block) for block, half_block in zip(later_shards, later_fetched)
    )
    down_weight = down_pack[:, :width]
    up_bias = rows_of_columns(down_pack[:, width:], 1)[0]
    context_in = to_rows(context_out, count, 1)
    context_low = (
        context_in.reshape(HEADS, half, 2, HEAD_DIM).transpose(2, 1, 0, 3).reshape(tok_rows, width)
    )

    attn_out = jnp.dot(context_low, out_weight, preferred_element_type=jnp.float32) + out_bias
    h_one = inputs.astype(jnp.float32) + attn_out
    norm_one, norm_one_back = jax.vjp(layer_norm, h_one, gain_first, shift_first)
    norm_low = norm_one.astype(low_type)
    up_pre = jnp.dot(norm_low, up_weight, preferred_element_type=jnp.float32) + up_bias
    gelu_out, gelu_back = jax.vjp(partial(jax.nn.gelu, approximate=False), up_pre)
    gelu_low = gelu_out.astype(low_type)
    down_out = jnp.dot(gelu_low, down_weight, preferred_element_type=jnp.float32) + down_bias
    h_two = norm_one + down_out
    result, norm_two_back = jax.vjp(layer_norm, h_two, gain_second, shift_second)
    activations = result.astype(low_type)[None]
    valid = (own_seg < 3).astype(jnp.float32)
    g_out = cotangent[0].astype(jnp.float32) * valid[:, None]
    d_htwo, grad_gain_second, grad_shift_second = norm_two_back(g_out)
    d_down = d_htwo.astype(low_type)
    d_gelu = jnp.einsum("td,fd->tf", d_down, down_weight, preferred_element_type=jnp.float32)
    (d_uppre,) = gelu_back(d_gelu)
    d_up = d_uppre.astype(low_type)
    d_yone = d_htwo + jnp.einsum("tf,df->td", d_up, up_weight, preferred_element_type=jnp.float32)
    d_hone, grad_gain_first, grad_shift_first = norm_one_back(d_yone)
    d_attn = d_hone.astype(low_type)
    d_context = jnp.einsum("td,cd->tc", d_attn, out_weight, preferred_element_type=jnp.float32)
    context_back = (
        d_context.astype(low_type)
        .reshape(2, half, HEADS, HEAD_DIM)
        .transpose(2, 1, 0, 3)
        .reshape(HEADS, half, LANES)
    )

    grad_wdown = jnp.einsum("tf,td->fd", gelu_low, d_down, preferred_element_type=jnp.float32)
    grad_wup = jnp.einsum("td,tf->df", norm_low, d_up, preferred_element_type=jnp.float32)
    grad_wout = jnp.einsum("tc,td->cd", context_low, d_attn, preferred_element_type=jnp.float32)
    up_bias_sums = jnp.sum(d_up.astype(jnp.float32), axis=0)
    lanes = 2 * LANES
    vec_block = jnp.concatenate(
        [
            jnp.stack(
                [
                    jnp.sum(d_attn.astype(jnp.float32), axis=0),
                    grad_gain_first,
                    grad_shift_first,
                    jnp.sum(d_down.astype(jnp.float32), axis=0),
                    grad_gain_second,
                    grad_shift_second,
                ],
                axis=1,
            ),
            up_bias_sums.reshape(width // shard, 4, shard).transpose(0, 2, 1).reshape(width, 4),
        ],
        axis=1,
    ).astype(low_type)
    out_block = jnp.concatenate(
        [grad_wout.astype(low_type), jnp.pad(vec_block, ((0, 0), (0, lanes - 10)))], axis=1
    )
    up_block = grad_wup.astype(low_type)
    down_block = grad_wdown.astype(low_type)
    def add_low(mine, given):
        return (mine.astype(jnp.float32) + given.astype(jnp.float32)).astype(low_type)

    def core_halves(block):
        view = block.reshape(2, 2, -1, block.shape[1])
        keep = lax.dynamic_index_in_dim(view, core, 1, keepdims=False)
        give = lax.dynamic_index_in_dim(view, 1 - core, 1, keepdims=False)
        return keep, lax.ppermute(give, "ctx", [(k, k ^ 1) for k in range(count)])

    def wa_halves(block):
        keep = lax.dynamic_index_in_dim(block, wa, 0, keepdims=False)
        give = lax.dynamic_index_in_dim(block, 1 - wa, 0, keepdims=False)
        return keep, lax.ppermute(give, "wa", [(0, 1), (1, 0)])

    context_back, down_block, out_block, up_block = lax.optimization_barrier(
        (context_back, down_block, out_block, up_block)
    )
    if direct:
        halves = [core_halves(block) for block in (up_block, down_block)]
        back_at_head = to_heads(context_back, count, 2)
        back_at_head, halves = lax.optimization_barrier((back_at_head, halves))
        halves = [wa_halves(add_low(*pair)) for pair in halves]
        grads_out = attend_back(meta, block_order, back_at_head, qa, ka, va, sums)
        grads_out, halves = lax.optimization_barrier((grads_out, halves))
        early = [add_low(*pair) for pair in halves]
    else:
        back_at_head = to_heads(context_back, count, 2)
        grads_out = attend_back(meta, block_order, back_at_head, qa, ka, va, sums)
    grads_in = to_rows(grads_out, count, 3)

    d_pair = grads_in[:, :tok_rows, :].transpose(1, 0, 2).reshape(tok_rows, 2 * width)
    d_queries = (
        grads_in[:, tok_rows:, :]
        .reshape(HEADS, half, 2, HEAD_DIM)
        .transpose(2, 1, 0, 3)
        .reshape(tok_rows, width)
        * jnp.asarray(0.125, low_type)
    )
    d_all = jnp.concatenate([d_queries, d_pair], axis=1)
    grad_all = jnp.einsum("tc,td->cd", inputs, d_all, preferred_element_type=jnp.float32)
    d_values = d_pair.reshape(tok_rows, HEADS, 2, HEAD_DIM)[:, :, 1, :].reshape(tok_rows, width)
    last_block = jnp.concatenate(
        [
            grad_all.astype(low_type),
            column_sums([d_queries.astype(jnp.float32), d_values.astype(jnp.float32)], lanes),
        ],
        axis=1,
    )
    if direct:
        up_sum, down_sum, last_sum, out_sum = grad_sum((*early, last_block, out_block), 4)
    else:
        up_sum, down_sum, last_sum, out_sum = (
            reduce_shards(block) for block in (up_block, down_block, last_block, out_block)
        )
    d_input = (
        d_hone
        + jnp.einsum("td,cd->tc", d_queries, query_weight, preferred_element_type=jnp.float32)
        + jnp.einsum("td,cd->tc", d_pair, pair_weight, preferred_element_type=jnp.float32)
    )
    input_grad = d_input.astype(low_type)[None]

    wide_grad = last_sum.astype(jnp.float32)
    pair_grad = wide_grad[:, width : 3 * width].reshape(shard, HEADS, 2, HEAD_DIM)
    out_grad = out_sum.astype(jnp.float32)
    return (
        activations,
        input_grad,
        wide_grad[:, :width],
        wide_grad[:, 3 * width],
        pair_grad[:, :, 0, :].reshape(shard, width),
        pair_grad[:, :, 1, :].reshape(shard, width),
        wide_grad[:, 3 * width + 1],
        out_grad[:, :width],
        out_grad[:, width],
        out_grad[:, width + 1],
        out_grad[:, width + 2],
        up_sum.astype(jnp.float32),
        out_grad[:, width + 6 : width + 10].T.reshape(-1),
        down_sum.astype(jnp.float32),
        out_grad[:, width + 3],
        out_grad[:, width + 4],
        out_grad[:, width + 5],
    )


def solution(mesh):
    placed = (
        P("wa", "ctx", None),
        P("wa", "ctx", None),
        P("wa", None),
        P(),
        P("wa", None),
        P("wa"),
        P("wa", None),
        P("wa", None),
        P("wa"),
        P("wa", None),
        P("wa"),
        P("wa"),
        P("wa"),
        P("wa", None),
        P("wa"),
        P("wa", None),
        P("wa"),
        P("wa"),
        P("wa"),
    )
    return jax.shard_map(
        partial(body, mesh.shape["ctx"]),
        mesh=mesh,
        in_specs=placed,
        out_specs=(
            P("wa", "ctx", None),
            P("wa", "ctx", None),
            P("wa", None),
            P("wa"),
            P("wa", None),
            P("wa", None),
            P("wa"),
            P("wa", None),
            P("wa"),
            P("wa"),
            P("wa"),
            P("wa", None),
            P("wa"),
            P("wa", None),
            P("wa"),
            P("wa"),
            P("wa"),
        ),
        check_vma=False,
    )
```

```python
from functools import partial

import jax
import jax.numpy as jnp
from jax import lax
from jax.experimental import pallas as pl
from jax.experimental.pallas import tpu as pltpu
from jax.sharding import PartitionSpec as P

HEADS = 12
HEAD_DIM = 64
LANES = 128
TILE = 512
FAR = -(2.0**40)
VMEM_BYTES = 60 << 20

low_type = jnp.bfloat16
epsilon = 1e-05


def dot_nt(left, right):
    return lax.dot_general(
        left, right, (((1,), (1,)), ((), ())), preferred_element_type=jnp.float32
    )


def dot_nn(left, right):
    return lax.dot_general(
        left, right, (((1,), (0,)), ((), ())), preferred_element_type=jnp.float32
    )


def layer_norm(hidden, gain_vec, shift_vec):
    centre = hidden - jnp.mean(hidden, axis=-1, keepdims=True)
    spread = jnp.mean(centre * centre, axis=-1, keepdims=True)
    return centre * lax.rsqrt(spread + epsilon) * gain_vec + shift_vec


def segment_of(position, seq_ends):
    return jnp.sum((position[:, None] >= seq_ends[None, :]).astype(jnp.int32), axis=1)


def owner_of(head, count):
    return head * count // HEADS


def greet_all(count, me):
    barrier = pltpu.get_barrier_semaphore()

    def greet(step, _):
        other = lax.rem(me + step, count)
        pl.semaphore_signal(
            barrier, inc=1, device_id={"ctx": other}, device_id_type=pl.DeviceIdType.MESH
        )
        return 0

    lax.fori_loop(1, count, greet, 0)
    pl.semaphore_wait(barrier, count - 1)


def to_heads_kernel(count, send_ref, recv_ref, send_sem, recv_sem, own_sem):
    me = lax.axis_index("ctx")
    greet_all(count, me)
    first = me * HEADS // count + 1

    def copy_for(head, source, owner):
        return pltpu.make_async_remote_copy(
            src_ref=send_ref.at[head],
            dst_ref=recv_ref.at[source],
            send_sem=send_sem.at[head],
            recv_sem=recv_sem.at[source],
            device_id={"ctx": owner},
            device_id_type=pl.DeviceIdType.MESH,
        )

    def own_copy(head):
        return pltpu.make_async_copy(send_ref.at[head], recv_ref.at[me], own_sem)

    def begin(step, _):
        head = lax.rem(first + step, HEADS)
        owner = owner_of(head, count)

        @pl.when(owner != me)
        def _():
            copy_for(head, me, owner).start()

        @pl.when(owner == me)
        def _():
            own_copy(head).start()

        return 0

    lax.fori_loop(0, HEADS, begin, 0)

    def finish(head, _):
        owner = owner_of(head, count)

        @pl.when(owner != me)
        def _():
            copy_for(head, me, owner).wait_send()

        @pl.when(owner == me)
        def _():
            own_copy(head).wait()

            def arrive(source, _):
                @pl.when(source != me)
                def _():
                    copy_for(head, source, owner).wait_recv()

                return 0

            lax.fori_loop(0, count, arrive, 0)

        return 0

    lax.fori_loop(0, HEADS, finish, 0)


def to_heads(send, count, collective_id):
    rows = send.shape[1]
    return pl.pallas_call(
        partial(to_heads_kernel, count),
        out_shape=jax.ShapeDtypeStruct((count, rows, LANES), low_type),
        in_specs=[pl.BlockSpec(memory_space=pltpu.VMEM)],
        out_specs=pl.BlockSpec(memory_space=pltpu.VMEM),
        scratch_shapes=[
            pltpu.SemaphoreType.DMA((HEADS,)),
            pltpu.SemaphoreType.DMA((count,)),
            pltpu.SemaphoreType.DMA,
        ],
        compiler_params=pltpu.CompilerParams(
            collective_id=collective_id, has_side_effects=True, vmem_limit_bytes=VMEM_BYTES
        ),
        cost_estimate=pl.CostEstimate(
            flops=rows * 250_000_000, bytes_accessed=send.size * 4, transcendentals=0
        ),
        name=f"to_heads_{rows}",
    )(send)


def to_rows_kernel(count, send_ref, recv_ref, send_sem, recv_sem, own_sem):
    me = lax.axis_index("ctx")
    greet_all(count, me)

    def copy_for(head, target):
        return pltpu.make_async_remote_copy(
            src_ref=send_ref.at[target],
            dst_ref=recv_ref.at[head],
            send_sem=send_sem.at[target],
            recv_sem=recv_sem.at[head],
            device_id={"ctx": target},
            device_id_type=pl.DeviceIdType.MESH,
        )

    def own_copy(head):
        return pltpu.make_async_copy(send_ref.at[me], recv_ref.at[head], own_sem)

    def begin(head, _):
        @pl.when(owner_of(head, count) == me)
        def _():
            own_copy(head).start()

            def push(step, _):
                copy_for(head, lax.rem(me + step, count)).start()
                return 0

            lax.fori_loop(1, count, push, 0)

        return 0

    lax.fori_loop(0, HEADS, begin, 0)

    def finish(head, _):
        @pl.when(owner_of(head, count) == me)
        def _():
            own_copy(head).wait()

            def leave(step, _):
                copy_for(head, lax.rem(me + step, count)).wait_send()
                return 0

            lax.fori_loop(1, count, leave, 0)

        @pl.when(owner_of(head, count) != me)
        def _():
            copy_for(head, me).wait_recv()

        return 0

    lax.fori_loop(0, HEADS, finish, 0)


def to_rows(send, count, collective_id):
    rows = send.shape[1]
    return pl.pallas_call(
        partial(to_rows_kernel, count),
        out_shape=jax.ShapeDtypeStruct((HEADS, rows, LANES), low_type),
        in_specs=[pl.BlockSpec(memory_space=pltpu.VMEM)],
        out_specs=pl.BlockSpec(memory_space=pltpu.VMEM),
        scratch_shapes=[
            pltpu.SemaphoreType.DMA((count,)),
            pltpu.SemaphoreType.DMA((HEADS,)),
            pltpu.SemaphoreType.DMA,
        ],
        compiler_params=pltpu.CompilerParams(
            collective_id=collective_id, has_side_effects=True, vmem_limit_bytes=VMEM_BYTES
        ),
        cost_estimate=pl.CostEstimate(
            flops=rows * 250_000_000, bytes_accessed=send.size * 4, transcendentals=0
        ),
        name=f"to_rows_{rows}",
    )(send)


def project_kernel(x_ref, pack_ref, bq_ref, bkv_ref, out_ref):
    rows, width = x_ref.shape
    half = rows // 2
    step = 4
    for base in range(0, HEADS, step):
        cols = slice(base * LANES, (base + step) * LANES)
        both = (dot_nn(x_ref[...], pack_ref[:, width + cols.start : width + cols.stop]) + bkv_ref[:, cols]).astype(low_type)
        for at in range(step):
            out_ref[base + at, 0:rows, :] = both[:, at * LANES : (at + 1) * LANES]
        cols = slice(base * HEAD_DIM, (base + step) * HEAD_DIM)
        query = ((dot_nn(x_ref[...], pack_ref[:, cols]) + bq_ref[:, cols]) * 0.125).astype(low_type)
        for at in range(step):
            lanes = slice(at * HEAD_DIM, (at + 1) * HEAD_DIM)
            out_ref[base + at, rows : rows + half, :] = jnp.concatenate(
                [query[:half, lanes], query[half:, lanes]], axis=1
            )


def project(x, pack, bq, bkv):
    rows = x.shape[0]
    vmem = pl.BlockSpec(memory_space=pltpu.VMEM)
    return pl.pallas_call(
        project_kernel,
        out_shape=jax.ShapeDtypeStruct((HEADS, rows + rows // 2, LANES), low_type),
        in_specs=[vmem] * 4,
        out_specs=vmem,
        compiler_params=pltpu.CompilerParams(vmem_limit_bytes=VMEM_BYTES),
        name="project",
    )(x, pack, bq, bkv)


def tile_range(meta_ref, first, last, total):
    end_a, end_b, end_c = meta_ref[0], meta_ref[1], meta_ref[2]
    low = jnp.where(
        first >= end_c, end_c, jnp.where(first >= end_b, end_b, jnp.where(first >= end_a, end_a, 0))
    )
    high = jnp.where(
        last >= end_c,
        total,
        jnp.where(last >= end_b, end_c, jnp.where(last >= end_a, end_b, end_a)),
    )
    return low // TILE, (high + TILE - 1) // TILE


def attend_kernel(meta_ref, order_ref, recv_ref, out_ref, qa_ref, ka_ref, va_ref, sum_ref):
    count = recv_ref.shape[0]
    half = recv_ref.shape[1] // 3
    total = qa_ref.shape[0]

    @pl.when(meta_ref[3] == 1)
    def _():
        lane = lax.broadcasted_iota(jnp.int32, (half, LANES), 1)
        lower = lane < HEAD_DIM
        row = lax.broadcasted_iota(jnp.int32, (half, LANES), 0)

        def place(source, _):
            query = recv_ref[source, 2 * half :, :].astype(jnp.float32)
            for part in range(2):
                first = pl.multiple_of(order_ref[2 * source + part] * half, half)
                position = first + row
                segment = (
                    (position >= meta_ref[0]).astype(jnp.int32)
                    + (position >= meta_ref[1]).astype(jnp.int32)
                    + (position >= meta_ref[2]).astype(jnp.int32)
                )
                mine = (lane - HEAD_DIM) == segment
                other = (lane < HEAD_DIM + 4) & (~mine)
                pair = recv_ref[source, part * half : (part + 1) * half, :].astype(jnp.float32)
                if part == 1:
                    query = pltpu.roll(query, HEAD_DIM, 1)
                mark_k = jnp.where(
                    other, FAR, jnp.where((lane >= HEAD_DIM + 4) & (lane < HEAD_DIM + 7), 1.0, 0.0)
                )
                rows = pl.ds(first, half)
                qa_ref[rows, :] = jnp.where(lower, query, jnp.where(mine, 1.0, 0.0)).astype(low_type)
                ka_ref[rows, :] = jnp.where(lower, pair, mark_k).astype(low_type)
                va_ref[rows, :] = jnp.where(lower, 1.0, pair).astype(low_type)
            return 0

        lax.fori_loop(0, count, place, 0)

        def query_step(index, _):
            first = pl.multiple_of(index * TILE, TILE)
            rows = pl.ds(first, TILE)
            begin, end = tile_range(meta_ref, first, first + TILE - 1, total)
            query = qa_ref[rows, :]
            sum_ref[rows, :] = jnp.zeros((TILE, LANES), jnp.float32)

            def key_step(key_index, _):
                keys = pl.ds(pl.multiple_of(key_index * TILE, TILE), TILE)
                expo = jnp.exp(dot_nt(query, ka_ref[keys, :])).astype(low_type)
                sum_ref[rows, :] += dot_nn(expo, va_ref[keys, :])
                return 0

            lax.fori_loop(begin, end, key_step, 0)
            return 0

        lax.fori_loop(0, total // TILE, query_step, 0)

        def give(source, _):
            parts = []
            for part in range(2):
                first = pl.multiple_of(order_ref[2 * source + part] * half, half)
                block = sum_ref[pl.ds(first, half), :]
                parts.append((block, pltpu.roll(block, HEAD_DIM, 1)))
            top = jnp.where(lower, parts[0][1], parts[1][0])
            bottom = jnp.where(lower, parts[0][0], parts[1][1])
            out_ref[source] = (top / bottom).astype(low_type)
            return 0

        lax.fori_loop(0, count, give, 0)


def attend(meta, order, recv):
    count, rows, _ = recv.shape
    total = count * rows * 2 // 3
    vmem = pl.BlockSpec(memory_space=pltpu.VMEM)
    smem = pl.BlockSpec(memory_space=pltpu.SMEM)
    whole = jax.ShapeDtypeStruct((total, LANES), low_type)
    return pl.pallas_call(
        attend_kernel,
        out_shape=(
            jax.ShapeDtypeStruct((count, rows // 3, LANES), low_type),
            whole,
            whole,
            whole,
            jax.ShapeDtypeStruct((total, LANES), jnp.float32),
        ),
        in_specs=[smem, smem, vmem],
        out_specs=(vmem,) * 5,
        compiler_params=pltpu.CompilerParams(vmem_limit_bytes=VMEM_BYTES),
        cost_estimate=pl.CostEstimate(
            flops=total * total * LANES * 8, bytes_accessed=total * LANES * 12, transcendentals=0
        ),
        name="attend",
    )(meta, order, recv)


def split_three(value):
    first = value.astype(low_type).astype(jnp.float32)
    rest = value - first
    second = rest.astype(low_type).astype(jnp.float32)
    return first, second, rest - second


def attend_back_kernel(
    meta_ref,
    order_ref,
    recv_ref,
    qa_ref,
    ka_ref,
    va_ref,
    sum_ref,
    out_ref,
    qb_ref,
    da_ref,
    kt_ref,
    dkv_ref,
    dq_ref,
    acc_ref,
):
    count = recv_ref.shape[0]
    half = recv_ref.shape[1]
    total = qa_ref.shape[0]

    @pl.when(meta_ref[3] == 1)
    def _():
        lane = lax.broadcasted_iota(jnp.int32, (half, LANES), 1)
        lower = lane < HEAD_DIM

        def place(source, _):
            given = recv_ref[source].astype(jnp.float32)
            for part in range(2):
                first = pl.multiple_of(order_ref[2 * source + part] * half, half)
                rows = pl.ds(first, half)
                block = sum_ref[rows, :]
                turned = pltpu.roll(block, HEAD_DIM, 1)
                d_context = pltpu.roll(given, HEAD_DIM, 1) if part == 0 else given
                product = jnp.where(lower, 0.0, d_context * (block / turned))
                minus = -jnp.sum(product, axis=1, keepdims=True)
                one, two, three = split_three(minus)
                mark = jnp.where(
                    lane == 0, one, jnp.where(lane == 1, two, jnp.where(lane == 2, three, 0.0))
                )
                da_ref[rows, :] = jnp.where(lower, mark, d_context).astype(low_type)
                one, two, three = split_three(-jnp.log(turned))
                at = lane - (HEAD_DIM + 4)
                mark = jnp.where(at == 0, one, jnp.where(at == 1, two, three))
                query = qa_ref[rows, :].astype(jnp.float32)
                qb_ref[rows, :] = jnp.where((at >= 0) & (at < 3), mark, query).astype(low_type)
            return 0

        lax.fori_loop(0, count, place, 0)

        def prepare(index, _):
            rows = pl.ds(pl.multiple_of(index * TILE, TILE), TILE)
            kt_ref[:, rows] = jnp.transpose(ka_ref[rows, :])[:HEAD_DIM, :]
            dkv_ref[rows, :] = jnp.zeros((TILE, LANES), jnp.float32)
            return 0

        lax.fori_loop(0, total // TILE, prepare, 0)

        lower_tile = lax.broadcasted_iota(jnp.int32, (TILE, LANES), 1) < HEAD_DIM

        def query_step(index, _):
            first = pl.multiple_of(index * TILE, TILE)
            rows = pl.ds(first, TILE)
            begin, end = tile_range(meta_ref, first, first + TILE - 1, total)
            query = qb_ref[rows, :]
            given = da_ref[rows, :]
            query_only = jnp.where(lower_tile, query.astype(jnp.float32), 0.0).astype(low_type)
            given_only = jnp.where(lower_tile, 0.0, given.astype(jnp.float32)).astype(low_type)
            acc_ref[...] = jnp.zeros_like(acc_ref)

            def key_step(key_index, _):
                keys = pl.ds(pl.multiple_of(key_index * TILE, TILE), TILE)
                prob = jnp.exp(dot_nt(ka_ref[keys, :], query))
                d_scores = (prob * dot_nt(va_ref[keys, :], given)).astype(low_type)
                dkv_ref[keys, :] += dot_nn(d_scores, query_only) + dot_nn(
                    prob.astype(low_type), given_only
                )
                acc_ref[...] += dot_nn(kt_ref[:, keys], d_scores)
                return 0

            lax.fori_loop(begin, end, key_step, 0)
            dq_ref[rows, :] = jnp.transpose(acc_ref[...])
            return 0

        lax.fori_loop(0, total // TILE, query_step, 0)

        def give(source, _):
            queries = []
            for part in range(2):
                first = pl.multiple_of(order_ref[2 * source + part] * half, half)
                rows = pl.ds(first, half)
                out_ref[source, part * half : (part + 1) * half, :] = dkv_ref[rows, :].astype(low_type)
                queries.append(dq_ref[rows, :])
            out_ref[source, 2 * half :, :] = jnp.concatenate(queries, axis=1).astype(low_type)
            return 0

        lax.fori_loop(0, count, give, 0)


def attend_back(meta, order, recv, qa, ka, va, sums):
    count, half, _ = recv.shape
    total = qa.shape[0]
    vmem = pl.BlockSpec(memory_space=pltpu.VMEM)
    smem = pl.BlockSpec(memory_space=pltpu.SMEM)
    return pl.pallas_call(
        attend_back_kernel,
        out_shape=jax.ShapeDtypeStruct((count, 3 * half, LANES), low_type),
        in_specs=[smem, smem] + [vmem] * 5,
        out_specs=vmem,
        scratch_shapes=[
            pltpu.VMEM((total, LANES), low_type),
            pltpu.VMEM((total, LANES), low_type),
            pltpu.VMEM((HEAD_DIM, total), low_type),
            pltpu.VMEM((total, LANES), jnp.float32),
            pltpu.VMEM((total, HEAD_DIM), jnp.float32),
            pltpu.VMEM((HEAD_DIM, TILE), jnp.float32),
        ],
        compiler_params=pltpu.CompilerParams(vmem_limit_bytes=VMEM_BYTES),
        cost_estimate=pl.CostEstimate(
            flops=total * total * LANES * 16, bytes_accessed=total * LANES * 16, transcendentals=0
        ),
        name="attend_back",
    )(meta, order, recv, qa, ka, va, sums)


PART_ORDERS = (("x", "z"), ("x", "z"), ("wa", "x", "z"), ("wa", "x", "z"))
GATHER_ORDERS = (("z", "x"), ("z", "x"), ("z", "x"), ("x", "z"))
PARTS = len(PART_ORDERS)
EARLY = sum(len(order) == 2 for order in PART_ORDERS)
STAGES = sum(len(order) for order in PART_ORDERS)
SIZES = {"wa": 2, "x": 2, "z": 4}


class Links:
    def __init__(self):
        me = lax.axis_index("ctx")
        self.at = {
            "core": lax.rem(me, 2),
            "x": lax.rem(me // 2, 2),
            "z": me // 4,
            "wa": lax.axis_index("wa"),
        }

    def peer(self, axis, value):
        at = dict(self.at)
        at[axis] = value
        return {"ctx": at["z"] * 4 + at["x"] * 2 + at["core"], "wa": at["wa"]}


def splits_rows(piece):
    return piece % 64 == 0


def grad_sum_kernel(*refs):
    refs = list(refs)
    sizes = (PARTS, PARTS, PARTS - EARLY, STAGES)
    g_refs, out_refs, core_bufs, bufs = (
        [refs.pop(0) for _ in range(number)] for number in sizes
    )
    core_bufs = [None] * EARLY + core_bufs
    send_sem, recv_sem = refs
    links = Links()
    core, x, z, wa = (links.at[name] for name in ("core", "x", "z", "wa"))
    barrier = pltpu.get_barrier_semaphore()
    peers = [links.peer("core", 1 - core), links.peer("x", 1 - x), links.peer("wa", 1 - wa)]
    peers += [links.peer("z", lax.rem(z + step, 4)) for step in range(1, 4)]
    for peer in peers:
        pl.semaphore_signal(barrier, inc=1, device_id=peer, device_id_type=pl.DeviceIdType.MESH)
    pl.semaphore_wait(barrier, len(peers))
    used = [0]

    def remote(src, dst, peer):
        index = used[0]
        used[0] += 1
        copy = pltpu.make_async_remote_copy(
            src_ref=src,
            dst_ref=dst,
            send_sem=send_sem.at[index],
            recv_sem=recv_sem.at[index],
            device_id=peer,
            device_id_type=pl.DeviceIdType.MESH,
        )
        copy.start()
        return copy

    def z_share(ref, value):
        piece, width = ref.shape[-2:]
        if value is None:
            return slice(None), slice(None)
        if splits_rows(piece):
            return pl.ds(pl.multiple_of(value * (piece // 4), 16), piece // 4), slice(None)
        return slice(None), pl.ds(pl.multiple_of(value * (width // 4), LANES), width // 4)

    def slab(part, held, axis=None, value=None):
        at = dict(links.at)
        if axis is not None:
            at[axis] = value
            held = held | {axis}
        return g_refs[part].at[
            pl.ds(0, 1) if part < EARLY else pl.ds(at["wa"], 1) if "wa" in held else pl.ds(0, 2),
            0 if part < EARLY else core,
            pl.ds(at["x"], 1) if "x" in held else pl.ds(0, 2),
            *z_share(g_refs[part], at["z"] if "z" in held else None),
        ]

    def add_into(target, sources):
        outer, inner, rows, _ = target.shape
        for a in range(outer):
            for b in range(inner):

                def add(group, _):
                    some = pl.ds(pl.multiple_of(group * 16, 16), 16)
                    total = target[a, b, some, :].astype(jnp.float32)
                    for source in sources:
                        total = total + source[a, b, some, :].astype(jnp.float32)
                    target[a, b, some, :] = total.astype(low_type)
                    return 0

                lax.fori_loop(0, rows // 16, add, 0)

    core_copies = [
        remote(g_refs[part].at[:, 1 - core], core_bufs[part], links.peer("core", 1 - core))
        if part >= EARLY
        else None
        for part in range(PARTS)
    ]
    first_buf = [sum(len(order) for order in PART_ORDERS[:part]) for part in range(PARTS)]

    def begin(part, stage):
        axis = PART_ORDERS[part][stage]
        held = set(PART_ORDERS[part][:stage])
        buf = bufs[first_buf[part] + stage]
        copies = []
        for step in range(1, SIZES[axis]):
            value = lax.rem(links.at[axis] + step, SIZES[axis])
            copies.append(
                remote(slab(part, held, axis, value), buf.at[step - 1], links.peer(axis, value))
            )
        return copies

    def out_slab(part, held):
        return out_refs[part].at[
            core,
            pl.ds(x, 1) if "x" in held else pl.ds(0, 2),
            *z_share(out_refs[part], z if "z" in held else None),
        ]

    def spread(part, stage):
        axis = GATHER_ORDERS[part][stage]
        block = out_slab(part, set(GATHER_ORDERS[part][stage:]))
        return [
            remote(block, block, links.peer(axis, lax.rem(links.at[axis] + step, SIZES[axis])))
            for step in range(1, SIZES[axis])
        ]

    def start_gather(part, stage):
        if stage < 2:
            return spread(part, stage)
        block = out_slab(part, set())
        return [remote(block, block, links.peer("core", 1 - core))]

    flying, passed = {}, {}
    for part in range(PARTS):
        passed[part] = 0 if part >= EARLY else 1
        flying[part] = begin(part, 0) if part < EARLY else [core_copies[part]]
    while any(flying.values()):
        for part in range(PARTS):
            if not flying[part]:
                continue
            order = PART_ORDERS[part]
            for copy in flying[part]:
                copy.wait()
            step = passed[part]
            passed[part] += 1
            if step == 0:
                add_into(slab(part, set()), [core_bufs[part]])
            elif step <= len(order):
                buf = bufs[first_buf[part] + step - 1]
                add_into(
                    slab(part, set(order[:step])),
                    [buf.at[at] for at in range(SIZES[order[step - 1]] - 1)],
                )
            if step < len(order):
                flying[part] = begin(part, step)
            elif step == len(order):
                out_slab(part, {"x", "z"})[...] = slab(part, {"wa", "x", "z"})[0]
                flying[part] = start_gather(part, 0)
            elif step <= len(order) + 2:
                flying[part] = start_gather(part, step - len(order))
            else:
                flying[part] = None


def grad_sum(grads, collective_id):
    bufs, core_bufs, outs, given = [], [], [], []
    for part, grad in enumerate(grads):
        rows, width = grad.shape
        early = part < EARLY
        piece = rows // 2 if early else rows // 8
        shape = {"wa": 1 if early else 2, "x": 2, "z": 4}
        for axis in PART_ORDERS[part]:
            shape[axis] //= SIZES[axis]
            share = (
                (piece * shape["z"] // 4, width)
                if splits_rows(piece)
                else (piece, width * shape["z"] // 4)
            )
            bufs.append(
                pltpu.VMEM((SIZES[axis] - 1, shape["wa"], shape["x"], *share), low_type)
            )
        if not early:
            core_bufs.append(pltpu.VMEM((2, 2, piece, width), low_type))
        outs.append(jax.ShapeDtypeStruct((2, 2, piece, width), low_type))
        lead = (1, 1) if early else (2, 2)
        given.append(grad.reshape(*lead, 2, piece, width))
    vmem = pl.BlockSpec(memory_space=pltpu.VMEM)
    size = sum(grad.size for grad in grads)
    sums = pl.pallas_call(
        grad_sum_kernel,
        out_shape=tuple(outs),
        in_specs=[vmem] * PARTS,
        out_specs=(vmem,) * PARTS,
        scratch_shapes=[
            *core_bufs,
            *bufs,
            pltpu.SemaphoreType.DMA((16 * PARTS,)),
            pltpu.SemaphoreType.DMA((16 * PARTS,)),
        ],
        compiler_params=pltpu.CompilerParams(
            collective_id=collective_id, has_side_effects=True, vmem_limit_bytes=VMEM_BYTES
        ),
        cost_estimate=pl.CostEstimate(
            flops=size * 20_000, bytes_accessed=size * 4, transcendentals=0
        ),
        name="grad_sum",
    )(*given)
    return [part.reshape(-1, part.shape[-1]) for part in sums]


def column_sums(terms, lanes):
    block = jnp.stack([jnp.sum(term, axis=0) for term in terms], axis=1).astype(low_type)
    return jnp.pad(block, ((0, 0), (0, lanes - len(terms))))


def reduce_shards(grad):
    part = lax.psum_scatter(
        grad.astype(low_type), ("wa", "ctx"), scatter_dimension=0, tiled=True
    )
    return lax.all_gather(part, "ctx", axis=0, tiled=True)


def body(
    count,
    tokens,
    cotangent,
    lengths,
    block_order,
    w_query,
    b_query,
    w_key,
    w_value,
    b_value,
    w_out,
    b_out,
    gain_one,
    shift_one,
    w_up,
    b_up,
    w_down,
    b_down,
    gain_two,
    shift_two,
):
    inputs = tokens[0]
    tok_rows, width = inputs.shape
    wide = w_up.shape[1]
    half = tok_rows // 2
    shard = w_query.shape[0]
    direct = count == 16 and width == 2 * shard and shard % 64 == 0 and wide == 4 * width
    me = lax.axis_index("ctx")
    seq_ends = jnp.cumsum(lengths[0])
    own_blocks = lax.dynamic_slice(block_order, (2 * me,), (2,))
    position = (own_blocks[:, None] * half + jnp.arange(half, dtype=jnp.int32)[None, :]).reshape(-1)
    own_seg = segment_of(position, seq_ends)
    owns = jnp.any(me == jnp.arange(HEADS, dtype=jnp.int32) * count // HEADS).astype(jnp.int32)
    meta = jnp.concatenate([seq_ends.astype(jnp.int32), owns[None]])

    core = me % 2
    wa = lax.axis_index("wa")

    def fetch_half(shard_block, after=None):
        if not direct:
            return None
        if after is not None:
            shard_block, _ = lax.optimization_barrier((shard_block, after))
        size, columns = shard_block.shape
        part = lax.dynamic_slice(shard_block, (core * (size // 2), 0), (size // 2, columns))
        return lax.ppermute(part, "wa", [(0, 1), (1, 0)])

    def gather_rows(shard_block, fetched):
        if not direct:
            return lax.all_gather(shard_block, "wa", axis=0, tiled=True)
        size, columns = shard_block.shape
        swapped = lax.ppermute(fetched, "ctx", [(k, k ^ 1) for k in range(count)])
        other = (1 - wa) * size
        whole = jnp.zeros((2 * size, columns), shard_block.dtype)
        whole = lax.dynamic_update_slice(whole, shard_block, (wa * size, 0))
        whole = lax.dynamic_update_slice(whole, fetched, (other + core * (size // 2), 0))
        return lax.dynamic_update_slice(whole, swapped, (other + (1 - core) * (size // 2), 0))

    pair = jnp.stack(
        [
            w_key.astype(low_type).reshape(shard, HEADS, HEAD_DIM),
            w_value.astype(low_type).reshape(shard, HEADS, HEAD_DIM),
        ],
        axis=2,
    ).reshape(shard, 2 * width)
    own_vectors = jnp.concatenate(
        [b_query, b_value, b_out, gain_one, shift_one, gain_two, shift_two, b_down, b_up]
    ).astype(low_type)
    if direct:
        other_vectors = lax.ppermute(own_vectors, "wa", [(0, 1), (1, 0)])
        flat_vectors = jnp.where(
            wa == 0,
            jnp.stack([own_vectors, other_vectors]),
            jnp.stack([other_vectors, own_vectors]),
        )
    else:
        flat_vectors = lax.all_gather(own_vectors, "wa", axis=0)
    flat_vectors = flat_vectors.astype(jnp.float32)

    def vector(index):
        return flat_vectors[:, index * shard : (index + 1) * shard].reshape(-1)

    first_shard = jnp.concatenate([w_query.astype(low_type), pair], axis=1)
    fetched = fetch_half(first_shard)
    later_shards = (
        w_out.astype(low_type),
        w_up.astype(low_type),
        w_down.astype(low_type),
    )
    later_fetched = tuple(fetch_half(block, fetched) for block in later_shards)
    first_pack = gather_rows(first_shard, fetched)
    query_weight = first_pack[:, :width]
    pair_weight = first_pack[:, width : 3 * width]
    query_bias, value_bias, out_bias, gain_first, shift_first, gain_second, shift_second, down_bias = (
        vector(index) for index in range(8)
    )
    up_bias = flat_vectors[:, 8 * shard :].reshape(-1)
    pair_bias = jnp.stack(
        [jnp.zeros((HEADS, HEAD_DIM), jnp.float32), value_bias.reshape(HEADS, HEAD_DIM)], axis=1
    ).reshape(1, 2 * width)

    packed = project(inputs, first_pack, query_bias[None, :], pair_bias)
    at_head = to_heads(packed, count, 0)
    context_out, qa, ka, va, sums = attend(meta, block_order, at_head)
    context_out, later_fetched = lax.optimization_barrier((context_out, later_fetched))
    out_weight, up_weight, down_weight = (
        gather_rows(block, half_block) for block, half_block in zip(later_shards, later_fetched)
    )
    context_in = to_rows(context_out, count, 1)
    context_low = (
        context_in.reshape(HEADS, half, 2, HEAD_DIM).transpose(2, 1, 0, 3).reshape(tok_rows, width)
    )

    attn_out = jnp.dot(context_low, out_weight, preferred_element_type=jnp.float32) + out_bias
    h_one = inputs.astype(jnp.float32) + attn_out
    norm_one, norm_one_back = jax.vjp(layer_norm, h_one, gain_first, shift_first)
    norm_low = norm_one.astype(low_type)
    up_pre = jnp.dot(norm_low, up_weight, preferred_element_type=jnp.float32) + up_bias
    gelu_out, gelu_back = jax.vjp(partial(jax.nn.gelu, approximate=False), up_pre)
    gelu_low = gelu_out.astype(low_type)
    down_out = jnp.dot(gelu_low, down_weight, preferred_element_type=jnp.float32) + down_bias
    h_two = norm_one + down_out
    result, norm_two_back = jax.vjp(layer_norm, h_two, gain_second, shift_second)
    activations = result.astype(low_type)[None]
    valid = (own_seg < 3).astype(jnp.float32)
    g_out = cotangent[0].astype(jnp.float32) * valid[:, None]
    d_htwo, grad_gain_second, grad_shift_second = norm_two_back(g_out)
    d_down = d_htwo.astype(low_type)
    d_gelu = jnp.einsum("td,fd->tf", d_down, down_weight, preferred_element_type=jnp.float32)
    (d_uppre,) = gelu_back(d_gelu)
    d_up = d_uppre.astype(low_type)
    d_yone = d_htwo + jnp.einsum("tf,df->td", d_up, up_weight, preferred_element_type=jnp.float32)
    d_hone, grad_gain_first, grad_shift_first = norm_one_back(d_yone)
    d_attn = d_hone.astype(low_type)
    d_context = jnp.einsum("td,cd->tc", d_attn, out_weight, preferred_element_type=jnp.float32)
    context_back = (
        d_context.astype(low_type)
        .reshape(2, half, HEADS, HEAD_DIM)
        .transpose(2, 1, 0, 3)
        .reshape(HEADS, half, LANES)
    )

    grad_wdown = jnp.einsum("tf,td->fd", gelu_low, d_down, preferred_element_type=jnp.float32)
    grad_wup = jnp.einsum("td,tf->df", norm_low, d_up, preferred_element_type=jnp.float32)
    grad_wout = jnp.einsum("tc,td->cd", context_low, d_attn, preferred_element_type=jnp.float32)
    up_bias_sums = jnp.sum(d_up.astype(jnp.float32), axis=0)
    lanes = 2 * LANES
    vec_block = jnp.concatenate(
        [
            jnp.stack(
                [
                    jnp.sum(d_attn.astype(jnp.float32), axis=0),
                    grad_gain_first,
                    grad_shift_first,
                    jnp.sum(d_down.astype(jnp.float32), axis=0),
                    grad_gain_second,
                    grad_shift_second,
                ],
                axis=1,
            ),
            up_bias_sums.reshape(width // shard, 4, shard).transpose(0, 2, 1).reshape(width, 4),
        ],
        axis=1,
    ).astype(low_type)
    out_block = jnp.concatenate(
        [grad_wout.astype(low_type), jnp.pad(vec_block, ((0, 0), (0, lanes - 10)))], axis=1
    )
    up_block = grad_wup.astype(low_type)
    down_block = grad_wdown.astype(low_type)
    def add_low(mine, given):
        return (mine.astype(jnp.float32) + given.astype(jnp.float32)).astype(low_type)

    def core_halves(block):
        view = block.reshape(2, 2, -1, block.shape[1])
        keep = lax.dynamic_index_in_dim(view, core, 1, keepdims=False)
        give = lax.dynamic_index_in_dim(view, 1 - core, 1, keepdims=False)
        return keep, lax.ppermute(give, "ctx", [(k, k ^ 1) for k in range(count)])

    def wa_halves(block):
        keep = lax.dynamic_index_in_dim(block, wa, 0, keepdims=False)
        give = lax.dynamic_index_in_dim(block, 1 - wa, 0, keepdims=False)
        return keep, lax.ppermute(give, "wa", [(0, 1), (1, 0)])

    context_back, down_block, out_block, up_block = lax.optimization_barrier(
        (context_back, down_block, out_block, up_block)
    )
    if direct:
        halves = [core_halves(block) for block in (up_block, down_block)]
        back_at_head = to_heads(context_back, count, 2)
        back_at_head, halves = lax.optimization_barrier((back_at_head, halves))
        halves = [wa_halves(add_low(*pair)) for pair in halves]
        grads_out = attend_back(meta, block_order, back_at_head, qa, ka, va, sums)
        grads_out, halves = lax.optimization_barrier((grads_out, halves))
        early = [add_low(*pair) for pair in halves]
    else:
        back_at_head = to_heads(context_back, count, 2)
        grads_out = attend_back(meta, block_order, back_at_head, qa, ka, va, sums)
    grads_in = to_rows(grads_out, count, 3)

    d_pair = grads_in[:, :tok_rows, :].transpose(1, 0, 2).reshape(tok_rows, 2 * width)
    d_queries = (
        grads_in[:, tok_rows:, :]
        .reshape(HEADS, half, 2, HEAD_DIM)
        .transpose(2, 1, 0, 3)
        .reshape(tok_rows, width)
        * jnp.asarray(0.125, low_type)
    )
    d_all = jnp.concatenate(
        [d_queries, d_pair, jnp.zeros((tok_rows, lanes), low_type)], axis=1
    )
    grad_all = jnp.einsum("tc,td->cd", inputs, d_all, preferred_element_type=jnp.float32)
    d_values = d_pair.reshape(tok_rows, HEADS, 2, HEAD_DIM)[:, :, 1, :].reshape(tok_rows, width)
    last_block = lax.dynamic_update_slice(
        grad_all.astype(low_type),
        column_sums([d_queries.astype(jnp.float32), d_values.astype(jnp.float32)], lanes),
        (0, 3 * width),
    )
    if direct:
        up_sum, down_sum, last_sum, out_sum = grad_sum((*early, last_block, out_block), 4)
    else:
        up_sum, down_sum, last_sum, out_sum = (
            reduce_shards(block) for block in (up_block, down_block, last_block, out_block)
        )
    d_input = (
        d_hone
        + jnp.einsum("td,cd->tc", d_queries, query_weight, preferred_element_type=jnp.float32)
        + jnp.einsum("td,cd->tc", d_pair, pair_weight, preferred_element_type=jnp.float32)
    )
    input_grad = d_input.astype(low_type)[None]

    wide_grad = last_sum.astype(jnp.float32)
    pair_grad = wide_grad[:, width : 3 * width].reshape(shard, HEADS, 2, HEAD_DIM)
    out_grad = out_sum.astype(jnp.float32)
    return (
        activations,
        input_grad,
        wide_grad[:, :width],
        wide_grad[:, 3 * width],
        pair_grad[:, :, 0, :].reshape(shard, width),
        pair_grad[:, :, 1, :].reshape(shard, width),
        wide_grad[:, 3 * width + 1],
        out_grad[:, :width],
        out_grad[:, width],
        out_grad[:, width + 1],
        out_grad[:, width + 2],
        up_sum.astype(jnp.float32),
        out_grad[:, width + 6 : width + 10].T.reshape(-1),
        down_sum.astype(jnp.float32),
        out_grad[:, width + 3],
        out_grad[:, width + 4],
        out_grad[:, width + 5],
    )


def solution(mesh):
    placed = (
        P("wa", "ctx", None),
        P("wa", "ctx", None),
        P("wa", None),
        P(),
        P("wa", None),
        P("wa"),
        P("wa", None),
        P("wa", None),
        P("wa"),
        P("wa", None),
        P("wa"),
        P("wa"),
        P("wa"),
        P("wa", None),
        P("wa"),
        P("wa", None),
        P("wa"),
        P("wa"),
        P("wa"),
    )
    return jax.shard_map(
        partial(body, mesh.shape["ctx"]),
        mesh=mesh,
        in_specs=placed,
        out_specs=(
            P("wa", "ctx", None),
            P("wa", "ctx", None),
            P("wa", None),
            P("wa"),
            P("wa", None),
            P("wa", None),
            P("wa"),
            P("wa", None),
            P("wa"),
            P("wa"),
            P("wa"),
            P("wa", None),
            P("wa"),
            P("wa", None),
            P("wa"),
            P("wa"),
            P("wa"),
        ),
        check_vma=False,
    )
```

```python
from functools import partial

import jax
import jax.numpy as jnp
from jax import lax
from jax.experimental import pallas as pl
from jax.experimental.pallas import tpu as pltpu
from jax.sharding import PartitionSpec as P

HEADS = 12
HEAD_DIM = 64
LANES = 128
TILE = 512
FAR = -(2.0**40)
VMEM_BYTES = 60 << 20

low_type = jnp.bfloat16
epsilon = 1e-05


def dot_nt(left, right):
    return lax.dot_general(
        left, right, (((1,), (1,)), ((), ())), preferred_element_type=jnp.float32
    )


def dot_nn(left, right):
    return lax.dot_general(
        left, right, (((1,), (0,)), ((), ())), preferred_element_type=jnp.float32
    )


def layer_norm(hidden, gain_vec, shift_vec):
    centre = hidden - jnp.mean(hidden, axis=-1, keepdims=True)
    spread = jnp.mean(centre * centre, axis=-1, keepdims=True)
    return centre * lax.rsqrt(spread + epsilon) * gain_vec + shift_vec


def segment_of(position, seq_ends):
    return jnp.sum((position[:, None] >= seq_ends[None, :]).astype(jnp.int32), axis=1)


def owner_of(head, count):
    return head * count // HEADS


def greet_all(count, me):
    barrier = pltpu.get_barrier_semaphore()

    def greet(step, _):
        other = lax.rem(me + step, count)
        pl.semaphore_signal(
            barrier, inc=1, device_id={"ctx": other}, device_id_type=pl.DeviceIdType.MESH
        )
        return 0

    lax.fori_loop(1, count, greet, 0)
    pl.semaphore_wait(barrier, count - 1)


def to_heads_kernel(count, send_ref, recv_ref, send_sem, recv_sem, own_sem):
    me = lax.axis_index("ctx")
    greet_all(count, me)
    first = me * HEADS // count + 1

    def copy_for(head, source, owner):
        return pltpu.make_async_remote_copy(
            src_ref=send_ref.at[head],
            dst_ref=recv_ref.at[source],
            send_sem=send_sem.at[head],
            recv_sem=recv_sem.at[source],
            device_id={"ctx": owner},
            device_id_type=pl.DeviceIdType.MESH,
        )

    def own_copy(head):
        return pltpu.make_async_copy(send_ref.at[head], recv_ref.at[me], own_sem)

    def begin(step, _):
        head = lax.rem(first + step, HEADS)
        owner = owner_of(head, count)

        @pl.when(owner != me)
        def _():
            copy_for(head, me, owner).start()

        @pl.when(owner == me)
        def _():
            own_copy(head).start()

        return 0

    lax.fori_loop(0, HEADS, begin, 0)

    def finish(head, _):
        owner = owner_of(head, count)

        @pl.when(owner != me)
        def _():
            copy_for(head, me, owner).wait_send()

        @pl.when(owner == me)
        def _():
            own_copy(head).wait()

            def arrive(source, _):
                @pl.when(source != me)
                def _():
                    copy_for(head, source, owner).wait_recv()

                return 0

            lax.fori_loop(0, count, arrive, 0)

        return 0

    lax.fori_loop(0, HEADS, finish, 0)


def to_heads(send, count, collective_id):
    rows = send.shape[1]
    return pl.pallas_call(
        partial(to_heads_kernel, count),
        out_shape=jax.ShapeDtypeStruct((count, rows, LANES), low_type),
        in_specs=[pl.BlockSpec(memory_space=pltpu.VMEM)],
        out_specs=pl.BlockSpec(memory_space=pltpu.VMEM),
        scratch_shapes=[
            pltpu.SemaphoreType.DMA((HEADS,)),
            pltpu.SemaphoreType.DMA((count,)),
            pltpu.SemaphoreType.DMA,
        ],
        compiler_params=pltpu.CompilerParams(
            collective_id=collective_id, has_side_effects=True, vmem_limit_bytes=VMEM_BYTES
        ),
        cost_estimate=pl.CostEstimate(
            flops=rows * 250_000_000, bytes_accessed=send.size * 4, transcendentals=0
        ),
        name=f"to_heads_{rows}",
    )(send)


def to_rows_kernel(count, send_ref, recv_ref, send_sem, recv_sem, own_sem):
    me = lax.axis_index("ctx")
    greet_all(count, me)

    def copy_for(head, target):
        return pltpu.make_async_remote_copy(
            src_ref=send_ref.at[target],
            dst_ref=recv_ref.at[head],
            send_sem=send_sem.at[target],
            recv_sem=recv_sem.at[head],
            device_id={"ctx": target},
            device_id_type=pl.DeviceIdType.MESH,
        )

    def own_copy(head):
        return pltpu.make_async_copy(send_ref.at[me], recv_ref.at[head], own_sem)

    def begin(head, _):
        @pl.when(owner_of(head, count) == me)
        def _():
            own_copy(head).start()

            def push(step, _):
                copy_for(head, lax.rem(me + step, count)).start()
                return 0

            lax.fori_loop(1, count, push, 0)

        return 0

    lax.fori_loop(0, HEADS, begin, 0)

    def finish(head, _):
        @pl.when(owner_of(head, count) == me)
        def _():
            own_copy(head).wait()

            def leave(step, _):
                copy_for(head, lax.rem(me + step, count)).wait_send()
                return 0

            lax.fori_loop(1, count, leave, 0)

        @pl.when(owner_of(head, count) != me)
        def _():
            copy_for(head, me).wait_recv()

        return 0

    lax.fori_loop(0, HEADS, finish, 0)


def to_rows(send, count, collective_id):
    rows = send.shape[1]
    return pl.pallas_call(
        partial(to_rows_kernel, count),
        out_shape=jax.ShapeDtypeStruct((HEADS, rows, LANES), low_type),
        in_specs=[pl.BlockSpec(memory_space=pltpu.VMEM)],
        out_specs=pl.BlockSpec(memory_space=pltpu.VMEM),
        scratch_shapes=[
            pltpu.SemaphoreType.DMA((count,)),
            pltpu.SemaphoreType.DMA((HEADS,)),
            pltpu.SemaphoreType.DMA,
        ],
        compiler_params=pltpu.CompilerParams(
            collective_id=collective_id, has_side_effects=True, vmem_limit_bytes=VMEM_BYTES
        ),
        cost_estimate=pl.CostEstimate(
            flops=rows * 250_000_000, bytes_accessed=send.size * 4, transcendentals=0
        ),
        name=f"to_rows_{rows}",
    )(send)


def project_kernel(x_ref, pack_ref, vec_ref, out_ref):
    rows, width = x_ref.shape
    half = rows // 2
    step = 4
    for base in range(0, HEADS, step):
        cols = slice(base * LANES, (base + step) * LANES)
        both = dot_nn(x_ref[...], pack_ref[:, width + cols.start : width + cols.stop])
        bias = vec_ref[1:2, base * HEAD_DIM : (base + step) * HEAD_DIM]
        blank = jnp.zeros((1, HEAD_DIM), jnp.float32)
        shifts = []
        for at in range(step):
            shifts += [blank, bias[:, at * HEAD_DIM : (at + 1) * HEAD_DIM]]
        both = (both + jnp.concatenate(shifts, axis=1)).astype(low_type)
        for at in range(step):
            out_ref[base + at, 0:rows, :] = both[:, at * LANES : (at + 1) * LANES]
        cols = slice(base * HEAD_DIM, (base + step) * HEAD_DIM)
        query = ((dot_nn(x_ref[...], pack_ref[:, cols]) + vec_ref[0:1, cols]) * 0.125).astype(low_type)
        for at in range(step):
            lanes = slice(at * HEAD_DIM, (at + 1) * HEAD_DIM)
            out_ref[base + at, rows : rows + half, :] = jnp.concatenate(
                [query[:half, lanes], query[half:, lanes]], axis=1
            )


def project(x, pack, vectors):
    rows = x.shape[0]
    vmem = pl.BlockSpec(memory_space=pltpu.VMEM)
    return pl.pallas_call(
        project_kernel,
        out_shape=jax.ShapeDtypeStruct((HEADS, rows + rows // 2, LANES), low_type),
        in_specs=[vmem] * 3,
        out_specs=vmem,
        compiler_params=pltpu.CompilerParams(vmem_limit_bytes=VMEM_BYTES),
        name="project",
    )(x, pack, vectors)


def tile_range(meta_ref, first, last, total):
    end_a, end_b, end_c = meta_ref[0], meta_ref[1], meta_ref[2]
    low = jnp.where(
        first >= end_c, end_c, jnp.where(first >= end_b, end_b, jnp.where(first >= end_a, end_a, 0))
    )
    high = jnp.where(
        last >= end_c,
        total,
        jnp.where(last >= end_b, end_c, jnp.where(last >= end_a, end_b, end_a)),
    )
    return low // TILE, (high + TILE - 1) // TILE


def attend_kernel(meta_ref, order_ref, recv_ref, out_ref, qa_ref, ka_ref, va_ref, sum_ref):
    count = recv_ref.shape[0]
    half = recv_ref.shape[1] // 3
    total = qa_ref.shape[0]

    @pl.when(meta_ref[3] == 1)
    def _():
        lane = lax.broadcasted_iota(jnp.int32, (half, LANES), 1)
        lower = lane < HEAD_DIM
        row = lax.broadcasted_iota(jnp.int32, (half, LANES), 0)

        def place(source, _):
            query = recv_ref[source, 2 * half :, :].astype(jnp.float32)
            for part in range(2):
                first = pl.multiple_of(order_ref[2 * source + part] * half, half)
                position = first + row
                segment = (
                    (position >= meta_ref[0]).astype(jnp.int32)
                    + (position >= meta_ref[1]).astype(jnp.int32)
                    + (position >= meta_ref[2]).astype(jnp.int32)
                )
                mine = (lane - HEAD_DIM) == segment
                other = (lane < HEAD_DIM + 4) & (~mine)
                pair = recv_ref[source, part * half : (part + 1) * half, :].astype(jnp.float32)
                if part == 1:
                    query = pltpu.roll(query, HEAD_DIM, 1)
                mark_k = jnp.where(
                    other, FAR, jnp.where((lane >= HEAD_DIM + 4) & (lane < HEAD_DIM + 7), 1.0, 0.0)
                )
                rows = pl.ds(first, half)
                qa_ref[rows, :] = jnp.where(lower, query, jnp.where(mine, 1.0, 0.0)).astype(low_type)
                ka_ref[rows, :] = jnp.where(lower, pair, mark_k).astype(low_type)
                va_ref[rows, :] = jnp.where(lower, 1.0, pair).astype(low_type)
            return 0

        lax.fori_loop(0, count, place, 0)

        def query_step(index, _):
            first = pl.multiple_of(index * TILE, TILE)
            rows = pl.ds(first, TILE)
            begin, end = tile_range(meta_ref, first, first + TILE - 1, total)
            query = qa_ref[rows, :]
            sum_ref[rows, :] = jnp.zeros((TILE, LANES), jnp.float32)

            def key_step(key_index, _):
                keys = pl.ds(pl.multiple_of(key_index * TILE, TILE), TILE)
                expo = jnp.exp(dot_nt(query, ka_ref[keys, :])).astype(low_type)
                sum_ref[rows, :] += dot_nn(expo, va_ref[keys, :])
                return 0

            lax.fori_loop(begin, end, key_step, 0)
            return 0

        lax.fori_loop(0, total // TILE, query_step, 0)

        def give(source, _):
            parts = []
            for part in range(2):
                first = pl.multiple_of(order_ref[2 * source + part] * half, half)
                block = sum_ref[pl.ds(first, half), :]
                parts.append((block, pltpu.roll(block, HEAD_DIM, 1)))
            top = jnp.where(lower, parts[0][1], parts[1][0])
            bottom = jnp.where(lower, parts[0][0], parts[1][1])
            out_ref[source] = (top / bottom).astype(low_type)
            return 0

        lax.fori_loop(0, count, give, 0)


def attend(meta, order, recv):
    count, rows, _ = recv.shape
    total = count * rows * 2 // 3
    vmem = pl.BlockSpec(memory_space=pltpu.VMEM)
    smem = pl.BlockSpec(memory_space=pltpu.SMEM)
    whole = jax.ShapeDtypeStruct((total, LANES), low_type)
    return pl.pallas_call(
        attend_kernel,
        out_shape=(
            jax.ShapeDtypeStruct((count, rows // 3, LANES), low_type),
            whole,
            whole,
            whole,
            jax.ShapeDtypeStruct((total, LANES), jnp.float32),
        ),
        in_specs=[smem, smem, vmem],
        out_specs=(vmem,) * 5,
        compiler_params=pltpu.CompilerParams(vmem_limit_bytes=VMEM_BYTES),
        cost_estimate=pl.CostEstimate(
            flops=total * total * LANES * 8, bytes_accessed=total * LANES * 12, transcendentals=0
        ),
        name="attend",
    )(meta, order, recv)


def split_three(value):
    first = value.astype(low_type).astype(jnp.float32)
    rest = value - first
    second = rest.astype(low_type).astype(jnp.float32)
    return first, second, rest - second


def attend_back_kernel(
    meta_ref,
    order_ref,
    recv_ref,
    qa_ref,
    ka_ref,
    va_ref,
    sum_ref,
    out_ref,
    qb_ref,
    da_ref,
    kt_ref,
    dkv_ref,
    dq_ref,
    acc_ref,
):
    count = recv_ref.shape[0]
    half = recv_ref.shape[1]
    total = qa_ref.shape[0]

    @pl.when(meta_ref[3] == 1)
    def _():
        lane = lax.broadcasted_iota(jnp.int32, (half, LANES), 1)
        lower = lane < HEAD_DIM

        def place(source, _):
            given = recv_ref[source].astype(jnp.float32)
            for part in range(2):
                first = pl.multiple_of(order_ref[2 * source + part] * half, half)
                rows = pl.ds(first, half)
                block = sum_ref[rows, :]
                turned = pltpu.roll(block, HEAD_DIM, 1)
                d_context = pltpu.roll(given, HEAD_DIM, 1) if part == 0 else given
                product = jnp.where(lower, 0.0, d_context * (block / turned))
                minus = -jnp.sum(product, axis=1, keepdims=True)
                one, two, three = split_three(minus)
                mark = jnp.where(
                    lane == 0, one, jnp.where(lane == 1, two, jnp.where(lane == 2, three, 0.0))
                )
                da_ref[rows, :] = jnp.where(lower, mark, d_context).astype(low_type)
                one, two, three = split_three(-jnp.log(turned))
                at = lane - (HEAD_DIM + 4)
                mark = jnp.where(at == 0, one, jnp.where(at == 1, two, three))
                query = qa_ref[rows, :].astype(jnp.float32)
                qb_ref[rows, :] = jnp.where((at >= 0) & (at < 3), mark, query).astype(low_type)
            return 0

        lax.fori_loop(0, count, place, 0)

        def prepare(index, _):
            rows = pl.ds(pl.multiple_of(index * TILE, TILE), TILE)
            kt_ref[:, rows] = jnp.transpose(ka_ref[rows, :])[:HEAD_DIM, :]
            dkv_ref[rows, :] = jnp.zeros((TILE, LANES), jnp.float32)
            return 0

        lax.fori_loop(0, total // TILE, prepare, 0)

        lower_tile = lax.broadcasted_iota(jnp.int32, (TILE, LANES), 1) < HEAD_DIM

        def query_step(index, _):
            first = pl.multiple_of(index * TILE, TILE)
            rows = pl.ds(first, TILE)
            begin, end = tile_range(meta_ref, first, first + TILE - 1, total)
            query = qb_ref[rows, :]
            given = da_ref[rows, :]
            query_only = jnp.where(lower_tile, query.astype(jnp.float32), 0.0).astype(low_type)
            given_only = jnp.where(lower_tile, 0.0, given.astype(jnp.float32)).astype(low_type)
            acc_ref[...] = jnp.zeros_like(acc_ref)

            def key_step(key_index, _):
                keys = pl.ds(pl.multiple_of(key_index * TILE, TILE), TILE)
                prob = jnp.exp(dot_nt(ka_ref[keys, :], query))
                d_scores = (prob * dot_nt(va_ref[keys, :], given)).astype(low_type)
                dkv_ref[keys, :] += dot_nn(d_scores, query_only) + dot_nn(
                    prob.astype(low_type), given_only
                )
                acc_ref[...] += dot_nn(kt_ref[:, keys], d_scores)
                return 0

            lax.fori_loop(begin, end, key_step, 0)
            dq_ref[rows, :] = jnp.transpose(acc_ref[...])
            return 0

        lax.fori_loop(0, total // TILE, query_step, 0)

        def give(source, _):
            queries = []
            for part in range(2):
                first = pl.multiple_of(order_ref[2 * source + part] * half, half)
                rows = pl.ds(first, half)
                out_ref[source, part * half : (part + 1) * half, :] = dkv_ref[rows, :].astype(low_type)
                queries.append(dq_ref[rows, :])
            out_ref[source, 2 * half :, :] = jnp.concatenate(queries, axis=1).astype(low_type)
            return 0

        lax.fori_loop(0, count, give, 0)


def attend_back(meta, order, recv, qa, ka, va, sums):
    count, half, _ = recv.shape
    total = qa.shape[0]
    vmem = pl.BlockSpec(memory_space=pltpu.VMEM)
    smem = pl.BlockSpec(memory_space=pltpu.SMEM)
    return pl.pallas_call(
        attend_back_kernel,
        out_shape=jax.ShapeDtypeStruct((count, 3 * half, LANES), low_type),
        in_specs=[smem, smem] + [vmem] * 5,
        out_specs=vmem,
        scratch_shapes=[
            pltpu.VMEM((total, LANES), low_type),
            pltpu.VMEM((total, LANES), low_type),
            pltpu.VMEM((HEAD_DIM, total), low_type),
            pltpu.VMEM((total, LANES), jnp.float32),
            pltpu.VMEM((total, HEAD_DIM), jnp.float32),
            pltpu.VMEM((HEAD_DIM, TILE), jnp.float32),
        ],
        compiler_params=pltpu.CompilerParams(vmem_limit_bytes=VMEM_BYTES),
        cost_estimate=pl.CostEstimate(
            flops=total * total * LANES * 16, bytes_accessed=total * LANES * 16, transcendentals=0
        ),
        name="attend_back",
    )(meta, order, recv, qa, ka, va, sums)


PART_ORDERS = (("x", "z"), ("x", "z"), ("wa", "x", "z"), ("wa", "x", "z"))
GATHER_ORDERS = (("z", "x"), ("z", "x"), ("z", "x"), ("x", "z"))
PARTS = len(PART_ORDERS)
EARLY = sum(len(order) == 2 for order in PART_ORDERS)
STAGES = sum(len(order) for order in PART_ORDERS)
SIZES = {"wa": 2, "x": 2, "z": 4}


class Links:
    def __init__(self):
        me = lax.axis_index("ctx")
        self.at = {
            "core": lax.rem(me, 2),
            "x": lax.rem(me // 2, 2),
            "z": me // 4,
            "wa": lax.axis_index("wa"),
        }

    def peer(self, axis, value):
        at = dict(self.at)
        at[axis] = value
        return {"ctx": at["z"] * 4 + at["x"] * 2 + at["core"], "wa": at["wa"]}


def splits_rows(piece):
    return piece % 64 == 0


def grad_sum_kernel(*refs):
    refs = list(refs)
    sizes = (PARTS, PARTS, PARTS - EARLY, STAGES)
    g_refs, out_refs, core_bufs, bufs = (
        [refs.pop(0) for _ in range(number)] for number in sizes
    )
    core_bufs = [None] * EARLY + core_bufs
    send_sem, recv_sem = refs
    links = Links()
    core, x, z, wa = (links.at[name] for name in ("core", "x", "z", "wa"))
    barrier = pltpu.get_barrier_semaphore()
    peers = [links.peer("core", 1 - core), links.peer("x", 1 - x), links.peer("wa", 1 - wa)]
    peers += [links.peer("z", lax.rem(z + step, 4)) for step in range(1, 4)]
    for peer in peers:
        pl.semaphore_signal(barrier, inc=1, device_id=peer, device_id_type=pl.DeviceIdType.MESH)
    pl.semaphore_wait(barrier, len(peers))
    used = [0]

    def remote(src, dst, peer):
        index = used[0]
        used[0] += 1
        copy = pltpu.make_async_remote_copy(
            src_ref=src,
            dst_ref=dst,
            send_sem=send_sem.at[index],
            recv_sem=recv_sem.at[index],
            device_id=peer,
            device_id_type=pl.DeviceIdType.MESH,
        )
        copy.start()
        return copy

    def z_share(ref, value):
        piece, width = ref.shape[-2:]
        if value is None:
            return slice(None), slice(None)
        if splits_rows(piece):
            return pl.ds(pl.multiple_of(value * (piece // 4), 16), piece // 4), slice(None)
        return slice(None), pl.ds(pl.multiple_of(value * (width // 4), LANES), width // 4)

    def slab(part, held, axis=None, value=None):
        at = dict(links.at)
        if axis is not None:
            at[axis] = value
            held = held | {axis}
        return g_refs[part].at[
            pl.ds(0, 1) if part < EARLY else pl.ds(at["wa"], 1) if "wa" in held else pl.ds(0, 2),
            0 if part < EARLY else core,
            pl.ds(at["x"], 1) if "x" in held else pl.ds(0, 2),
            *z_share(g_refs[part], at["z"] if "z" in held else None),
        ]

    def add_into(target, sources):
        outer, inner, rows, _ = target.shape
        for a in range(outer):
            for b in range(inner):

                def add(group, _):
                    some = pl.ds(pl.multiple_of(group * 16, 16), 16)
                    total = target[a, b, some, :].astype(jnp.float32)
                    for source in sources:
                        total = total + source[a, b, some, :].astype(jnp.float32)
                    target[a, b, some, :] = total.astype(low_type)
                    return 0

                lax.fori_loop(0, rows // 16, add, 0)

    core_copies = [
        remote(g_refs[part].at[:, 1 - core], core_bufs[part], links.peer("core", 1 - core))
        if part >= EARLY
        else None
        for part in range(PARTS)
    ]
    first_buf = [sum(len(order) for order in PART_ORDERS[:part]) for part in range(PARTS)]

    def begin(part, stage):
        axis = PART_ORDERS[part][stage]
        held = set(PART_ORDERS[part][:stage])
        buf = bufs[first_buf[part] + stage]
        copies = []
        for step in range(1, SIZES[axis]):
            value = lax.rem(links.at[axis] + step, SIZES[axis])
            copies.append(
                remote(slab(part, held, axis, value), buf.at[step - 1], links.peer(axis, value))
            )
        return copies

    def out_slab(part, held):
        return out_refs[part].at[
            core,
            pl.ds(x, 1) if "x" in held else pl.ds(0, 2),
            *z_share(out_refs[part], z if "z" in held else None),
        ]

    def spread(part, stage):
        axis = GATHER_ORDERS[part][stage]
        block = out_slab(part, set(GATHER_ORDERS[part][stage:]))
        return [
            remote(block, block, links.peer(axis, lax.rem(links.at[axis] + step, SIZES[axis])))
            for step in range(1, SIZES[axis])
        ]

    def start_gather(part, stage):
        if stage < 2:
            return spread(part, stage)
        block = out_slab(part, set())
        return [remote(block, block, links.peer("core", 1 - core))]

    flying, passed = {}, {}
    for part in range(PARTS):
        passed[part] = 0 if part >= EARLY else 1
        flying[part] = begin(part, 0) if part < EARLY else [core_copies[part]]
    while any(flying.values()):
        for part in range(PARTS):
            if not flying[part]:
                continue
            order = PART_ORDERS[part]
            for copy in flying[part]:
                copy.wait()
            step = passed[part]
            passed[part] += 1
            if step == 0:
                add_into(slab(part, set()), [core_bufs[part]])
            elif step <= len(order):
                buf = bufs[first_buf[part] + step - 1]
                add_into(
                    slab(part, set(order[:step])),
                    [buf.at[at] for at in range(SIZES[order[step - 1]] - 1)],
                )
            if step < len(order):
                flying[part] = begin(part, step)
            elif step == len(order):
                out_slab(part, {"x", "z"})[...] = slab(part, {"wa", "x", "z"})[0]
                flying[part] = start_gather(part, 0)
            elif step <= len(order) + 2:
                flying[part] = start_gather(part, step - len(order))
            else:
                flying[part] = None


def grad_sum(grads, collective_id):
    bufs, core_bufs, outs, given = [], [], [], []
    for part, grad in enumerate(grads):
        rows, width = grad.shape
        early = part < EARLY
        piece = rows // 2 if early else rows // 8
        shape = {"wa": 1 if early else 2, "x": 2, "z": 4}
        for axis in PART_ORDERS[part]:
            shape[axis] //= SIZES[axis]
            share = (
                (piece * shape["z"] // 4, width)
                if splits_rows(piece)
                else (piece, width * shape["z"] // 4)
            )
            bufs.append(
                pltpu.VMEM((SIZES[axis] - 1, shape["wa"], shape["x"], *share), low_type)
            )
        if not early:
            core_bufs.append(pltpu.VMEM((2, 2, piece, width), low_type))
        outs.append(jax.ShapeDtypeStruct((2, 2, piece, width), low_type))
        lead = (1, 1) if early else (2, 2)
        given.append(grad.reshape(*lead, 2, piece, width))
    vmem = pl.BlockSpec(memory_space=pltpu.VMEM)
    size = sum(grad.size for grad in grads)
    sums = pl.pallas_call(
        grad_sum_kernel,
        out_shape=tuple(outs),
        in_specs=[vmem] * PARTS,
        out_specs=(vmem,) * PARTS,
        scratch_shapes=[
            *core_bufs,
            *bufs,
            pltpu.SemaphoreType.DMA((16 * PARTS,)),
            pltpu.SemaphoreType.DMA((16 * PARTS,)),
        ],
        compiler_params=pltpu.CompilerParams(
            collective_id=collective_id, has_side_effects=True, vmem_limit_bytes=VMEM_BYTES
        ),
        cost_estimate=pl.CostEstimate(
            flops=size * 20_000, bytes_accessed=size * 4, transcendentals=0
        ),
        name="grad_sum",
    )(*given)
    return [part.reshape(-1, part.shape[-1]) for part in sums]


def column_sums(terms, lanes):
    block = jnp.stack([jnp.sum(term, axis=0) for term in terms], axis=1).astype(low_type)
    return jnp.pad(block, ((0, 0), (0, lanes - len(terms))))


def reduce_shards(grad):
    part = lax.psum_scatter(
        grad.astype(low_type), ("wa", "ctx"), scatter_dimension=0, tiled=True
    )
    return lax.all_gather(part, "ctx", axis=0, tiled=True)


def body(
    count,
    tokens,
    cotangent,
    lengths,
    block_order,
    w_query,
    b_query,
    w_key,
    w_value,
    b_value,
    w_out,
    b_out,
    gain_one,
    shift_one,
    w_up,
    b_up,
    w_down,
    b_down,
    gain_two,
    shift_two,
):
    inputs = tokens[0]
    tok_rows, width = inputs.shape
    wide = w_up.shape[1]
    half = tok_rows // 2
    shard = w_query.shape[0]
    direct = count == 16 and width == 2 * shard and shard % 64 == 0 and wide == 4 * width
    me = lax.axis_index("ctx")
    seq_ends = jnp.cumsum(lengths[0])
    own_blocks = lax.dynamic_slice(block_order, (2 * me,), (2,))
    position = (own_blocks[:, None] * half + jnp.arange(half, dtype=jnp.int32)[None, :]).reshape(-1)
    own_seg = segment_of(position, seq_ends)
    owns = jnp.any(me == jnp.arange(HEADS, dtype=jnp.int32) * count // HEADS).astype(jnp.int32)
    meta = jnp.concatenate([seq_ends.astype(jnp.int32), owns[None]])

    core = me % 2
    wa = lax.axis_index("wa")

    def fetch_half(shard_block, after=None):
        if not direct:
            return None
        if after is not None:
            shard_block, _ = lax.optimization_barrier((shard_block, after))
        size, columns = shard_block.shape
        part = lax.dynamic_slice(shard_block, (core * (size // 2), 0), (size // 2, columns))
        return lax.ppermute(part, "wa", [(0, 1), (1, 0)])

    def gather_rows(shard_block, fetched):
        if not direct:
            return lax.all_gather(shard_block, "wa", axis=0, tiled=True)
        size, columns = shard_block.shape
        swapped = lax.ppermute(fetched, "ctx", [(k, k ^ 1) for k in range(count)])
        other = (1 - wa) * size
        whole = jnp.zeros((2 * size, columns), shard_block.dtype)
        whole = lax.dynamic_update_slice(whole, shard_block, (wa * size, 0))
        whole = lax.dynamic_update_slice(whole, fetched, (other + core * (size // 2), 0))
        return lax.dynamic_update_slice(whole, swapped, (other + (1 - core) * (size // 2), 0))

    pair = jnp.stack(
        [
            w_key.astype(low_type).reshape(shard, HEADS, HEAD_DIM),
            w_value.astype(low_type).reshape(shard, HEADS, HEAD_DIM),
        ],
        axis=2,
    ).reshape(shard, 2 * width)
    own_vectors = jnp.concatenate(
        [
            jnp.stack(
                [b_query, b_value, b_out, gain_one, shift_one, gain_two, shift_two, b_down]
            ),
            b_up.reshape(4, shard),
            jnp.zeros((4, shard), jnp.float32),
        ],
        axis=0,
    ).astype(low_type)
    if direct:
        other_vectors = lax.ppermute(own_vectors, "wa", [(0, 1), (1, 0)])
        vector_rows = jnp.where(
            wa == 0,
            jnp.concatenate([own_vectors, other_vectors], axis=1),
            jnp.concatenate([other_vectors, own_vectors], axis=1),
        ).astype(jnp.float32)
    else:
        vector_rows = (
            lax.all_gather(own_vectors, "wa", axis=1, tiled=True)
        ).astype(jnp.float32)

    first_shard = jnp.concatenate([w_query.astype(low_type), pair], axis=1)
    fetched = fetch_half(first_shard)
    later_shards = (
        w_out.astype(low_type),
        w_up.astype(low_type),
        w_down.astype(low_type),
    )
    later_fetched = tuple(fetch_half(block, fetched) for block in later_shards)
    first_pack = gather_rows(first_shard, fetched)
    query_weight = first_pack[:, :width]
    pair_weight = first_pack[:, width : 3 * width]
    out_bias, gain_first, shift_first, gain_second, shift_second, down_bias = (
        vector_rows[index] for index in range(2, 8)
    )
    up_bias = (
        vector_rows[8:12].reshape(4, width // shard, shard).transpose(1, 0, 2).reshape(-1)
    )

    packed = project(inputs, first_pack, vector_rows)
    at_head = to_heads(packed, count, 0)
    context_out, qa, ka, va, sums = attend(meta, block_order, at_head)
    context_out, later_fetched = lax.optimization_barrier((context_out, later_fetched))
    out_weight, up_weight, down_weight = (
        gather_rows(block, half_block) for block, half_block in zip(later_shards, later_fetched)
    )
    context_in = to_rows(context_out, count, 1)
    context_low = (
        context_in.reshape(HEADS, half, 2, HEAD_DIM).transpose(2, 1, 0, 3).reshape(tok_rows, width)
    )

    attn_out = jnp.dot(context_low, out_weight, preferred_element_type=jnp.float32) + out_bias
    h_one = inputs.astype(jnp.float32) + attn_out
    norm_one, norm_one_back = jax.vjp(layer_norm, h_one, gain_first, shift_first)
    norm_low = norm_one.astype(low_type)
    up_pre = jnp.dot(norm_low, up_weight, preferred_element_type=jnp.float32) + up_bias
    gelu_out, gelu_back = jax.vjp(partial(jax.nn.gelu, approximate=False), up_pre)
    gelu_low = gelu_out.astype(low_type)
    down_out = jnp.dot(gelu_low, down_weight, preferred_element_type=jnp.float32) + down_bias
    h_two = norm_one + down_out
    result, norm_two_back = jax.vjp(layer_norm, h_two, gain_second, shift_second)
    activations = result.astype(low_type)[None]
    valid = (own_seg < 3).astype(jnp.float32)
    g_out = cotangent[0].astype(jnp.float32) * valid[:, None]
    d_htwo, grad_gain_second, grad_shift_second = norm_two_back(g_out)
    d_down = d_htwo.astype(low_type)
    d_gelu = jnp.einsum("td,fd->tf", d_down, down_weight, preferred_element_type=jnp.float32)
    (d_uppre,) = gelu_back(d_gelu)
    d_up = d_uppre.astype(low_type)
    d_yone = d_htwo + jnp.einsum("tf,df->td", d_up, up_weight, preferred_element_type=jnp.float32)
    d_hone, grad_gain_first, grad_shift_first = norm_one_back(d_yone)
    d_attn = d_hone.astype(low_type)
    d_context = jnp.einsum("td,cd->tc", d_attn, out_weight, preferred_element_type=jnp.float32)
    context_back = (
        d_context.astype(low_type)
        .reshape(2, half, HEADS, HEAD_DIM)
        .transpose(2, 1, 0, 3)
        .reshape(HEADS, half, LANES)
    )

    grad_wdown = jnp.einsum("tf,td->fd", gelu_low, d_down, preferred_element_type=jnp.float32)
    grad_wup = jnp.einsum("td,tf->df", norm_low, d_up, preferred_element_type=jnp.float32)
    grad_wout = jnp.einsum("tc,td->cd", context_low, d_attn, preferred_element_type=jnp.float32)
    up_bias_sums = jnp.sum(d_up.astype(jnp.float32), axis=0)
    lanes = 2 * LANES
    vec_block = jnp.concatenate(
        [
            jnp.stack(
                [
                    jnp.sum(d_attn.astype(jnp.float32), axis=0),
                    grad_gain_first,
                    grad_shift_first,
                    jnp.sum(d_down.astype(jnp.float32), axis=0),
                    grad_gain_second,
                    grad_shift_second,
                ],
                axis=1,
            ),
            up_bias_sums.reshape(width // shard, 4, shard).transpose(0, 2, 1).reshape(width, 4),
        ],
        axis=1,
    ).astype(low_type)
    out_block = jnp.concatenate(
        [grad_wout.astype(low_type), jnp.pad(vec_block, ((0, 0), (0, lanes - 10)))], axis=1
    )
    up_block = grad_wup.astype(low_type)
    down_block = grad_wdown.astype(low_type)
    def add_low(mine, given):
        return (mine.astype(jnp.float32) + given.astype(jnp.float32)).astype(low_type)

    def core_halves(block):
        view = block.reshape(2, 2, -1, block.shape[1])
        keep = lax.dynamic_index_in_dim(view, core, 1, keepdims=False)
        give = lax.dynamic_index_in_dim(view, 1 - core, 1, keepdims=False)
        return keep, lax.ppermute(give, "ctx", [(k, k ^ 1) for k in range(count)])

    def wa_halves(block):
        keep = lax.dynamic_index_in_dim(block, wa, 0, keepdims=False)
        give = lax.dynamic_index_in_dim(block, 1 - wa, 0, keepdims=False)
        return keep, lax.ppermute(give, "wa", [(0, 1), (1, 0)])

    context_back, down_block, out_block, up_block = lax.optimization_barrier(
        (context_back, down_block, out_block, up_block)
    )
    if direct:
        halves = [core_halves(block) for block in (up_block, down_block)]
        back_at_head = to_heads(context_back, count, 2)
        back_at_head, halves = lax.optimization_barrier((back_at_head, halves))
        halves = [wa_halves(add_low(*pair)) for pair in halves]
        grads_out = attend_back(meta, block_order, back_at_head, qa, ka, va, sums)
        grads_out, halves = lax.optimization_barrier((grads_out, halves))
        early = [add_low(*pair) for pair in halves]
    else:
        back_at_head = to_heads(context_back, count, 2)
        grads_out = attend_back(meta, block_order, back_at_head, qa, ka, va, sums)
    grads_in = to_rows(grads_out, count, 3)

    d_pair = grads_in[:, :tok_rows, :].transpose(1, 0, 2).reshape(tok_rows, 2 * width)
    d_queries = (
        grads_in[:, tok_rows:, :]
        .reshape(HEADS, half, 2, HEAD_DIM)
        .transpose(2, 1, 0, 3)
        .reshape(tok_rows, width)
        * jnp.asarray(0.125, low_type)
    )
    d_keys, d_values = (
        grads_in[:, :tok_rows, low : low + HEAD_DIM].transpose(1, 0, 2).reshape(tok_rows, width)
        for low in (0, HEAD_DIM)
    )
    d_all = jnp.concatenate(
        [d_queries, d_keys, d_values, jnp.zeros((tok_rows, lanes), low_type)], axis=1
    )
    grad_all = jnp.einsum("tc,td->cd", inputs, d_all, preferred_element_type=jnp.float32)
    last_block = lax.dynamic_update_slice(
        grad_all.astype(low_type),
        column_sums([d_queries.astype(jnp.float32), d_values.astype(jnp.float32)], lanes),
        (0, 3 * width),
    )
    if direct:
        up_sum, down_sum, last_sum, out_sum = grad_sum((*early, last_block, out_block), 4)
    else:
        up_sum, down_sum, last_sum, out_sum = (
            reduce_shards(block) for block in (up_block, down_block, last_block, out_block)
        )
    d_input = (
        d_hone
        + jnp.einsum("td,cd->tc", d_queries, query_weight, preferred_element_type=jnp.float32)
        + jnp.einsum("td,cd->tc", d_pair, pair_weight, preferred_element_type=jnp.float32)
    )
    input_grad = d_input.astype(low_type)[None]

    wide_grad = last_sum.astype(jnp.float32)
    out_grad = out_sum.astype(jnp.float32)
    return (
        activations,
        input_grad,
        wide_grad[:, :width],
        wide_grad[:, 3 * width],
        wide_grad[:, width : 2 * width],
        wide_grad[:, 2 * width : 3 * width],
        wide_grad[:, 3 * width + 1],
        out_grad[:, :width],
        out_grad[:, width],
        out_grad[:, width + 1],
        out_grad[:, width + 2],
        up_sum.astype(jnp.float32),
        out_grad[:, width + 6 : width + 10].T.reshape(-1),
        down_sum.astype(jnp.float32),
        out_grad[:, width + 3],
        out_grad[:, width + 4],
        out_grad[:, width + 5],
    )


def solution(mesh):
    placed = (
        P("wa", "ctx", None),
        P("wa", "ctx", None),
        P("wa", None),
        P(),
        P("wa", None),
        P("wa"),
        P("wa", None),
        P("wa", None),
        P("wa"),
        P("wa", None),
        P("wa"),
        P("wa"),
        P("wa"),
        P("wa", None),
        P("wa"),
        P("wa", None),
        P("wa"),
        P("wa"),
        P("wa"),
    )
    return jax.shard_map(
        partial(body, mesh.shape["ctx"]),
        mesh=mesh,
        in_specs=placed,
        out_specs=(
            P("wa", "ctx", None),
            P("wa", "ctx", None),
            P("wa", None),
            P("wa"),
            P("wa", None),
            P("wa", None),
            P("wa"),
            P("wa", None),
            P("wa"),
            P("wa"),
            P("wa"),
            P("wa", None),
            P("wa"),
            P("wa", None),
            P("wa"),
            P("wa"),
            P("wa"),
        ),
        check_vma=False,
    )
```

```python
from functools import partial

import jax
import jax.numpy as jnp
from jax import lax
from jax.experimental import pallas as pl
from jax.experimental.pallas import tpu as pltpu
from jax.sharding import PartitionSpec as P

HEADS = 12
HEAD_DIM = 64
LANES = 128
TILE = 512
FAR = -(2.0**40)
VMEM_BYTES = 60 << 20

low_type = jnp.bfloat16
epsilon = 1e-05


def dot_nt(left, right):
    return lax.dot_general(
        left, right, (((1,), (1,)), ((), ())), preferred_element_type=jnp.float32
    )


def dot_nn(left, right):
    return lax.dot_general(
        left, right, (((1,), (0,)), ((), ())), preferred_element_type=jnp.float32
    )


def layer_norm(hidden, gain_vec, shift_vec):
    centre = hidden - jnp.mean(hidden, axis=-1, keepdims=True)
    spread = jnp.mean(centre * centre, axis=-1, keepdims=True)
    return centre * lax.rsqrt(spread + epsilon) * gain_vec + shift_vec


def segment_of(position, seq_ends):
    return jnp.sum((position[:, None] >= seq_ends[None, :]).astype(jnp.int32), axis=1)


def owner_of(head, count):
    if count == 16:
        line, place = head // 3, head % 3
        return 4 * line + place + (line % 2) * ((place + 1) // 2)
    return head * count // HEADS


def greet_all(count, me):
    barrier = pltpu.get_barrier_semaphore()

    def greet(step, _):
        other = lax.rem(me + step, count)
        pl.semaphore_signal(
            barrier, inc=1, device_id={"ctx": other}, device_id_type=pl.DeviceIdType.MESH
        )
        return 0

    lax.fori_loop(1, count, greet, 0)
    pl.semaphore_wait(barrier, count - 1)


def to_heads_kernel(count, send_ref, recv_ref, send_sem, recv_sem, own_sem):
    me = lax.axis_index("ctx")
    greet_all(count, me)
    first = me * HEADS // count + 1

    def copy_for(head, source, owner):
        return pltpu.make_async_remote_copy(
            src_ref=send_ref.at[head],
            dst_ref=recv_ref.at[source],
            send_sem=send_sem.at[head],
            recv_sem=recv_sem.at[source],
            device_id={"ctx": owner},
            device_id_type=pl.DeviceIdType.MESH,
        )

    def own_copy(head):
        return pltpu.make_async_copy(send_ref.at[head], recv_ref.at[me], own_sem)

    def begin(step, _):
        head = lax.rem(first + step, HEADS)
        owner = owner_of(head, count)

        @pl.when(owner != me)
        def _():
            copy_for(head, me, owner).start()

        @pl.when(owner == me)
        def _():
            own_copy(head).start()

        return 0

    lax.fori_loop(0, HEADS, begin, 0)

    def finish(head, _):
        owner = owner_of(head, count)

        @pl.when(owner != me)
        def _():
            copy_for(head, me, owner).wait_send()

        @pl.when(owner == me)
        def _():
            own_copy(head).wait()

            def arrive(source, _):
                @pl.when(source != me)
                def _():
                    copy_for(head, source, owner).wait_recv()

                return 0

            lax.fori_loop(0, count, arrive, 0)

        return 0

    lax.fori_loop(0, HEADS, finish, 0)


def to_heads(send, count, collective_id):
    rows = send.shape[1]
    return pl.pallas_call(
        partial(to_heads_kernel, count),
        out_shape=jax.ShapeDtypeStruct((count, rows, LANES), low_type),
        in_specs=[pl.BlockSpec(memory_space=pltpu.VMEM)],
        out_specs=pl.BlockSpec(memory_space=pltpu.VMEM),
        scratch_shapes=[
            pltpu.SemaphoreType.DMA((HEADS,)),
            pltpu.SemaphoreType.DMA((count,)),
            pltpu.SemaphoreType.DMA,
        ],
        compiler_params=pltpu.CompilerParams(
            collective_id=collective_id, has_side_effects=True, vmem_limit_bytes=VMEM_BYTES
        ),
        cost_estimate=pl.CostEstimate(
            flops=rows * 250_000_000, bytes_accessed=send.size * 4, transcendentals=0
        ),
        name=f"to_heads_{rows}",
    )(send)


def to_rows_kernel(count, send_ref, recv_ref, send_sem, recv_sem, own_sem):
    me = lax.axis_index("ctx")
    greet_all(count, me)

    def copy_for(head, target):
        return pltpu.make_async_remote_copy(
            src_ref=send_ref.at[target],
            dst_ref=recv_ref.at[head],
            send_sem=send_sem.at[target],
            recv_sem=recv_sem.at[head],
            device_id={"ctx": target},
            device_id_type=pl.DeviceIdType.MESH,
        )

    def own_copy(head):
        return pltpu.make_async_copy(send_ref.at[me], recv_ref.at[head], own_sem)

    def begin(head, _):
        @pl.when(owner_of(head, count) == me)
        def _():
            own_copy(head).start()

            def push(step, _):
                copy_for(head, lax.rem(me + step, count)).start()
                return 0

            lax.fori_loop(1, count, push, 0)

        return 0

    lax.fori_loop(0, HEADS, begin, 0)

    def finish(head, _):
        @pl.when(owner_of(head, count) == me)
        def _():
            own_copy(head).wait()

            def leave(step, _):
                copy_for(head, lax.rem(me + step, count)).wait_send()
                return 0

            lax.fori_loop(1, count, leave, 0)

        @pl.when(owner_of(head, count) != me)
        def _():
            copy_for(head, me).wait_recv()

        return 0

    lax.fori_loop(0, HEADS, finish, 0)


def to_rows(send, count, collective_id):
    rows = send.shape[1]
    return pl.pallas_call(
        partial(to_rows_kernel, count),
        out_shape=jax.ShapeDtypeStruct((HEADS, rows, LANES), low_type),
        in_specs=[pl.BlockSpec(memory_space=pltpu.VMEM)],
        out_specs=pl.BlockSpec(memory_space=pltpu.VMEM),
        scratch_shapes=[
            pltpu.SemaphoreType.DMA((count,)),
            pltpu.SemaphoreType.DMA((HEADS,)),
            pltpu.SemaphoreType.DMA,
        ],
        compiler_params=pltpu.CompilerParams(
            collective_id=collective_id, has_side_effects=True, vmem_limit_bytes=VMEM_BYTES
        ),
        cost_estimate=pl.CostEstimate(
            flops=rows * 250_000_000, bytes_accessed=send.size * 4, transcendentals=0
        ),
        name=f"to_rows_{rows}",
    )(send)


def project_kernel(x_ref, pack_ref, vec_ref, out_ref):
    rows, width = x_ref.shape
    half = rows // 2
    step = 4
    for base in range(0, HEADS, step):
        cols = slice(base * LANES, (base + step) * LANES)
        both = dot_nn(x_ref[...], pack_ref[:, width + cols.start : width + cols.stop])
        bias = vec_ref[1:2, base * HEAD_DIM : (base + step) * HEAD_DIM]
        blank = jnp.zeros((1, HEAD_DIM), jnp.float32)
        shifts = []
        for at in range(step):
            shifts += [blank, bias[:, at * HEAD_DIM : (at + 1) * HEAD_DIM]]
        both = (both + jnp.concatenate(shifts, axis=1)).astype(low_type)
        for at in range(step):
            out_ref[base + at, 0:rows, :] = both[:, at * LANES : (at + 1) * LANES]
        cols = slice(base * HEAD_DIM, (base + step) * HEAD_DIM)
        query = ((dot_nn(x_ref[...], pack_ref[:, cols]) + vec_ref[0:1, cols]) * 0.125).astype(low_type)
        for at in range(step):
            lanes = slice(at * HEAD_DIM, (at + 1) * HEAD_DIM)
            out_ref[base + at, rows : rows + half, :] = jnp.concatenate(
                [query[:half, lanes], query[half:, lanes]], axis=1
            )


def project(x, pack, vectors):
    rows = x.shape[0]
    vmem = pl.BlockSpec(memory_space=pltpu.VMEM)
    return pl.pallas_call(
        project_kernel,
        out_shape=jax.ShapeDtypeStruct((HEADS, rows + rows // 2, LANES), low_type),
        in_specs=[vmem] * 3,
        out_specs=vmem,
        compiler_params=pltpu.CompilerParams(vmem_limit_bytes=VMEM_BYTES),
        name="project",
    )(x, pack, vectors)


def tile_range(meta_ref, first, last, total):
    end_a, end_b, end_c = meta_ref[0], meta_ref[1], meta_ref[2]
    low = jnp.where(
        first >= end_c, end_c, jnp.where(first >= end_b, end_b, jnp.where(first >= end_a, end_a, 0))
    )
    high = jnp.where(
        last >= end_c,
        total,
        jnp.where(last >= end_b, end_c, jnp.where(last >= end_a, end_b, end_a)),
    )
    return low // TILE, (high + TILE - 1) // TILE


def attend_kernel(meta_ref, order_ref, recv_ref, out_ref, qa_ref, ka_ref, va_ref, sum_ref):
    count = recv_ref.shape[0]
    half = recv_ref.shape[1] // 3
    total = qa_ref.shape[0]

    @pl.when(meta_ref[3] == 1)
    def _():
        lane = lax.broadcasted_iota(jnp.int32, (half, LANES), 1)
        lower = lane < HEAD_DIM
        row = lax.broadcasted_iota(jnp.int32, (half, LANES), 0)

        def place(source, _):
            query = recv_ref[source, 2 * half :, :].astype(jnp.float32)
            for part in range(2):
                first = pl.multiple_of(order_ref[2 * source + part] * half, half)
                position = first + row
                segment = (
                    (position >= meta_ref[0]).astype(jnp.int32)
                    + (position >= meta_ref[1]).astype(jnp.int32)
                    + (position >= meta_ref[2]).astype(jnp.int32)
                )
                mine = (lane - HEAD_DIM) == segment
                other = (lane < HEAD_DIM + 4) & (~mine)
                pair = recv_ref[source, part * half : (part + 1) * half, :].astype(jnp.float32)
                if part == 1:
                    query = pltpu.roll(query, HEAD_DIM, 1)
                mark_k = jnp.where(
                    other, FAR, jnp.where((lane >= HEAD_DIM + 4) & (lane < HEAD_DIM + 7), 1.0, 0.0)
                )
                rows = pl.ds(first, half)
                qa_ref[rows, :] = jnp.where(lower, query, jnp.where(mine, 1.0, 0.0)).astype(low_type)
                ka_ref[rows, :] = jnp.where(lower, pair, mark_k).astype(low_type)
                va_ref[rows, :] = jnp.where(lower, 1.0, pair).astype(low_type)
            return 0

        lax.fori_loop(0, count, place, 0)

        def query_step(index, _):
            first = pl.multiple_of(index * TILE, TILE)
            rows = pl.ds(first, TILE)
            begin, end = tile_range(meta_ref, first, first + TILE - 1, total)
            query = qa_ref[rows, :]
            sum_ref[rows, :] = jnp.zeros((TILE, LANES), jnp.float32)

            def key_step(key_index, _):
                keys = pl.ds(pl.multiple_of(key_index * TILE, TILE), TILE)
                expo = jnp.exp(dot_nt(query, ka_ref[keys, :])).astype(low_type)
                sum_ref[rows, :] += dot_nn(expo, va_ref[keys, :])
                return 0

            lax.fori_loop(begin, end, key_step, 0)
            return 0

        lax.fori_loop(0, total // TILE, query_step, 0)

        def give(source, _):
            parts = []
            for part in range(2):
                first = pl.multiple_of(order_ref[2 * source + part] * half, half)
                block = sum_ref[pl.ds(first, half), :]
                parts.append((block, pltpu.roll(block, HEAD_DIM, 1)))
            top = jnp.where(lower, parts[0][1], parts[1][0])
            bottom = jnp.where(lower, parts[0][0], parts[1][1])
            out_ref[source] = (top / bottom).astype(low_type)
            return 0

        lax.fori_loop(0, count, give, 0)


def attend(meta, order, recv):
    count, rows, _ = recv.shape
    total = count * rows * 2 // 3
    vmem = pl.BlockSpec(memory_space=pltpu.VMEM)
    smem = pl.BlockSpec(memory_space=pltpu.SMEM)
    whole = jax.ShapeDtypeStruct((total, LANES), low_type)
    return pl.pallas_call(
        attend_kernel,
        out_shape=(
            jax.ShapeDtypeStruct((count, rows // 3, LANES), low_type),
            whole,
            whole,
            whole,
            jax.ShapeDtypeStruct((total, LANES), jnp.float32),
        ),
        in_specs=[smem, smem, vmem],
        out_specs=(vmem,) * 5,
        compiler_params=pltpu.CompilerParams(vmem_limit_bytes=VMEM_BYTES),
        cost_estimate=pl.CostEstimate(
            flops=total * total * LANES * 8, bytes_accessed=total * LANES * 12, transcendentals=0
        ),
        name="attend",
    )(meta, order, recv)


def split_three(value):
    first = value.astype(low_type).astype(jnp.float32)
    rest = value - first
    second = rest.astype(low_type).astype(jnp.float32)
    return first, second, rest - second


def attend_back_kernel(
    meta_ref,
    order_ref,
    recv_ref,
    qa_ref,
    ka_ref,
    va_ref,
    sum_ref,
    out_ref,
    qb_ref,
    da_ref,
    kt_ref,
    dkv_ref,
    dq_ref,
    acc_ref,
):
    count = recv_ref.shape[0]
    half = recv_ref.shape[1]
    total = qa_ref.shape[0]

    @pl.when(meta_ref[3] == 1)
    def _():
        lane = lax.broadcasted_iota(jnp.int32, (half, LANES), 1)
        lower = lane < HEAD_DIM

        def place(source, _):
            given = recv_ref[source].astype(jnp.float32)
            for part in range(2):
                first = pl.multiple_of(order_ref[2 * source + part] * half, half)
                rows = pl.ds(first, half)
                block = sum_ref[rows, :]
                turned = pltpu.roll(block, HEAD_DIM, 1)
                d_context = pltpu.roll(given, HEAD_DIM, 1) if part == 0 else given
                product = jnp.where(lower, 0.0, d_context * (block / turned))
                minus = -jnp.sum(product, axis=1, keepdims=True)
                one, two, three = split_three(minus)
                mark = jnp.where(
                    lane == 0, one, jnp.where(lane == 1, two, jnp.where(lane == 2, three, 0.0))
                )
                da_ref[rows, :] = jnp.where(lower, mark, d_context).astype(low_type)
                one, two, three = split_three(-jnp.log(turned))
                at = lane - (HEAD_DIM + 4)
                mark = jnp.where(at == 0, one, jnp.where(at == 1, two, three))
                query = qa_ref[rows, :].astype(jnp.float32)
                qb_ref[rows, :] = jnp.where((at >= 0) & (at < 3), mark, query).astype(low_type)
            return 0

        lax.fori_loop(0, count, place, 0)

        def prepare(index, _):
            rows = pl.ds(pl.multiple_of(index * TILE, TILE), TILE)
            kt_ref[:, rows] = jnp.transpose(ka_ref[rows, :])[:HEAD_DIM, :]
            dkv_ref[rows, :] = jnp.zeros((TILE, LANES), jnp.float32)
            return 0

        lax.fori_loop(0, total // TILE, prepare, 0)

        lower_tile = lax.broadcasted_iota(jnp.int32, (TILE, LANES), 1) < HEAD_DIM

        def query_step(index, _):
            first = pl.multiple_of(index * TILE, TILE)
            rows = pl.ds(first, TILE)
            begin, end = tile_range(meta_ref, first, first + TILE - 1, total)
            query = qb_ref[rows, :]
            given = da_ref[rows, :]
            query_only = jnp.where(lower_tile, query.astype(jnp.float32), 0.0).astype(low_type)
            given_only = jnp.where(lower_tile, 0.0, given.astype(jnp.float32)).astype(low_type)
            acc_ref[...] = jnp.zeros_like(acc_ref)

            def key_step(key_index, _):
                keys = pl.ds(pl.multiple_of(key_index * TILE, TILE), TILE)
                prob = jnp.exp(dot_nt(ka_ref[keys, :], query))
                d_scores = (prob * dot_nt(va_ref[keys, :], given)).astype(low_type)
                dkv_ref[keys, :] += dot_nn(d_scores, query_only) + dot_nn(
                    prob.astype(low_type), given_only
                )
                acc_ref[...] += dot_nn(kt_ref[:, keys], d_scores)
                return 0

            lax.fori_loop(begin, end, key_step, 0)
            dq_ref[rows, :] = jnp.transpose(acc_ref[...])
            return 0

        lax.fori_loop(0, total // TILE, query_step, 0)

        def give(source, _):
            queries = []
            for part in range(2):
                first = pl.multiple_of(order_ref[2 * source + part] * half, half)
                rows = pl.ds(first, half)
                out_ref[source, part * half : (part + 1) * half, :] = dkv_ref[rows, :].astype(low_type)
                queries.append(dq_ref[rows, :])
            out_ref[source, 2 * half :, :] = jnp.concatenate(queries, axis=1).astype(low_type)
            return 0

        lax.fori_loop(0, count, give, 0)


def attend_back(meta, order, recv, qa, ka, va, sums):
    count, half, _ = recv.shape
    total = qa.shape[0]
    vmem = pl.BlockSpec(memory_space=pltpu.VMEM)
    smem = pl.BlockSpec(memory_space=pltpu.SMEM)
    return pl.pallas_call(
        attend_back_kernel,
        out_shape=jax.ShapeDtypeStruct((count, 3 * half, LANES), low_type),
        in_specs=[smem, smem] + [vmem] * 5,
        out_specs=vmem,
        scratch_shapes=[
            pltpu.VMEM((total, LANES), low_type),
            pltpu.VMEM((total, LANES), low_type),
            pltpu.VMEM((HEAD_DIM, total), low_type),
            pltpu.VMEM((total, LANES), jnp.float32),
            pltpu.VMEM((total, HEAD_DIM), jnp.float32),
            pltpu.VMEM((HEAD_DIM, TILE), jnp.float32),
        ],
        compiler_params=pltpu.CompilerParams(vmem_limit_bytes=VMEM_BYTES),
        cost_estimate=pl.CostEstimate(
            flops=total * total * LANES * 16, bytes_accessed=total * LANES * 16, transcendentals=0
        ),
        name="attend_back",
    )(meta, order, recv, qa, ka, va, sums)


PART_ORDERS = (("x", "z"), ("x", "z"), ("wa", "x", "z"), ("wa", "x", "z"))
GATHER_ORDERS = (("z", "x"), ("z", "x"), ("z", "x"), ("x", "z"))
PARTS = len(PART_ORDERS)
EARLY = sum(len(order) == 2 for order in PART_ORDERS)
STAGES = sum(len(order) for order in PART_ORDERS)
SIZES = {"wa": 2, "x": 2, "z": 4}


class Links:
    def __init__(self):
        me = lax.axis_index("ctx")
        self.at = {
            "core": lax.rem(me, 2),
            "x": lax.rem(me // 2, 2),
            "z": me // 4,
            "wa": lax.axis_index("wa"),
        }

    def peer(self, axis, value):
        at = dict(self.at)
        at[axis] = value
        return {"ctx": at["z"] * 4 + at["x"] * 2 + at["core"], "wa": at["wa"]}


def splits_rows(piece):
    return piece % 64 == 0


def grad_sum_kernel(*refs):
    refs = list(refs)
    sizes = (PARTS, PARTS, PARTS - EARLY, STAGES)
    g_refs, out_refs, core_bufs, bufs = (
        [refs.pop(0) for _ in range(number)] for number in sizes
    )
    core_bufs = [None] * EARLY + core_bufs
    send_sem, recv_sem = refs
    links = Links()
    core, x, z, wa = (links.at[name] for name in ("core", "x", "z", "wa"))
    barrier = pltpu.get_barrier_semaphore()
    peers = [links.peer("core", 1 - core), links.peer("x", 1 - x), links.peer("wa", 1 - wa)]
    peers += [links.peer("z", lax.rem(z + step, 4)) for step in range(1, 4)]
    for peer in peers:
        pl.semaphore_signal(barrier, inc=1, device_id=peer, device_id_type=pl.DeviceIdType.MESH)
    pl.semaphore_wait(barrier, len(peers))
    used = [0]

    def remote(src, dst, peer):
        index = used[0]
        used[0] += 1
        copy = pltpu.make_async_remote_copy(
            src_ref=src,
            dst_ref=dst,
            send_sem=send_sem.at[index],
            recv_sem=recv_sem.at[index],
            device_id=peer,
            device_id_type=pl.DeviceIdType.MESH,
        )
        copy.start()
        return copy

    def z_share(ref, value):
        piece, width = ref.shape[-2:]
        if value is None:
            return slice(None), slice(None)
        if splits_rows(piece):
            return pl.ds(pl.multiple_of(value * (piece // 4), 16), piece // 4), slice(None)
        return slice(None), pl.ds(pl.multiple_of(value * (width // 4), LANES), width // 4)

    def slab(part, held, axis=None, value=None):
        at = dict(links.at)
        if axis is not None:
            at[axis] = value
            held = held | {axis}
        return g_refs[part].at[
            pl.ds(0, 1) if part < EARLY else pl.ds(at["wa"], 1) if "wa" in held else pl.ds(0, 2),
            0 if part < EARLY else core,
            pl.ds(at["x"], 1) if "x" in held else pl.ds(0, 2),
            *z_share(g_refs[part], at["z"] if "z" in held else None),
        ]

    def add_into(target, sources):
        outer, inner, rows, _ = target.shape
        for a in range(outer):
            for b in range(inner):

                def add(group, _):
                    some = pl.ds(pl.multiple_of(group * 16, 16), 16)
                    total = target[a, b, some, :].astype(jnp.float32)
                    for source in sources:
                        total = total + source[a, b, some, :].astype(jnp.float32)
                    target[a, b, some, :] = total.astype(low_type)
                    return 0

                lax.fori_loop(0, rows // 16, add, 0)

    core_copies = [
        remote(g_refs[part].at[:, 1 - core], core_bufs[part], links.peer("core", 1 - core))
        if part >= EARLY
        else None
        for part in range(PARTS)
    ]
    first_buf = [sum(len(order) for order in PART_ORDERS[:part]) for part in range(PARTS)]

    def begin(part, stage):
        axis = PART_ORDERS[part][stage]
        held = set(PART_ORDERS[part][:stage])
        buf = bufs[first_buf[part] + stage]
        copies = []
        for step in range(1, SIZES[axis]):
            value = lax.rem(links.at[axis] + step, SIZES[axis])
            copies.append(
                remote(slab(part, held, axis, value), buf.at[step - 1], links.peer(axis, value))
            )
        return copies

    def out_slab(part, held):
        return out_refs[part].at[
            core,
            pl.ds(x, 1) if "x" in held else pl.ds(0, 2),
            *z_share(out_refs[part], z if "z" in held else None),
        ]

    def spread(part, stage):
        axis = GATHER_ORDERS[part][stage]
        block = out_slab(part, set(GATHER_ORDERS[part][stage:]))
        return [
            remote(block, block, links.peer(axis, lax.rem(links.at[axis] + step, SIZES[axis])))
            for step in range(1, SIZES[axis])
        ]

    def start_gather(part, stage):
        if stage < 2:
            return spread(part, stage)
        block = out_slab(part, set())
        return [remote(block, block, links.peer("core", 1 - core))]

    flying, passed = {}, {}
    for part in range(PARTS):
        passed[part] = 0 if part >= EARLY else 1
        flying[part] = begin(part, 0) if part < EARLY else [core_copies[part]]
    while any(flying.values()):
        for part in range(PARTS):
            if not flying[part]:
                continue
            order = PART_ORDERS[part]
            for copy in flying[part]:
                copy.wait()
            step = passed[part]
            passed[part] += 1
            if step == 0:
                add_into(slab(part, set()), [core_bufs[part]])
            elif step <= len(order):
                buf = bufs[first_buf[part] + step - 1]
                add_into(
                    slab(part, set(order[:step])),
                    [buf.at[at] for at in range(SIZES[order[step - 1]] - 1)],
                )
            if step < len(order):
                flying[part] = begin(part, step)
            elif step == len(order):
                out_slab(part, {"x", "z"})[...] = slab(part, {"wa", "x", "z"})[0]
                flying[part] = start_gather(part, 0)
            elif step <= len(order) + 2:
                flying[part] = start_gather(part, step - len(order))
            else:
                flying[part] = None


def grad_sum(grads, collective_id):
    bufs, core_bufs, outs, given = [], [], [], []
    for part, grad in enumerate(grads):
        rows, width = grad.shape
        early = part < EARLY
        piece = rows // 2 if early else rows // 8
        shape = {"wa": 1 if early else 2, "x": 2, "z": 4}
        for axis in PART_ORDERS[part]:
            shape[axis] //= SIZES[axis]
            share = (
                (piece * shape["z"] // 4, width)
                if splits_rows(piece)
                else (piece, width * shape["z"] // 4)
            )
            bufs.append(
                pltpu.VMEM((SIZES[axis] - 1, shape["wa"], shape["x"], *share), low_type)
            )
        if not early:
            core_bufs.append(pltpu.VMEM((2, 2, piece, width), low_type))
        outs.append(jax.ShapeDtypeStruct((2, 2, piece, width), low_type))
        lead = (1, 1) if early else (2, 2)
        given.append(grad.reshape(*lead, 2, piece, width))
    vmem = pl.BlockSpec(memory_space=pltpu.VMEM)
    size = sum(grad.size for grad in grads)
    sums = pl.pallas_call(
        grad_sum_kernel,
        out_shape=tuple(outs),
        in_specs=[vmem] * PARTS,
        out_specs=(vmem,) * PARTS,
        scratch_shapes=[
            *core_bufs,
            *bufs,
            pltpu.SemaphoreType.DMA((16 * PARTS,)),
            pltpu.SemaphoreType.DMA((16 * PARTS,)),
        ],
        compiler_params=pltpu.CompilerParams(
            collective_id=collective_id, has_side_effects=True, vmem_limit_bytes=VMEM_BYTES
        ),
        cost_estimate=pl.CostEstimate(
            flops=size * 20_000, bytes_accessed=size * 4, transcendentals=0
        ),
        name="grad_sum",
    )(*given)
    return [part.reshape(-1, part.shape[-1]) for part in sums]


def column_sums(terms, lanes):
    total = 0.0
    for index, term in enumerate(terms):
        place = lax.broadcasted_iota(jnp.int32, (term.shape[0], lanes), 1) == index
        total = total + jnp.einsum(
            "td,tk->dk", term, place.astype(low_type), preferred_element_type=jnp.float32
        )
    return total.astype(low_type)


def reduce_shards(grad):
    part = lax.psum_scatter(
        grad.astype(low_type), ("wa", "ctx"), scatter_dimension=0, tiled=True
    )
    return lax.all_gather(part, "ctx", axis=0, tiled=True)


def body(
    count,
    tokens,
    cotangent,
    lengths,
    block_order,
    w_query,
    b_query,
    w_key,
    w_value,
    b_value,
    w_out,
    b_out,
    gain_one,
    shift_one,
    w_up,
    b_up,
    w_down,
    b_down,
    gain_two,
    shift_two,
):
    inputs = tokens[0]
    tok_rows, width = inputs.shape
    wide = w_up.shape[1]
    half = tok_rows // 2
    shard = w_query.shape[0]
    direct = count == 16 and width == 2 * shard and shard % 64 == 0 and wide == 4 * width
    me = lax.axis_index("ctx")
    seq_ends = jnp.cumsum(lengths[0])
    own_blocks = lax.dynamic_slice(block_order, (2 * me,), (2,))
    position = (own_blocks[:, None] * half + jnp.arange(half, dtype=jnp.int32)[None, :]).reshape(-1)
    own_seg = segment_of(position, seq_ends)
    owns = jnp.any(me == owner_of(jnp.arange(HEADS, dtype=jnp.int32), count)).astype(jnp.int32)
    meta = jnp.concatenate([seq_ends.astype(jnp.int32), owns[None]])

    core = me % 2
    wa = lax.axis_index("wa")

    def fetch_half(shard_block, after=None):
        if not direct:
            return None
        size, columns = shard_block.shape
        part = lax.dynamic_slice(shard_block, (core * (size // 2), 0), (size // 2, columns))
        if after is not None:
            part = lax.optimization_barrier(part)
            part, _ = lax.optimization_barrier((part, after))
        return lax.ppermute(part, "wa", [(0, 1), (1, 0)])

    def gather_rows(shard_block, fetched):
        if not direct:
            return lax.all_gather(shard_block, "wa", axis=0, tiled=True)
        size, columns = shard_block.shape
        swapped = lax.ppermute(fetched, "ctx", [(k, k ^ 1) for k in range(count)])
        other = (1 - wa) * size
        whole = jnp.zeros((2 * size, columns), shard_block.dtype)
        whole = lax.dynamic_update_slice(whole, shard_block, (wa * size, 0))
        whole = lax.dynamic_update_slice(whole, fetched, (other + core * (size // 2), 0))
        return lax.dynamic_update_slice(whole, swapped, (other + (1 - core) * (size // 2), 0))

    pair = jnp.stack(
        [
            w_key.astype(low_type).reshape(shard, HEADS, HEAD_DIM),
            w_value.astype(low_type).reshape(shard, HEADS, HEAD_DIM),
        ],
        axis=2,
    ).reshape(shard, 2 * width)
    own_vectors = jnp.concatenate(
        [
            jnp.stack(
                [b_query, b_value, b_out, gain_one, shift_one, gain_two, shift_two, b_down]
            ),
            b_up.reshape(4, shard),
            jnp.zeros((4, shard), jnp.float32),
        ],
        axis=0,
    ).astype(low_type)
    if direct:
        other_vectors = lax.ppermute(own_vectors, "wa", [(0, 1), (1, 0)])
        vector_rows = jnp.where(
            wa == 0,
            jnp.concatenate([own_vectors, other_vectors], axis=1),
            jnp.concatenate([other_vectors, own_vectors], axis=1),
        ).astype(jnp.float32)
    else:
        vector_rows = (
            lax.all_gather(own_vectors, "wa", axis=1, tiled=True)
        ).astype(jnp.float32)

    first_shard = jnp.concatenate([w_query.astype(low_type), pair], axis=1)
    fetched = fetch_half(first_shard)
    later_shards = (
        w_out.astype(low_type),
        w_up.astype(low_type),
        w_down.astype(low_type),
    )
    later_fetched = tuple(fetch_half(block, fetched) for block in later_shards)
    first_pack = gather_rows(first_shard, fetched)
    query_weight = first_pack[:, :width]
    pair_weight = first_pack[:, width : 3 * width]
    out_bias, gain_first, shift_first, gain_second, shift_second, down_bias = (
        vector_rows[index] for index in range(2, 8)
    )
    up_bias = (
        vector_rows[8:12].reshape(4, width // shard, shard).transpose(1, 0, 2).reshape(-1)
    )

    packed = project(inputs, first_pack, vector_rows)
    at_head = to_heads(packed, count, 0)
    context_out, qa, ka, va, sums = attend(meta, block_order, at_head)
    context_out, later_fetched = lax.optimization_barrier((context_out, later_fetched))
    out_weight, up_weight, down_weight = (
        gather_rows(block, half_block) for block, half_block in zip(later_shards, later_fetched)
    )
    context_in = to_rows(context_out, count, 1)
    context_low = (
        context_in.reshape(HEADS, half, 2, HEAD_DIM).transpose(2, 1, 0, 3).reshape(tok_rows, width)
    )

    attn_out = jnp.dot(context_low, out_weight, preferred_element_type=jnp.float32) + out_bias
    h_one = inputs.astype(jnp.float32) + attn_out
    norm_one, norm_one_back = jax.vjp(layer_norm, h_one, gain_first, shift_first)
    norm_low = norm_one.astype(low_type)
    up_pre = jnp.dot(norm_low, up_weight, preferred_element_type=jnp.float32) + up_bias
    gelu_out, gelu_back = jax.vjp(partial(jax.nn.gelu, approximate=False), up_pre)
    gelu_low = gelu_out.astype(low_type)
    down_out = jnp.dot(gelu_low, down_weight, preferred_element_type=jnp.float32) + down_bias
    h_two = norm_one + down_out
    result, norm_two_back = jax.vjp(layer_norm, h_two, gain_second, shift_second)
    activations = result.astype(low_type)[None]
    valid = (own_seg < 3).astype(jnp.float32)
    g_out = cotangent[0].astype(jnp.float32) * valid[:, None]
    d_htwo, grad_gain_second, grad_shift_second = norm_two_back(g_out)
    d_down = d_htwo.astype(low_type)
    d_gelu = jnp.einsum("td,fd->tf", d_down, down_weight, preferred_element_type=jnp.float32)
    (d_uppre,) = gelu_back(d_gelu)
    d_up = d_uppre.astype(low_type)
    d_yone = d_htwo + jnp.einsum("tf,df->td", d_up, up_weight, preferred_element_type=jnp.float32)
    d_hone, grad_gain_first, grad_shift_first = norm_one_back(d_yone)
    d_attn = d_hone.astype(low_type)
    d_context = jnp.einsum("td,cd->tc", d_attn, out_weight, preferred_element_type=jnp.float32)
    context_back = (
        d_context.astype(low_type)
        .reshape(2, half, HEADS, HEAD_DIM)
        .transpose(2, 1, 0, 3)
        .reshape(HEADS, half, LANES)
    )

    grad_wdown = jnp.einsum("tf,td->fd", gelu_low, d_down, preferred_element_type=jnp.float32)
    grad_wup = jnp.einsum("td,tf->df", norm_low, d_up, preferred_element_type=jnp.float32)
    grad_wout = jnp.einsum("tc,td->cd", context_low, d_attn, preferred_element_type=jnp.float32)
    up_bias_sums = jnp.sum(d_up.astype(jnp.float32), axis=0)
    lanes = 2 * LANES
    vec_block = jnp.concatenate(
        [
            jnp.stack(
                [
                    jnp.sum(d_attn.astype(jnp.float32), axis=0),
                    grad_gain_first,
                    grad_shift_first,
                    jnp.sum(d_down.astype(jnp.float32), axis=0),
                    grad_gain_second,
                    grad_shift_second,
                ],
                axis=1,
            ),
            up_bias_sums.reshape(width // shard, 4, shard).transpose(0, 2, 1).reshape(width, 4),
        ],
        axis=1,
    ).astype(low_type)
    out_block = jnp.concatenate(
        [grad_wout.astype(low_type), jnp.pad(vec_block, ((0, 0), (0, lanes - 10)))], axis=1
    )
    up_block = grad_wup.astype(low_type)
    down_block = grad_wdown.astype(low_type)
    def add_low(mine, given):
        return (mine.astype(jnp.float32) + given.astype(jnp.float32)).astype(low_type)

    def core_halves(block):
        view = block.reshape(2, 2, -1, block.shape[1])
        keep = lax.dynamic_index_in_dim(view, core, 1, keepdims=False)
        give = lax.dynamic_index_in_dim(view, 1 - core, 1, keepdims=False)
        return keep, lax.ppermute(give, "ctx", [(k, k ^ 1) for k in range(count)])

    def wa_halves(block):
        keep = lax.dynamic_index_in_dim(block, wa, 0, keepdims=False)
        give = lax.dynamic_index_in_dim(block, 1 - wa, 0, keepdims=False)
        return keep, lax.ppermute(give, "wa", [(0, 1), (1, 0)])

    context_back, down_block, out_block, up_block = lax.optimization_barrier(
        (context_back, down_block, out_block, up_block)
    )
    if direct:
        halves = [core_halves(block) for block in (up_block, down_block)]
        back_at_head = to_heads(context_back, count, 2)
        back_at_head, halves = lax.optimization_barrier((back_at_head, halves))
        halves = [wa_halves(add_low(*pair)) for pair in halves]
        grads_out = attend_back(meta, block_order, back_at_head, qa, ka, va, sums)
        grads_out, halves = lax.optimization_barrier((grads_out, halves))
        early = [add_low(*pair) for pair in halves]
    else:
        back_at_head = to_heads(context_back, count, 2)
        grads_out = attend_back(meta, block_order, back_at_head, qa, ka, va, sums)
    grads_in = to_rows(grads_out, count, 3)

    d_pair = grads_in[:, :tok_rows, :].transpose(1, 0, 2).reshape(tok_rows, 2 * width)
    d_queries = (
        grads_in[:, tok_rows:, :]
        .reshape(HEADS, half, 2, HEAD_DIM)
        .transpose(2, 1, 0, 3)
        .reshape(tok_rows, width)
        * jnp.asarray(0.125, low_type)
    )
    d_keys, d_values = (
        grads_in[:, :tok_rows, low : low + HEAD_DIM].transpose(1, 0, 2).reshape(tok_rows, width)
        for low in (0, HEAD_DIM)
    )
    d_all = jnp.concatenate(
        [d_queries, d_keys, d_values, jnp.zeros((tok_rows, lanes), low_type)], axis=1
    )
    grad_all = jnp.einsum("tc,td->cd", inputs, d_all, preferred_element_type=jnp.float32)
    last_block = lax.dynamic_update_slice(
        grad_all.astype(low_type),
        column_sums([d_queries, d_values], lanes),
        (0, 3 * width),
    )
    if direct:
        up_sum, down_sum, last_sum, out_sum = grad_sum((*early, last_block, out_block), 4)
    else:
        up_sum, down_sum, last_sum, out_sum = (
            reduce_shards(block) for block in (up_block, down_block, last_block, out_block)
        )
    d_input = (
        d_hone
        + jnp.einsum("td,cd->tc", d_queries, query_weight, preferred_element_type=jnp.float32)
        + jnp.einsum("td,cd->tc", d_pair, pair_weight, preferred_element_type=jnp.float32)
    )
    input_grad = d_input.astype(low_type)[None]

    wide_grad = last_sum.astype(jnp.float32)
    out_grad = out_sum.astype(jnp.float32)
    return (
        activations,
        input_grad,
        wide_grad[:, :width],
        wide_grad[:, 3 * width],
        wide_grad[:, width : 2 * width],
        wide_grad[:, 2 * width : 3 * width],
        wide_grad[:, 3 * width + 1],
        out_grad[:, :width],
        out_grad[:, width],
        out_grad[:, width + 1],
        out_grad[:, width + 2],
        up_sum.astype(jnp.float32),
        out_grad[:, width + 6 : width + 10].T.reshape(-1),
        down_sum.astype(jnp.float32),
        out_grad[:, width + 3],
        out_grad[:, width + 4],
        out_grad[:, width + 5],
    )


def solution(mesh):
    placed = (
        P("wa", "ctx", None),
        P("wa", "ctx", None),
        P("wa", None),
        P(),
        P("wa", None),
        P("wa"),
        P("wa", None),
        P("wa", None),
        P("wa"),
        P("wa", None),
        P("wa"),
        P("wa"),
        P("wa"),
        P("wa", None),
        P("wa"),
        P("wa", None),
        P("wa"),
        P("wa"),
        P("wa"),
    )
    return jax.shard_map(
        partial(body, mesh.shape["ctx"]),
        mesh=mesh,
        in_specs=placed,
        out_specs=(
            P("wa", "ctx", None),
            P("wa", "ctx", None),
            P("wa", None),
            P("wa"),
            P("wa", None),
            P("wa", None),
            P("wa"),
            P("wa", None),
            P("wa"),
            P("wa"),
            P("wa"),
            P("wa", None),
            P("wa"),
            P("wa", None),
            P("wa"),
            P("wa"),
            P("wa"),
        ),
        check_vma=False,
    )
```

```python
from functools import partial

import jax
import jax.numpy as jnp
from jax import lax
from jax.experimental import pallas as pl
from jax.experimental.pallas import tpu as pltpu
from jax.sharding import PartitionSpec as P

HEADS = 12
HEAD_DIM = 64
LANES = 128
TILE = 512
FAR = -(2.0**40)
VMEM_BYTES = 60 << 20

low_type = jnp.bfloat16
epsilon = 1e-05


def dot_nt(left, right):
    return lax.dot_general(
        left, right, (((1,), (1,)), ((), ())), preferred_element_type=jnp.float32
    )


def dot_nn(left, right):
    return lax.dot_general(
        left, right, (((1,), (0,)), ((), ())), preferred_element_type=jnp.float32
    )


def layer_norm(hidden, gain_vec, shift_vec):
    centre = hidden - jnp.mean(hidden, axis=-1, keepdims=True)
    spread = jnp.mean(centre * centre, axis=-1, keepdims=True)
    return centre * lax.rsqrt(spread + epsilon) * gain_vec + shift_vec


def segment_of(position, seq_ends):
    return jnp.sum((position[:, None] >= seq_ends[None, :]).astype(jnp.int32), axis=1)


def owner_of(head, count):
    return head * count // HEADS


def greet_all(count, me):
    barrier = pltpu.get_barrier_semaphore()

    def greet(step, _):
        other = lax.rem(me + step, count)
        pl.semaphore_signal(
            barrier, inc=1, device_id={"ctx": other}, device_id_type=pl.DeviceIdType.MESH
        )
        return 0

    lax.fori_loop(1, count, greet, 0)
    pl.semaphore_wait(barrier, count - 1)


def to_heads_kernel(count, send_ref, recv_ref, send_sem, recv_sem, own_sem):
    me = lax.axis_index("ctx")
    greet_all(count, me)
    first = me * HEADS // count + 1

    def copy_for(head, source, owner):
        return pltpu.make_async_remote_copy(
            src_ref=send_ref.at[head],
            dst_ref=recv_ref.at[source],
            send_sem=send_sem.at[head],
            recv_sem=recv_sem.at[source],
            device_id={"ctx": owner},
            device_id_type=pl.DeviceIdType.MESH,
        )

    def own_copy(head):
        return pltpu.make_async_copy(send_ref.at[head], recv_ref.at[me], own_sem)

    def begin(step, _):
        head = lax.rem(first + step, HEADS)
        owner = owner_of(head, count)

        @pl.when(owner != me)
        def _():
            copy_for(head, me, owner).start()

        @pl.when(owner == me)
        def _():
            own_copy(head).start()

        return 0

    lax.fori_loop(0, HEADS, begin, 0)

    def finish(head, _):
        owner = owner_of(head, count)

        @pl.when(owner != me)
        def _():
            copy_for(head, me, owner).wait_send()

        @pl.when(owner == me)
        def _():
            own_copy(head).wait()

            def arrive(source, _):
                @pl.when(source != me)
                def _():
                    copy_for(head, source, owner).wait_recv()

                return 0

            lax.fori_loop(0, count, arrive, 0)

        return 0

    lax.fori_loop(0, HEADS, finish, 0)


def to_heads(send, count, collective_id):
    rows = send.shape[1]
    return pl.pallas_call(
        partial(to_heads_kernel, count),
        out_shape=jax.ShapeDtypeStruct((count, rows, LANES), low_type),
        in_specs=[pl.BlockSpec(memory_space=pltpu.VMEM)],
        out_specs=pl.BlockSpec(memory_space=pltpu.VMEM),
        scratch_shapes=[
            pltpu.SemaphoreType.DMA((HEADS,)),
            pltpu.SemaphoreType.DMA((count,)),
            pltpu.SemaphoreType.DMA,
        ],
        compiler_params=pltpu.CompilerParams(
            collective_id=collective_id, has_side_effects=True, vmem_limit_bytes=VMEM_BYTES
        ),
        cost_estimate=pl.CostEstimate(
            flops=rows * 250_000_000, bytes_accessed=send.size * 4, transcendentals=0
        ),
        name=f"to_heads_{rows}",
    )(send)


def to_rows_kernel(count, send_ref, recv_ref, send_sem, recv_sem, own_sem):
    me = lax.axis_index("ctx")
    greet_all(count, me)

    def copy_for(head, target):
        return pltpu.make_async_remote_copy(
            src_ref=send_ref.at[target],
            dst_ref=recv_ref.at[head],
            send_sem=send_sem.at[target],
            recv_sem=recv_sem.at[head],
            device_id={"ctx": target},
            device_id_type=pl.DeviceIdType.MESH,
        )

    def own_copy(head):
        return pltpu.make_async_copy(send_ref.at[me], recv_ref.at[head], own_sem)

    def begin(head, _):
        @pl.when(owner_of(head, count) == me)
        def _():
            own_copy(head).start()

            def push(step, _):
                copy_for(head, lax.rem(me + step, count)).start()
                return 0

            lax.fori_loop(1, count, push, 0)

        return 0

    lax.fori_loop(0, HEADS, begin, 0)

    def finish(head, _):
        @pl.when(owner_of(head, count) == me)
        def _():
            own_copy(head).wait()

            def leave(step, _):
                copy_for(head, lax.rem(me + step, count)).wait_send()
                return 0

            lax.fori_loop(1, count, leave, 0)

        @pl.when(owner_of(head, count) != me)
        def _():
            copy_for(head, me).wait_recv()

        return 0

    lax.fori_loop(0, HEADS, finish, 0)


def to_rows(send, count, collective_id):
    rows = send.shape[1]
    return pl.pallas_call(
        partial(to_rows_kernel, count),
        out_shape=jax.ShapeDtypeStruct((HEADS, rows, LANES), low_type),
        in_specs=[pl.BlockSpec(memory_space=pltpu.VMEM)],
        out_specs=pl.BlockSpec(memory_space=pltpu.VMEM),
        scratch_shapes=[
            pltpu.SemaphoreType.DMA((count,)),
            pltpu.SemaphoreType.DMA((HEADS,)),
            pltpu.SemaphoreType.DMA,
        ],
        compiler_params=pltpu.CompilerParams(
            collective_id=collective_id, has_side_effects=True, vmem_limit_bytes=VMEM_BYTES
        ),
        cost_estimate=pl.CostEstimate(
            flops=rows * 250_000_000, bytes_accessed=send.size * 4, transcendentals=0
        ),
        name=f"to_rows_{rows}",
    )(send)


def project_kernel(x_ref, pack_ref, vec_ref, out_ref):
    rows, width = x_ref.shape
    half = rows // 2
    step = 4
    for base in range(0, HEADS, step):
        cols = slice(base * LANES, (base + step) * LANES)
        both = dot_nn(x_ref[...], pack_ref[:, width + cols.start : width + cols.stop])
        bias = vec_ref[1:2, base * HEAD_DIM : (base + step) * HEAD_DIM]
        blank = jnp.zeros((1, HEAD_DIM), jnp.float32)
        shifts = []
        for at in range(step):
            shifts += [blank, bias[:, at * HEAD_DIM : (at + 1) * HEAD_DIM]]
        both = (both + jnp.concatenate(shifts, axis=1)).astype(low_type)
        for at in range(step):
            out_ref[base + at, 0:rows, :] = both[:, at * LANES : (at + 1) * LANES]
        cols = slice(base * HEAD_DIM, (base + step) * HEAD_DIM)
        query = ((dot_nn(x_ref[...], pack_ref[:, cols]) + vec_ref[0:1, cols]) * 0.125).astype(low_type)
        for at in range(step):
            lanes = slice(at * HEAD_DIM, (at + 1) * HEAD_DIM)
            out_ref[base + at, rows : rows + half, :] = jnp.concatenate(
                [query[:half, lanes], query[half:, lanes]], axis=1
            )


def project(x, pack, vectors):
    rows = x.shape[0]
    vmem = pl.BlockSpec(memory_space=pltpu.VMEM)
    return pl.pallas_call(
        project_kernel,
        out_shape=jax.ShapeDtypeStruct((HEADS, rows + rows // 2, LANES), low_type),
        in_specs=[vmem] * 3,
        out_specs=vmem,
        compiler_params=pltpu.CompilerParams(vmem_limit_bytes=VMEM_BYTES),
        name="project",
    )(x, pack, vectors)


def tile_range(meta_ref, first, last, total, step):
    end_a, end_b, end_c = meta_ref[0], meta_ref[1], meta_ref[2]
    low = jnp.where(
        first >= end_c, end_c, jnp.where(first >= end_b, end_b, jnp.where(first >= end_a, end_a, 0))
    )
    high = jnp.where(
        last >= end_c,
        total,
        jnp.where(last >= end_b, end_c, jnp.where(last >= end_a, end_b, end_a)),
    )
    return low // step, (high + step - 1) // step


def attend_kernel(meta_ref, order_ref, recv_ref, out_ref, qa_ref, ka_ref, va_ref, sum_ref):
    count = recv_ref.shape[0]
    half = recv_ref.shape[1] // 3
    total = qa_ref.shape[0]

    @pl.when(meta_ref[3] == 1)
    def _():
        lane = lax.broadcasted_iota(jnp.int32, (half, LANES), 1)
        lower = lane < HEAD_DIM
        row = lax.broadcasted_iota(jnp.int32, (half, LANES), 0)

        def place(source, _):
            query = recv_ref[source, 2 * half :, :].astype(jnp.float32)
            for part in range(2):
                first = pl.multiple_of(order_ref[2 * source + part] * half, half)
                position = first + row
                segment = (
                    (position >= meta_ref[0]).astype(jnp.int32)
                    + (position >= meta_ref[1]).astype(jnp.int32)
                    + (position >= meta_ref[2]).astype(jnp.int32)
                )
                mine = (lane - HEAD_DIM) == segment
                other = (lane < HEAD_DIM + 4) & (~mine)
                pair = recv_ref[source, part * half : (part + 1) * half, :].astype(jnp.float32)
                if part == 1:
                    query = pltpu.roll(query, HEAD_DIM, 1)
                mark_k = jnp.where(
                    other, FAR, jnp.where((lane >= HEAD_DIM + 4) & (lane < HEAD_DIM + 7), 1.0, 0.0)
                )
                rows = pl.ds(first, half)
                qa_ref[rows, :] = jnp.where(lower, query, jnp.where(mine, 1.0, 0.0)).astype(low_type)
                ka_ref[rows, :] = jnp.where(lower, pair, mark_k).astype(low_type)
                va_ref[rows, :] = jnp.where(lower, 1.0, pair).astype(low_type)
            return 0

        lax.fori_loop(0, count, place, 0)

        def query_step(index, _):
            first = pl.multiple_of(index * TILE, TILE)
            rows = pl.ds(first, TILE)
            begin, end = tile_range(meta_ref, first, first + TILE - 1, total, 2 * TILE)
            query = qa_ref[rows, :]
            sum_ref[rows, :] = jnp.zeros((TILE, LANES), jnp.float32)

            def key_step(key_index, _):
                gained = 0.0
                for part in range(2):
                    keys = pl.ds(pl.multiple_of((2 * key_index + part) * TILE, TILE), TILE)
                    expo = jnp.exp(dot_nt(query, ka_ref[keys, :])).astype(low_type)
                    gained = gained + dot_nn(expo, va_ref[keys, :])
                sum_ref[rows, :] += gained
                return 0

            lax.fori_loop(begin, end, key_step, 0)
            return 0

        lax.fori_loop(0, total // TILE, query_step, 0)

        def give(source, _):
            parts = []
            for part in range(2):
                first = pl.multiple_of(order_ref[2 * source + part] * half, half)
                block = sum_ref[pl.ds(first, half), :]
                parts.append((block, pltpu.roll(block, HEAD_DIM, 1)))
            top = jnp.where(lower, parts[0][1], parts[1][0])
            bottom = jnp.where(lower, parts[0][0], parts[1][1])
            out_ref[source] = (top / bottom).astype(low_type)
            return 0

        lax.fori_loop(0, count, give, 0)


def attend(meta, order, recv):
    count, rows, _ = recv.shape
    total = count * rows * 2 // 3
    vmem = pl.BlockSpec(memory_space=pltpu.VMEM)
    smem = pl.BlockSpec(memory_space=pltpu.SMEM)
    whole = jax.ShapeDtypeStruct((total, LANES), low_type)
    return pl.pallas_call(
        attend_kernel,
        out_shape=(
            jax.ShapeDtypeStruct((count, rows // 3, LANES), low_type),
            whole,
            whole,
            whole,
            jax.ShapeDtypeStruct((total, LANES), jnp.float32),
        ),
        in_specs=[smem, smem, vmem],
        out_specs=(vmem,) * 5,
        compiler_params=pltpu.CompilerParams(vmem_limit_bytes=VMEM_BYTES),
        cost_estimate=pl.CostEstimate(
            flops=total * total * LANES * 8, bytes_accessed=total * LANES * 12, transcendentals=0
        ),
        name="attend",
    )(meta, order, recv)


def split_three(value):
    first = value.astype(low_type).astype(jnp.float32)
    rest = value - first
    second = rest.astype(low_type).astype(jnp.float32)
    return first, second, rest - second


def attend_back_kernel(
    meta_ref,
    order_ref,
    recv_ref,
    qa_ref,
    ka_ref,
    va_ref,
    sum_ref,
    out_ref,
    qb_ref,
    da_ref,
    kt_ref,
    dkv_ref,
    dq_ref,
    acc_ref,
):
    count = recv_ref.shape[0]
    half = recv_ref.shape[1]
    total = qa_ref.shape[0]

    @pl.when(meta_ref[3] == 1)
    def _():
        lane = lax.broadcasted_iota(jnp.int32, (half, LANES), 1)
        lower = lane < HEAD_DIM

        def place(source, _):
            given = recv_ref[source].astype(jnp.float32)
            for part in range(2):
                first = pl.multiple_of(order_ref[2 * source + part] * half, half)
                rows = pl.ds(first, half)
                block = sum_ref[rows, :]
                turned = pltpu.roll(block, HEAD_DIM, 1)
                d_context = pltpu.roll(given, HEAD_DIM, 1) if part == 0 else given
                product = jnp.where(lower, 0.0, d_context * (block / turned))
                minus = -jnp.sum(product, axis=1, keepdims=True)
                one, two, three = split_three(minus)
                mark = jnp.where(
                    lane == 0, one, jnp.where(lane == 1, two, jnp.where(lane == 2, three, 0.0))
                )
                da_ref[rows, :] = jnp.where(lower, mark, d_context).astype(low_type)
                one, two, three = split_three(-jnp.log(turned))
                at = lane - (HEAD_DIM + 4)
                mark = jnp.where(at == 0, one, jnp.where(at == 1, two, three))
                query = qa_ref[rows, :].astype(jnp.float32)
                qb_ref[rows, :] = jnp.where((at >= 0) & (at < 3), mark, query).astype(low_type)
            return 0

        lax.fori_loop(0, count, place, 0)

        def prepare(index, _):
            rows = pl.ds(pl.multiple_of(index * TILE, TILE), TILE)
            kt_ref[:, rows] = jnp.transpose(ka_ref[rows, :])[:HEAD_DIM, :]
            dkv_ref[rows, :] = jnp.zeros((TILE, LANES), jnp.float32)
            return 0

        lax.fori_loop(0, total // TILE, prepare, 0)

        lower_tile = lax.broadcasted_iota(jnp.int32, (TILE, LANES), 1) < HEAD_DIM

        def query_step(index, _):
            first = pl.multiple_of(index * TILE, TILE)
            rows = pl.ds(first, TILE)
            begin, end = tile_range(meta_ref, first, first + TILE - 1, total, TILE)
            query = qb_ref[rows, :]
            given = da_ref[rows, :]
            query_only = jnp.where(lower_tile, query.astype(jnp.float32), 0.0).astype(low_type)
            given_only = jnp.where(lower_tile, 0.0, given.astype(jnp.float32)).astype(low_type)
            acc_ref[...] = jnp.zeros_like(acc_ref)

            def key_step(key_index, _):
                keys = pl.ds(pl.multiple_of(key_index * TILE, TILE), TILE)
                prob = jnp.exp(dot_nt(ka_ref[keys, :], query))
                d_scores = (prob * dot_nt(va_ref[keys, :], given)).astype(low_type)
                dkv_ref[keys, :] += dot_nn(d_scores, query_only) + dot_nn(
                    prob.astype(low_type), given_only
                )
                acc_ref[...] += dot_nn(kt_ref[:, keys], d_scores)
                return 0

            lax.fori_loop(begin, end, key_step, 0)
            dq_ref[rows, :] = jnp.transpose(acc_ref[...])
            return 0

        lax.fori_loop(0, total // TILE, query_step, 0)

        def give(source, _):
            queries = []
            for part in range(2):
                first = pl.multiple_of(order_ref[2 * source + part] * half, half)
                rows = pl.ds(first, half)
                out_ref[source, part * half : (part + 1) * half, :] = dkv_ref[rows, :].astype(low_type)
                queries.append(dq_ref[rows, :])
            out_ref[source, 2 * half :, :] = jnp.concatenate(queries, axis=1).astype(low_type)
            return 0

        lax.fori_loop(0, count, give, 0)


def attend_back(meta, order, recv, qa, ka, va, sums):
    count, half, _ = recv.shape
    total = qa.shape[0]
    vmem = pl.BlockSpec(memory_space=pltpu.VMEM)
    smem = pl.BlockSpec(memory_space=pltpu.SMEM)
    return pl.pallas_call(
        attend_back_kernel,
        out_shape=jax.ShapeDtypeStruct((count, 3 * half, LANES), low_type),
        in_specs=[smem, smem] + [vmem] * 5,
        out_specs=vmem,
        scratch_shapes=[
            pltpu.VMEM((total, LANES), low_type),
            pltpu.VMEM((total, LANES), low_type),
            pltpu.VMEM((HEAD_DIM, total), low_type),
            pltpu.VMEM((total, LANES), jnp.float32),
            pltpu.VMEM((total, HEAD_DIM), jnp.float32),
            pltpu.VMEM((HEAD_DIM, TILE), jnp.float32),
        ],
        compiler_params=pltpu.CompilerParams(vmem_limit_bytes=VMEM_BYTES),
        cost_estimate=pl.CostEstimate(
            flops=total * total * LANES * 16, bytes_accessed=total * LANES * 16, transcendentals=0
        ),
        name="attend_back",
    )(meta, order, recv, qa, ka, va, sums)


PART_ORDERS = (("x", "z"), ("x", "z"), ("wa", "x", "z"), ("wa", "x", "z"))
GATHER_ORDERS = (("z", "x"), ("z", "x"), ("z", "x"), ("x", "z"))
PARTS = len(PART_ORDERS)
EARLY = sum(len(order) == 2 for order in PART_ORDERS)
STAGES = sum(len(order) for order in PART_ORDERS)
SIZES = {"wa": 2, "x": 2, "z": 4}


class Links:
    def __init__(self):
        me = lax.axis_index("ctx")
        self.at = {
            "core": lax.rem(me, 2),
            "x": lax.rem(me // 2, 2),
            "z": me // 4,
            "wa": lax.axis_index("wa"),
        }

    def peer(self, axis, value):
        at = dict(self.at)
        at[axis] = value
        return {"ctx": at["z"] * 4 + at["x"] * 2 + at["core"], "wa": at["wa"]}


def splits_rows(piece):
    return piece % 64 == 0


def grad_sum_kernel(*refs):
    refs = list(refs)
    sizes = (PARTS, PARTS, PARTS - EARLY, STAGES)
    g_refs, out_refs, core_bufs, bufs = (
        [refs.pop(0) for _ in range(number)] for number in sizes
    )
    core_bufs = [None] * EARLY + core_bufs
    send_sem, recv_sem = refs
    links = Links()
    core, x, z, wa = (links.at[name] for name in ("core", "x", "z", "wa"))
    barrier = pltpu.get_barrier_semaphore()
    peers = [links.peer("core", 1 - core), links.peer("x", 1 - x), links.peer("wa", 1 - wa)]
    peers += [links.peer("z", lax.rem(z + step, 4)) for step in range(1, 4)]
    for peer in peers:
        pl.semaphore_signal(barrier, inc=1, device_id=peer, device_id_type=pl.DeviceIdType.MESH)
    pl.semaphore_wait(barrier, len(peers))
    used = [0]

    def remote(src, dst, peer):
        index = used[0]
        used[0] += 1
        copy = pltpu.make_async_remote_copy(
            src_ref=src,
            dst_ref=dst,
            send_sem=send_sem.at[index],
            recv_sem=recv_sem.at[index],
            device_id=peer,
            device_id_type=pl.DeviceIdType.MESH,
        )
        copy.start()
        return copy

    def z_share(ref, value):
        piece, width = ref.shape[-2:]
        if value is None:
            return slice(None), slice(None)
        if splits_rows(piece):
            return pl.ds(pl.multiple_of(value * (piece // 4), 16), piece // 4), slice(None)
        return slice(None), pl.ds(pl.multiple_of(value * (width // 4), LANES), width // 4)

    def slab(part, held, axis=None, value=None):
        at = dict(links.at)
        if axis is not None:
            at[axis] = value
            held = held | {axis}
        return g_refs[part].at[
            pl.ds(0, 1) if part < EARLY else pl.ds(at["wa"], 1) if "wa" in held else pl.ds(0, 2),
            0 if part < EARLY else core,
            pl.ds(at["x"], 1) if "x" in held else pl.ds(0, 2),
            *z_share(g_refs[part], at["z"] if "z" in held else None),
        ]

    def add_into(target, sources):
        outer, inner, rows, _ = target.shape
        for a in range(outer):
            for b in range(inner):

                def add(group, _):
                    some = pl.ds(pl.multiple_of(group * 16, 16), 16)
                    total = target[a, b, some, :].astype(jnp.float32)
                    for source in sources:
                        total = total + source[a, b, some, :].astype(jnp.float32)
                    target[a, b, some, :] = total.astype(low_type)
                    return 0

                lax.fori_loop(0, rows // 16, add, 0)

    core_copies = [
        remote(g_refs[part].at[:, 1 - core], core_bufs[part], links.peer("core", 1 - core))
        if part >= EARLY
        else None
        for part in range(PARTS)
    ]
    first_buf = [sum(len(order) for order in PART_ORDERS[:part]) for part in range(PARTS)]

    def begin(part, stage):
        axis = PART_ORDERS[part][stage]
        held = set(PART_ORDERS[part][:stage])
        buf = bufs[first_buf[part] + stage]
        copies = []
        for step in range(1, SIZES[axis]):
            value = lax.rem(links.at[axis] + step, SIZES[axis])
            copies.append(
                remote(slab(part, held, axis, value), buf.at[step - 1], links.peer(axis, value))
            )
        return copies

    def out_slab(part, held):
        return out_refs[part].at[
            core,
            pl.ds(x, 1) if "x" in held else pl.ds(0, 2),
            *z_share(out_refs[part], z if "z" in held else None),
        ]

    def spread(part, stage):
        axis = GATHER_ORDERS[part][stage]
        block = out_slab(part, set(GATHER_ORDERS[part][stage:]))
        return [
            remote(block, block, links.peer(axis, lax.rem(links.at[axis] + step, SIZES[axis])))
            for step in range(1, SIZES[axis])
        ]

    def start_gather(part, stage):
        if stage < 2:
            return spread(part, stage)
        block = out_slab(part, set())
        return [remote(block, block, links.peer("core", 1 - core))]

    flying, passed = {}, {}
    for part in range(PARTS):
        passed[part] = 0 if part >= EARLY else 1
        flying[part] = begin(part, 0) if part < EARLY else [core_copies[part]]
    while any(flying.values()):
        for part in range(PARTS):
            if not flying[part]:
                continue
            order = PART_ORDERS[part]
            for copy in flying[part]:
                copy.wait()
            step = passed[part]
            passed[part] += 1
            if step == 0:
                add_into(slab(part, set()), [core_bufs[part]])
            elif step <= len(order):
                buf = bufs[first_buf[part] + step - 1]
                add_into(
                    slab(part, set(order[:step])),
                    [buf.at[at] for at in range(SIZES[order[step - 1]] - 1)],
                )
            if step < len(order):
                flying[part] = begin(part, step)
            elif step == len(order):
                out_slab(part, {"x", "z"})[...] = slab(part, {"wa", "x", "z"})[0]
                flying[part] = start_gather(part, 0)
            elif step <= len(order) + 2:
                flying[part] = start_gather(part, step - len(order))
            else:
                flying[part] = None


def grad_sum(grads, collective_id):
    bufs, core_bufs, outs, given = [], [], [], []
    for part, grad in enumerate(grads):
        rows, width = grad.shape
        early = part < EARLY
        piece = rows // 2 if early else rows // 8
        shape = {"wa": 1 if early else 2, "x": 2, "z": 4}
        for axis in PART_ORDERS[part]:
            shape[axis] //= SIZES[axis]
            share = (
                (piece * shape["z"] // 4, width)
                if splits_rows(piece)
                else (piece, width * shape["z"] // 4)
            )
            bufs.append(
                pltpu.VMEM((SIZES[axis] - 1, shape["wa"], shape["x"], *share), low_type)
            )
        if not early:
            core_bufs.append(pltpu.VMEM((2, 2, piece, width), low_type))
        outs.append(jax.ShapeDtypeStruct((2, 2, piece, width), low_type))
        lead = (1, 1) if early else (2, 2)
        given.append(grad.reshape(*lead, 2, piece, width))
    vmem = pl.BlockSpec(memory_space=pltpu.VMEM)
    size = sum(grad.size for grad in grads)
    sums = pl.pallas_call(
        grad_sum_kernel,
        out_shape=tuple(outs),
        in_specs=[vmem] * PARTS,
        out_specs=(vmem,) * PARTS,
        scratch_shapes=[
            *core_bufs,
            *bufs,
            pltpu.SemaphoreType.DMA((16 * PARTS,)),
            pltpu.SemaphoreType.DMA((16 * PARTS,)),
        ],
        compiler_params=pltpu.CompilerParams(
            collective_id=collective_id, has_side_effects=True, vmem_limit_bytes=VMEM_BYTES
        ),
        cost_estimate=pl.CostEstimate(
            flops=size * 20_000, bytes_accessed=size * 4, transcendentals=0
        ),
        name="grad_sum",
    )(*given)
    return [part.reshape(-1, part.shape[-1]) for part in sums]


def column_sums(terms, lanes):
    block = jnp.stack([jnp.sum(term, axis=0) for term in terms], axis=1).astype(low_type)
    return jnp.pad(block, ((0, 0), (0, lanes - len(terms))))


def reduce_shards(grad):
    part = lax.psum_scatter(
        grad.astype(low_type), ("wa", "ctx"), scatter_dimension=0, tiled=True
    )
    return lax.all_gather(part, "ctx", axis=0, tiled=True)


def body(
    count,
    tokens,
    cotangent,
    lengths,
    block_order,
    w_query,
    b_query,
    w_key,
    w_value,
    b_value,
    w_out,
    b_out,
    gain_one,
    shift_one,
    w_up,
    b_up,
    w_down,
    b_down,
    gain_two,
    shift_two,
):
    inputs = tokens[0]
    tok_rows, width = inputs.shape
    wide = w_up.shape[1]
    half = tok_rows // 2
    shard = w_query.shape[0]
    direct = count == 16 and width == 2 * shard and shard % 64 == 0 and wide == 4 * width
    me = lax.axis_index("ctx")
    seq_ends = jnp.cumsum(lengths[0])
    own_blocks = lax.dynamic_slice(block_order, (2 * me,), (2,))
    position = (own_blocks[:, None] * half + jnp.arange(half, dtype=jnp.int32)[None, :]).reshape(-1)
    own_seg = segment_of(position, seq_ends)
    owns = jnp.any(me == jnp.arange(HEADS, dtype=jnp.int32) * count // HEADS).astype(jnp.int32)
    meta = jnp.concatenate([seq_ends.astype(jnp.int32), owns[None]])

    core = me % 2
    wa = lax.axis_index("wa")

    def fetch_half(shard_block, after=None):
        if not direct:
            return None
        if after is not None:
            shard_block, _ = lax.optimization_barrier((shard_block, after))
        size, columns = shard_block.shape
        part = lax.dynamic_slice(shard_block, (core * (size // 2), 0), (size // 2, columns))
        return lax.ppermute(part, "wa", [(0, 1), (1, 0)])

    def gather_rows(shard_block, fetched):
        if not direct:
            return lax.all_gather(shard_block, "wa", axis=0, tiled=True)
        size, columns = shard_block.shape
        swapped = lax.ppermute(fetched, "ctx", [(k, k ^ 1) for k in range(count)])
        other = (1 - wa) * size
        whole = jnp.zeros((2 * size, columns), shard_block.dtype)
        whole = lax.dynamic_update_slice(whole, shard_block, (wa * size, 0))
        whole = lax.dynamic_update_slice(whole, fetched, (other + core * (size // 2), 0))
        return lax.dynamic_update_slice(whole, swapped, (other + (1 - core) * (size // 2), 0))

    pair = jnp.stack(
        [
            w_key.astype(low_type).reshape(shard, HEADS, HEAD_DIM),
            w_value.astype(low_type).reshape(shard, HEADS, HEAD_DIM),
        ],
        axis=2,
    ).reshape(shard, 2 * width)
    own_vectors = jnp.concatenate(
        [
            jnp.stack(
                [b_query, b_value, b_out, gain_one, shift_one, gain_two, shift_two, b_down]
            ),
            b_up.reshape(4, shard),
            jnp.zeros((4, shard), jnp.float32),
        ],
        axis=0,
    ).astype(low_type)
    if direct:
        other_vectors = lax.ppermute(own_vectors, "wa", [(0, 1), (1, 0)])
        vector_rows = jnp.where(
            wa == 0,
            jnp.concatenate([own_vectors, other_vectors], axis=1),
            jnp.concatenate([other_vectors, own_vectors], axis=1),
        ).astype(jnp.float32)
    else:
        vector_rows = (
            lax.all_gather(own_vectors, "wa", axis=1, tiled=True)
        ).astype(jnp.float32)

    first_shard = jnp.concatenate([w_query.astype(low_type), pair], axis=1)
    fetched = fetch_half(first_shard)
    later_shards = (
        w_out.astype(low_type),
        w_up.astype(low_type),
        w_down.astype(low_type),
    )
    later_fetched = tuple(fetch_half(block, fetched) for block in later_shards)
    first_pack = gather_rows(first_shard, fetched)
    query_weight = first_pack[:, :width]
    pair_weight = first_pack[:, width : 3 * width]
    out_bias, gain_first, shift_first, gain_second, shift_second, down_bias = (
        vector_rows[index] for index in range(2, 8)
    )
    up_bias = (
        vector_rows[8:12].reshape(4, width // shard, shard).transpose(1, 0, 2).reshape(-1)
    )

    packed = project(inputs, first_pack, vector_rows)
    at_head = to_heads(packed, count, 0)
    context_out, qa, ka, va, sums = attend(meta, block_order, at_head)
    context_out, later_fetched = lax.optimization_barrier((context_out, later_fetched))
    out_weight, up_weight, down_weight = (
        gather_rows(block, half_block) for block, half_block in zip(later_shards, later_fetched)
    )
    context_in = to_rows(context_out, count, 1)
    context_low = (
        context_in.reshape(HEADS, half, 2, HEAD_DIM).transpose(2, 1, 0, 3).reshape(tok_rows, width)
    )

    attn_out = jnp.dot(context_low, out_weight, preferred_element_type=jnp.float32) + out_bias
    h_one = inputs.astype(jnp.float32) + attn_out
    norm_one, norm_one_back = jax.vjp(layer_norm, h_one, gain_first, shift_first)
    norm_low = norm_one.astype(low_type)
    up_pre = jnp.dot(norm_low, up_weight, preferred_element_type=jnp.float32) + up_bias
    gelu_out, gelu_back = jax.vjp(partial(jax.nn.gelu, approximate=False), up_pre)
    gelu_low = gelu_out.astype(low_type)
    down_out = jnp.dot(gelu_low, down_weight, preferred_element_type=jnp.float32) + down_bias
    h_two = norm_one + down_out
    result, norm_two_back = jax.vjp(layer_norm, h_two, gain_second, shift_second)
    activations = result.astype(low_type)[None]
    valid = (own_seg < 3).astype(jnp.float32)
    g_out = cotangent[0].astype(jnp.float32) * valid[:, None]
    d_htwo, grad_gain_second, grad_shift_second = norm_two_back(g_out)
    d_down = d_htwo.astype(low_type)
    d_gelu = jnp.einsum("td,fd->tf", d_down, down_weight, preferred_element_type=jnp.float32)
    (d_uppre,) = gelu_back(d_gelu)
    d_up = d_uppre.astype(low_type)
    d_yone = d_htwo + jnp.einsum("tf,df->td", d_up, up_weight, preferred_element_type=jnp.float32)
    d_hone, grad_gain_first, grad_shift_first = norm_one_back(d_yone)
    d_attn = d_hone.astype(low_type)
    d_context = jnp.einsum("td,cd->tc", d_attn, out_weight, preferred_element_type=jnp.float32)
    context_back = (
        d_context.astype(low_type)
        .reshape(2, half, HEADS, HEAD_DIM)
        .transpose(2, 1, 0, 3)
        .reshape(HEADS, half, LANES)
    )

    grad_wdown = jnp.einsum("tf,td->fd", gelu_low, d_down, preferred_element_type=jnp.float32)
    grad_wup = jnp.einsum("td,tf->df", norm_low, d_up, preferred_element_type=jnp.float32)
    grad_wout = jnp.einsum("tc,td->cd", context_low, d_attn, preferred_element_type=jnp.float32)
    up_bias_sums = jnp.sum(d_up.astype(jnp.float32), axis=0)
    lanes = 2 * LANES
    vec_block = jnp.concatenate(
        [
            jnp.stack(
                [
                    jnp.sum(d_attn.astype(jnp.float32), axis=0),
                    grad_gain_first,
                    grad_shift_first,
                    jnp.sum(d_down.astype(jnp.float32), axis=0),
                    grad_gain_second,
                    grad_shift_second,
                ],
                axis=1,
            ),
            up_bias_sums.reshape(width // shard, 4, shard).transpose(0, 2, 1).reshape(width, 4),
        ],
        axis=1,
    ).astype(low_type)
    out_block = jnp.concatenate(
        [grad_wout.astype(low_type), jnp.pad(vec_block, ((0, 0), (0, lanes - 10)))], axis=1
    )
    up_block = grad_wup.astype(low_type)
    down_block = grad_wdown.astype(low_type)
    def add_low(mine, given):
        return (mine.astype(jnp.float32) + given.astype(jnp.float32)).astype(low_type)

    def core_halves(block):
        view = block.reshape(2, 2, -1, block.shape[1])
        keep = jnp.where(core == 0, view[:, 0], view[:, 1])
        give = jnp.where(core == 0, view[:, 1], view[:, 0])
        return keep, lax.ppermute(give, "ctx", [(k, k ^ 1) for k in range(count)])

    def wa_halves(block):
        keep = jnp.where(wa == 0, block[0], block[1])
        give = jnp.where(wa == 0, block[1], block[0])
        return keep, lax.ppermute(give, "wa", [(0, 1), (1, 0)])

    context_back, down_block, out_block, up_block = lax.optimization_barrier(
        (context_back, down_block, out_block, up_block)
    )
    if direct:
        halves = [core_halves(block) for block in (up_block, down_block)]
        back_at_head = to_heads(context_back, count, 2)
        back_at_head, halves = lax.optimization_barrier((back_at_head, halves))
        halves = [wa_halves(add_low(*pair)) for pair in halves]
        grads_out = attend_back(meta, block_order, back_at_head, qa, ka, va, sums)
        grads_out, halves = lax.optimization_barrier((grads_out, halves))
        early = [add_low(*pair) for pair in halves]
    else:
        back_at_head = to_heads(context_back, count, 2)
        grads_out = attend_back(meta, block_order, back_at_head, qa, ka, va, sums)
    grads_in = to_rows(grads_out, count, 3)

    d_pair = grads_in[:, :tok_rows, :].transpose(1, 0, 2).reshape(tok_rows, 2 * width)
    d_queries = (
        grads_in[:, tok_rows:, :]
        .reshape(HEADS, half, 2, HEAD_DIM)
        .transpose(2, 1, 0, 3)
        .reshape(tok_rows, width)
        * jnp.asarray(0.125, low_type)
    )
    d_keys, d_values = (
        grads_in[:, :tok_rows, low : low + HEAD_DIM].transpose(1, 0, 2).reshape(tok_rows, width)
        for low in (0, HEAD_DIM)
    )
    d_all = jnp.concatenate(
        [d_queries, d_keys, d_values, jnp.zeros((tok_rows, lanes), low_type)], axis=1
    )
    grad_all = jnp.einsum("tc,td->cd", inputs, d_all, preferred_element_type=jnp.float32)
    last_block = lax.dynamic_update_slice(
        grad_all.astype(low_type),
        column_sums([d_queries.astype(jnp.float32), d_values.astype(jnp.float32)], lanes),
        (0, 3 * width),
    )
    if direct:
        up_sum, down_sum, last_sum, out_sum = grad_sum((*early, last_block, out_block), 4)
    else:
        up_sum, down_sum, last_sum, out_sum = (
            reduce_shards(block) for block in (up_block, down_block, last_block, out_block)
        )
    d_input = (
        d_hone
        + jnp.einsum("td,cd->tc", d_queries, query_weight, preferred_element_type=jnp.float32)
        + jnp.einsum("td,cd->tc", d_pair, pair_weight, preferred_element_type=jnp.float32)
    )
    input_grad = d_input.astype(low_type)[None]

    wide_grad = last_sum.astype(jnp.float32)
    out_grad = out_sum.astype(jnp.float32)
    return (
        activations,
        input_grad,
        wide_grad[:, :width],
        wide_grad[:, 3 * width],
        wide_grad[:, width : 2 * width],
        wide_grad[:, 2 * width : 3 * width],
        wide_grad[:, 3 * width + 1],
        out_grad[:, :width],
        out_grad[:, width],
        out_grad[:, width + 1],
        out_grad[:, width + 2],
        up_sum.astype(jnp.float32),
        out_grad[:, width + 6 : width + 10].T.reshape(-1),
        down_sum.astype(jnp.float32),
        out_grad[:, width + 3],
        out_grad[:, width + 4],
        out_grad[:, width + 5],
    )


def solution(mesh):
    placed = (
        P("wa", "ctx", None),
        P("wa", "ctx", None),
        P("wa", None),
        P(),
        P("wa", None),
        P("wa"),
        P("wa", None),
        P("wa", None),
        P("wa"),
        P("wa", None),
        P("wa"),
        P("wa"),
        P("wa"),
        P("wa", None),
        P("wa"),
        P("wa", None),
        P("wa"),
        P("wa"),
        P("wa"),
    )
    return jax.shard_map(
        partial(body, mesh.shape["ctx"]),
        mesh=mesh,
        in_specs=placed,
        out_specs=(
            P("wa", "ctx", None),
            P("wa", "ctx", None),
            P("wa", None),
            P("wa"),
            P("wa", None),
            P("wa", None),
            P("wa"),
            P("wa", None),
            P("wa"),
            P("wa"),
            P("wa"),
            P("wa", None),
            P("wa"),
            P("wa", None),
            P("wa"),
            P("wa"),
            P("wa"),
        ),
        check_vma=False,
    )
```

```python
from functools import partial

import jax
import jax.numpy as jnp
from jax import lax
from jax.experimental import pallas as pl
from jax.experimental.pallas import tpu as pltpu
from jax.sharding import PartitionSpec as P

HEADS = 12
HEAD_DIM = 64
LANES = 128
TILE = 512
FAR = -(2.0**40)
VMEM_BYTES = 60 << 20

low_type = jnp.bfloat16
epsilon = 1e-05


def dot_nt(left, right):
    return lax.dot_general(
        left, right, (((1,), (1,)), ((), ())), preferred_element_type=jnp.float32
    )


def dot_nn(left, right):
    return lax.dot_general(
        left, right, (((1,), (0,)), ((), ())), preferred_element_type=jnp.float32
    )


def layer_norm(hidden, gain_vec, shift_vec):
    centre = hidden - jnp.mean(hidden, axis=-1, keepdims=True)
    spread = jnp.mean(centre * centre, axis=-1, keepdims=True)
    return centre * lax.rsqrt(spread + epsilon) * gain_vec + shift_vec


def segment_of(position, seq_ends):
    return jnp.sum((position[:, None] >= seq_ends[None, :]).astype(jnp.int32), axis=1)


def owner_of(head, count):
    return head * count // HEADS


def greet_all(count, me):
    barrier = pltpu.get_barrier_semaphore()

    def greet(step, _):
        other = lax.rem(me + step, count)
        pl.semaphore_signal(
            barrier, inc=1, device_id={"ctx": other}, device_id_type=pl.DeviceIdType.MESH
        )
        return 0

    lax.fori_loop(1, count, greet, 0)
    pl.semaphore_wait(barrier, count - 1)


def to_heads_kernel(count, send_ref, recv_ref, send_sem, recv_sem, own_sem):
    me = lax.axis_index("ctx")
    greet_all(count, me)
    first = me * HEADS // count + 1

    def copy_for(head, source, owner):
        return pltpu.make_async_remote_copy(
            src_ref=send_ref.at[head],
            dst_ref=recv_ref.at[source],
            send_sem=send_sem.at[head],
            recv_sem=recv_sem.at[source],
            device_id={"ctx": owner},
            device_id_type=pl.DeviceIdType.MESH,
        )

    def own_copy(head):
        return pltpu.make_async_copy(send_ref.at[head], recv_ref.at[me], own_sem)

    def begin(step, _):
        head = lax.rem(first + step, HEADS)
        owner = owner_of(head, count)

        @pl.when(owner != me)
        def _():
            copy_for(head, me, owner).start()

        @pl.when(owner == me)
        def _():
            own_copy(head).start()

        return 0

    lax.fori_loop(0, HEADS, begin, 0)

    def finish(head, _):
        owner = owner_of(head, count)

        @pl.when(owner != me)
        def _():
            copy_for(head, me, owner).wait_send()

        @pl.when(owner == me)
        def _():
            own_copy(head).wait()

            def arrive(source, _):
                @pl.when(source != me)
                def _():
                    copy_for(head, source, owner).wait_recv()

                return 0

            lax.fori_loop(0, count, arrive, 0)

        return 0

    lax.fori_loop(0, HEADS, finish, 0)


def to_heads(send, count, collective_id):
    rows = send.shape[1]
    return pl.pallas_call(
        partial(to_heads_kernel, count),
        out_shape=jax.ShapeDtypeStruct((count, rows, LANES), low_type),
        in_specs=[pl.BlockSpec(memory_space=pltpu.VMEM)],
        out_specs=pl.BlockSpec(memory_space=pltpu.VMEM),
        scratch_shapes=[
            pltpu.SemaphoreType.DMA((HEADS,)),
            pltpu.SemaphoreType.DMA((count,)),
            pltpu.SemaphoreType.DMA,
        ],
        compiler_params=pltpu.CompilerParams(
            collective_id=collective_id, has_side_effects=True, vmem_limit_bytes=VMEM_BYTES
        ),
        cost_estimate=pl.CostEstimate(
            flops=rows * 250_000_000, bytes_accessed=send.size * 4, transcendentals=0
        ),
        name=f"to_heads_{rows}",
    )(send)


def to_rows_kernel(count, send_ref, recv_ref, send_sem, recv_sem, own_sem):
    me = lax.axis_index("ctx")
    greet_all(count, me)

    def copy_for(head, target):
        return pltpu.make_async_remote_copy(
            src_ref=send_ref.at[target],
            dst_ref=recv_ref.at[head],
            send_sem=send_sem.at[target],
            recv_sem=recv_sem.at[head],
            device_id={"ctx": target},
            device_id_type=pl.DeviceIdType.MESH,
        )

    def own_copy(head):
        return pltpu.make_async_copy(send_ref.at[me], recv_ref.at[head], own_sem)

    def begin(head, _):
        @pl.when(owner_of(head, count) == me)
        def _():
            own_copy(head).start()

            def push(step, _):
                copy_for(head, lax.rem(me + step, count)).start()
                return 0

            lax.fori_loop(1, count, push, 0)

        return 0

    lax.fori_loop(0, HEADS, begin, 0)

    def finish(head, _):
        @pl.when(owner_of(head, count) == me)
        def _():
            own_copy(head).wait()

            def leave(step, _):
                copy_for(head, lax.rem(me + step, count)).wait_send()
                return 0

            lax.fori_loop(1, count, leave, 0)

        @pl.when(owner_of(head, count) != me)
        def _():
            copy_for(head, me).wait_recv()

        return 0

    lax.fori_loop(0, HEADS, finish, 0)


def to_rows(send, count, collective_id):
    rows = send.shape[1]
    return pl.pallas_call(
        partial(to_rows_kernel, count),
        out_shape=jax.ShapeDtypeStruct((HEADS, rows, LANES), low_type),
        in_specs=[pl.BlockSpec(memory_space=pltpu.VMEM)],
        out_specs=pl.BlockSpec(memory_space=pltpu.VMEM),
        scratch_shapes=[
            pltpu.SemaphoreType.DMA((count,)),
            pltpu.SemaphoreType.DMA((HEADS,)),
            pltpu.SemaphoreType.DMA,
        ],
        compiler_params=pltpu.CompilerParams(
            collective_id=collective_id, has_side_effects=True, vmem_limit_bytes=VMEM_BYTES
        ),
        cost_estimate=pl.CostEstimate(
            flops=rows * 250_000_000, bytes_accessed=send.size * 4, transcendentals=0
        ),
        name=f"to_rows_{rows}",
    )(send)


def project_kernel(x_ref, pack_ref, vec_ref, out_ref):
    rows, width = x_ref.shape
    half = rows // 2
    step = 4
    for base in range(0, HEADS, step):
        cols = slice(base * LANES, (base + step) * LANES)
        both = dot_nn(x_ref[...], pack_ref[:, width + cols.start : width + cols.stop])
        bias = vec_ref[1:2, base * HEAD_DIM : (base + step) * HEAD_DIM]
        blank = jnp.zeros((1, HEAD_DIM), jnp.float32)
        shifts = []
        for at in range(step):
            shifts += [blank, bias[:, at * HEAD_DIM : (at + 1) * HEAD_DIM]]
        both = (both + jnp.concatenate(shifts, axis=1)).astype(low_type)
        for at in range(step):
            out_ref[base + at, 0:rows, :] = both[:, at * LANES : (at + 1) * LANES]
        cols = slice(base * HEAD_DIM, (base + step) * HEAD_DIM)
        query = ((dot_nn(x_ref[...], pack_ref[:, cols]) + vec_ref[0:1, cols]) * 0.125).astype(low_type)
        for at in range(step):
            lanes = slice(at * HEAD_DIM, (at + 1) * HEAD_DIM)
            out_ref[base + at, rows : rows + half, :] = jnp.concatenate(
                [query[:half, lanes], query[half:, lanes]], axis=1
            )


def project(x, pack, vectors):
    rows = x.shape[0]
    vmem = pl.BlockSpec(memory_space=pltpu.VMEM)
    return pl.pallas_call(
        project_kernel,
        out_shape=jax.ShapeDtypeStruct((HEADS, rows + rows // 2, LANES), low_type),
        in_specs=[vmem] * 3,
        out_specs=vmem,
        compiler_params=pltpu.CompilerParams(vmem_limit_bytes=VMEM_BYTES),
        name="project",
    )(x, pack, vectors)


def unpack_kernel(grads_ref, all_ref, pair_ref, sums_ref):
    rows, width = pair_ref.shape[0], pair_ref.shape[1] // 2
    half = rows // 2
    low_lanes, high_lanes = slice(0, HEAD_DIM), slice(HEAD_DIM, LANES)
    for base in range(0, HEADS, 2):
        at = base * HEAD_DIM
        for head in (base, base + 1):
            pair_ref[:, head * LANES : (head + 1) * LANES] = grads_ref[head, 0:rows, :]
        first, second = grads_ref[base], grads_ref[base + 1]
        for part, lanes in ((0, low_lanes), (1, high_lanes)):
            query = jnp.concatenate([first[rows:, lanes], second[rows:, lanes]], axis=1)
            all_ref[part * half : (part + 1) * half, at : at + LANES] = (
                query.astype(jnp.float32) * 0.125
            ).astype(low_type)
            kept = jnp.concatenate([first[:rows, lanes], second[:rows, lanes]], axis=1)
            start = (part + 1) * width + at
            all_ref[:, start : start + LANES] = kept
    lanes = all_ref.shape[1] - 3 * width
    all_ref[:, 3 * width :] = jnp.zeros((rows, lanes), low_type)
    query_sums = jnp.sum(all_ref[:, 0:width].astype(jnp.float32), axis=0, keepdims=True)
    value_sums = jnp.sum(
        all_ref[:, 2 * width : 3 * width].astype(jnp.float32), axis=0, keepdims=True
    )
    row = lax.broadcasted_iota(jnp.int32, (LANES, width), 0)
    block = jnp.where(row == 0, query_sums, jnp.where(row == 1, value_sums, 0.0))
    sums_ref[:, 0:LANES] = jnp.transpose(block).astype(low_type)
    sums_ref[:, LANES:] = jnp.zeros((width, lanes - LANES), low_type)


def unpack(grads, width):
    rows = grads.shape[1] * 2 // 3
    lanes = 2 * LANES
    vmem = pl.BlockSpec(memory_space=pltpu.VMEM)
    return pl.pallas_call(
        unpack_kernel,
        out_shape=(
            jax.ShapeDtypeStruct((rows, 3 * width + lanes), low_type),
            jax.ShapeDtypeStruct((rows, 2 * width), low_type),
            jax.ShapeDtypeStruct((width, lanes), low_type),
        ),
        in_specs=[vmem],
        out_specs=(vmem,) * 3,
        compiler_params=pltpu.CompilerParams(vmem_limit_bytes=VMEM_BYTES),
        name="unpack",
    )(grads)


def tile_range(meta_ref, first, last, total, step):
    end_a, end_b, end_c = meta_ref[0], meta_ref[1], meta_ref[2]
    low = jnp.where(
        first >= end_c, end_c, jnp.where(first >= end_b, end_b, jnp.where(first >= end_a, end_a, 0))
    )
    high = jnp.where(
        last >= end_c,
        total,
        jnp.where(last >= end_b, end_c, jnp.where(last >= end_a, end_b, end_a)),
    )
    return low // step, (high + step - 1) // step


def attend_kernel(meta_ref, order_ref, recv_ref, out_ref, qa_ref, ka_ref, va_ref, sum_ref):
    count = recv_ref.shape[0]
    half = recv_ref.shape[1] // 3
    total = qa_ref.shape[0]

    @pl.when(meta_ref[3] == 1)
    def _():
        lane = lax.broadcasted_iota(jnp.int32, (half, LANES), 1)
        lower = lane < HEAD_DIM
        row = lax.broadcasted_iota(jnp.int32, (half, LANES), 0)

        def place(source, _):
            query = recv_ref[source, 2 * half :, :].astype(jnp.float32)
            for part in range(2):
                first = pl.multiple_of(order_ref[2 * source + part] * half, half)
                position = first + row
                segment = (
                    (position >= meta_ref[0]).astype(jnp.int32)
                    + (position >= meta_ref[1]).astype(jnp.int32)
                    + (position >= meta_ref[2]).astype(jnp.int32)
                )
                mine = (lane - HEAD_DIM) == segment
                other = (lane < HEAD_DIM + 4) & (~mine)
                pair = recv_ref[source, part * half : (part + 1) * half, :].astype(jnp.float32)
                if part == 1:
                    query = pltpu.roll(query, HEAD_DIM, 1)
                mark_k = jnp.where(
                    other, FAR, jnp.where((lane >= HEAD_DIM + 4) & (lane < HEAD_DIM + 7), 1.0, 0.0)
                )
                rows = pl.ds(first, half)
                qa_ref[rows, :] = jnp.where(lower, query, jnp.where(mine, 1.0, 0.0)).astype(low_type)
                ka_ref[rows, :] = jnp.where(lower, pair, mark_k).astype(low_type)
                va_ref[rows, :] = jnp.where(lower, 1.0, pair).astype(low_type)
            return 0

        lax.fori_loop(0, count, place, 0)

        def query_step(index, _):
            first = pl.multiple_of(index * TILE, TILE)
            rows = pl.ds(first, TILE)
            begin, end = tile_range(meta_ref, first, first + TILE - 1, total, 2 * TILE)
            query = qa_ref[rows, :]
            sum_ref[rows, :] = jnp.zeros((TILE, LANES), jnp.float32)

            def key_step(key_index, _):
                gained = 0.0
                for part in range(2):
                    keys = pl.ds(pl.multiple_of((2 * key_index + part) * TILE, TILE), TILE)
                    expo = jnp.exp(dot_nt(query, ka_ref[keys, :])).astype(low_type)
                    gained = gained + dot_nn(expo, va_ref[keys, :])
                sum_ref[rows, :] += gained
                return 0

            lax.fori_loop(begin, end, key_step, 0)
            return 0

        lax.fori_loop(0, total // TILE, query_step, 0)

        def give(source, _):
            parts = []
            for part in range(2):
                first = pl.multiple_of(order_ref[2 * source + part] * half, half)
                block = sum_ref[pl.ds(first, half), :]
                parts.append((block, pltpu.roll(block, HEAD_DIM, 1)))
            top = jnp.where(lower, parts[0][1], parts[1][0])
            bottom = jnp.where(lower, parts[0][0], parts[1][1])
            out_ref[source] = (top / bottom).astype(low_type)
            return 0

        lax.fori_loop(0, count, give, 0)


def attend(meta, order, recv):
    count, rows, _ = recv.shape
    total = count * rows * 2 // 3
    vmem = pl.BlockSpec(memory_space=pltpu.VMEM)
    smem = pl.BlockSpec(memory_space=pltpu.SMEM)
    whole = jax.ShapeDtypeStruct((total, LANES), low_type)
    return pl.pallas_call(
        attend_kernel,
        out_shape=(
            jax.ShapeDtypeStruct((count, rows // 3, LANES), low_type),
            whole,
            whole,
            whole,
            jax.ShapeDtypeStruct((total, LANES), jnp.float32),
        ),
        in_specs=[smem, smem, vmem],
        out_specs=(vmem,) * 5,
        compiler_params=pltpu.CompilerParams(vmem_limit_bytes=VMEM_BYTES),
        cost_estimate=pl.CostEstimate(
            flops=total * total * LANES * 8, bytes_accessed=total * LANES * 12, transcendentals=0
        ),
        name="attend",
    )(meta, order, recv)


def split_three(value):
    first = value.astype(low_type).astype(jnp.float32)
    rest = value - first
    second = rest.astype(low_type).astype(jnp.float32)
    return first, second, rest - second


def attend_back_kernel(
    meta_ref,
    order_ref,
    recv_ref,
    qa_ref,
    ka_ref,
    va_ref,
    sum_ref,
    out_ref,
    qb_ref,
    da_ref,
    kt_ref,
    dkv_ref,
    dq_ref,
    acc_ref,
):
    count = recv_ref.shape[0]
    half = recv_ref.shape[1]
    total = qa_ref.shape[0]

    @pl.when(meta_ref[3] == 1)
    def _():
        lane = lax.broadcasted_iota(jnp.int32, (half, LANES), 1)
        lower = lane < HEAD_DIM

        def place(source, _):
            given = recv_ref[source].astype(jnp.float32)
            for part in range(2):
                first = pl.multiple_of(order_ref[2 * source + part] * half, half)
                rows = pl.ds(first, half)
                block = sum_ref[rows, :]
                turned = pltpu.roll(block, HEAD_DIM, 1)
                d_context = pltpu.roll(given, HEAD_DIM, 1) if part == 0 else given
                product = jnp.where(lower, 0.0, d_context * (block / turned))
                minus = -jnp.sum(product, axis=1, keepdims=True)
                one, two, three = split_three(minus)
                mark = jnp.where(
                    lane == 0, one, jnp.where(lane == 1, two, jnp.where(lane == 2, three, 0.0))
                )
                da_ref[rows, :] = jnp.where(lower, mark, d_context).astype(low_type)
                one, two, three = split_three(-jnp.log(turned))
                at = lane - (HEAD_DIM + 4)
                mark = jnp.where(at == 0, one, jnp.where(at == 1, two, three))
                query = qa_ref[rows, :].astype(jnp.float32)
                qb_ref[rows, :] = jnp.where((at >= 0) & (at < 3), mark, query).astype(low_type)
            return 0

        lax.fori_loop(0, count, place, 0)

        def prepare(index, _):
            rows = pl.ds(pl.multiple_of(index * TILE, TILE), TILE)
            kt_ref[:, rows] = jnp.transpose(ka_ref[rows, :])[:HEAD_DIM, :]
            dkv_ref[rows, :] = jnp.zeros((TILE, LANES), jnp.float32)
            return 0

        lax.fori_loop(0, total // TILE, prepare, 0)

        lower_tile = lax.broadcasted_iota(jnp.int32, (TILE, LANES), 1) < HEAD_DIM

        def query_step(index, _):
            first = pl.multiple_of(index * TILE, TILE)
            rows = pl.ds(first, TILE)
            begin, end = tile_range(meta_ref, first, first + TILE - 1, total, TILE)
            query = qb_ref[rows, :]
            given = da_ref[rows, :]
            query_only = jnp.where(lower_tile, query.astype(jnp.float32), 0.0).astype(low_type)
            given_only = jnp.where(lower_tile, 0.0, given.astype(jnp.float32)).astype(low_type)
            acc_ref[...] = jnp.zeros_like(acc_ref)

            def key_step(key_index, _):
                keys = pl.ds(pl.multiple_of(key_index * TILE, TILE), TILE)
                prob = jnp.exp(dot_nt(ka_ref[keys, :], query))
                d_scores = (prob * dot_nt(va_ref[keys, :], given)).astype(low_type)
                dkv_ref[keys, :] += dot_nn(d_scores, query_only) + dot_nn(
                    prob.astype(low_type), given_only
                )
                acc_ref[...] += dot_nn(kt_ref[:, keys], d_scores)
                return 0

            lax.fori_loop(begin, end, key_step, 0)
            dq_ref[rows, :] = jnp.transpose(acc_ref[...])
            return 0

        lax.fori_loop(0, total // TILE, query_step, 0)

        def give(source, _):
            queries = []
            for part in range(2):
                first = pl.multiple_of(order_ref[2 * source + part] * half, half)
                rows = pl.ds(first, half)
                out_ref[source, part * half : (part + 1) * half, :] = dkv_ref[rows, :].astype(low_type)
                queries.append(dq_ref[rows, :])
            out_ref[source, 2 * half :, :] = jnp.concatenate(queries, axis=1).astype(low_type)
            return 0

        lax.fori_loop(0, count, give, 0)


def attend_back(meta, order, recv, qa, ka, va, sums):
    count, half, _ = recv.shape
    total = qa.shape[0]
    vmem = pl.BlockSpec(memory_space=pltpu.VMEM)
    smem = pl.BlockSpec(memory_space=pltpu.SMEM)
    return pl.pallas_call(
        attend_back_kernel,
        out_shape=jax.ShapeDtypeStruct((count, 3 * half, LANES), low_type),
        in_specs=[smem, smem] + [vmem] * 5,
        out_specs=vmem,
        scratch_shapes=[
            pltpu.VMEM((total, LANES), low_type),
            pltpu.VMEM((total, LANES), low_type),
            pltpu.VMEM((HEAD_DIM, total), low_type),
            pltpu.VMEM((total, LANES), jnp.float32),
            pltpu.VMEM((total, HEAD_DIM), jnp.float32),
            pltpu.VMEM((HEAD_DIM, TILE), jnp.float32),
        ],
        compiler_params=pltpu.CompilerParams(vmem_limit_bytes=VMEM_BYTES),
        cost_estimate=pl.CostEstimate(
            flops=total * total * LANES * 16, bytes_accessed=total * LANES * 16, transcendentals=0
        ),
        name="attend_back",
    )(meta, order, recv, qa, ka, va, sums)


PART_ORDERS = (("x", "z"), ("x", "z"), ("wa", "x", "z"), ("x", "wa", "z"))
GATHER_ORDERS = (("z", "x"), ("z", "x"), ("z", "x"), ("x", "z"))
PARTS = len(PART_ORDERS)
EARLY = sum(len(order) == 2 for order in PART_ORDERS)
STAGES = sum(len(order) for order in PART_ORDERS)
SIZES = {"wa": 2, "x": 2, "z": 4}


class Links:
    def __init__(self):
        me = lax.axis_index("ctx")
        self.at = {
            "core": lax.rem(me, 2),
            "x": lax.rem(me // 2, 2),
            "z": me // 4,
            "wa": lax.axis_index("wa"),
        }

    def peer(self, axis, value):
        at = dict(self.at)
        at[axis] = value
        return {"ctx": at["z"] * 4 + at["x"] * 2 + at["core"], "wa": at["wa"]}


def splits_rows(piece):
    return piece % 64 == 0


def grad_sum_kernel(*refs):
    refs = list(refs)
    sizes = (PARTS, PARTS, PARTS - EARLY, STAGES)
    g_refs, out_refs, core_bufs, bufs = (
        [refs.pop(0) for _ in range(number)] for number in sizes
    )
    core_bufs = [None] * EARLY + core_bufs
    send_sem, recv_sem = refs
    links = Links()
    core, x, z, wa = (links.at[name] for name in ("core", "x", "z", "wa"))
    barrier = pltpu.get_barrier_semaphore()
    peers = [links.peer("core", 1 - core), links.peer("x", 1 - x), links.peer("wa", 1 - wa)]
    peers += [links.peer("z", lax.rem(z + step, 4)) for step in range(1, 4)]
    for peer in peers:
        pl.semaphore_signal(barrier, inc=1, device_id=peer, device_id_type=pl.DeviceIdType.MESH)
    pl.semaphore_wait(barrier, len(peers))
    used = [0]

    def remote(src, dst, peer):
        index = used[0]
        used[0] += 1
        copy = pltpu.make_async_remote_copy(
            src_ref=src,
            dst_ref=dst,
            send_sem=send_sem.at[index],
            recv_sem=recv_sem.at[index],
            device_id=peer,
            device_id_type=pl.DeviceIdType.MESH,
        )
        copy.start()
        return copy

    def z_share(ref, value):
        piece, width = ref.shape[-2:]
        if value is None:
            return slice(None), slice(None)
        if splits_rows(piece):
            return pl.ds(pl.multiple_of(value * (piece // 4), 16), piece // 4), slice(None)
        return slice(None), pl.ds(pl.multiple_of(value * (width // 4), LANES), width // 4)

    def slab(part, held, axis=None, value=None):
        at = dict(links.at)
        if axis is not None:
            at[axis] = value
            held = held | {axis}
        return g_refs[part].at[
            pl.ds(0, 1) if part < EARLY else pl.ds(at["wa"], 1) if "wa" in held else pl.ds(0, 2),
            0 if part < EARLY else core,
            pl.ds(at["x"], 1) if "x" in held else pl.ds(0, 2),
            *z_share(g_refs[part], at["z"] if "z" in held else None),
        ]

    def add_into(target, sources):
        outer, inner, rows, _ = target.shape
        for a in range(outer):
            for b in range(inner):

                def add(group, _):
                    some = pl.ds(pl.multiple_of(group * 16, 16), 16)
                    total = target[a, b, some, :].astype(jnp.float32)
                    for source in sources:
                        total = total + source[a, b, some, :].astype(jnp.float32)
                    target[a, b, some, :] = total.astype(low_type)
                    return 0

                lax.fori_loop(0, rows // 16, add, 0)

    core_copies = [
        remote(g_refs[part].at[:, 1 - core], core_bufs[part], links.peer("core", 1 - core))
        if part >= EARLY
        else None
        for part in range(PARTS)
    ]
    first_buf = [sum(len(order) for order in PART_ORDERS[:part]) for part in range(PARTS)]

    def begin(part, stage):
        axis = PART_ORDERS[part][stage]
        held = set(PART_ORDERS[part][:stage])
        buf = bufs[first_buf[part] + stage]
        copies = []
        for step in range(1, SIZES[axis]):
            value = lax.rem(links.at[axis] + step, SIZES[axis])
            copies.append(
                remote(slab(part, held, axis, value), buf.at[step - 1], links.peer(axis, value))
            )
        return copies

    def out_slab(part, held):
        return out_refs[part].at[
            core,
            pl.ds(x, 1) if "x" in held else pl.ds(0, 2),
            *z_share(out_refs[part], z if "z" in held else None),
        ]

    def spread(part, stage):
        axis = GATHER_ORDERS[part][stage]
        block = out_slab(part, set(GATHER_ORDERS[part][stage:]))
        return [
            remote(block, block, links.peer(axis, lax.rem(links.at[axis] + step, SIZES[axis])))
            for step in range(1, SIZES[axis])
        ]

    def start_gather(part, stage):
        if stage < 2:
            return spread(part, stage)
        block = out_slab(part, set())
        return [remote(block, block, links.peer("core", 1 - core))]

    flying, passed = {}, {}
    for part in range(PARTS):
        passed[part] = 0 if part >= EARLY else 1
        flying[part] = begin(part, 0) if part < EARLY else [core_copies[part]]
    while any(flying.values()):
        for part in range(PARTS):
            if not flying[part]:
                continue
            order = PART_ORDERS[part]
            for copy in flying[part]:
                copy.wait()
            step = passed[part]
            passed[part] += 1
            if step == 0:
                add_into(slab(part, set()), [core_bufs[part]])
            elif step <= len(order):
                buf = bufs[first_buf[part] + step - 1]
                add_into(
                    slab(part, set(order[:step])),
                    [buf.at[at] for at in range(SIZES[order[step - 1]] - 1)],
                )
            if step < len(order):
                flying[part] = begin(part, step)
            elif step == len(order):
                out_slab(part, {"x", "z"})[...] = slab(part, {"wa", "x", "z"})[0]
                flying[part] = start_gather(part, 0)
            elif step <= len(order) + 2:
                flying[part] = start_gather(part, step - len(order))
            else:
                flying[part] = None


def grad_sum(grads, collective_id):
    bufs, core_bufs, outs, given = [], [], [], []
    for part, grad in enumerate(grads):
        rows, width = grad.shape
        early = part < EARLY
        piece = rows // 2 if early else rows // 8
        shape = {"wa": 1 if early else 2, "x": 2, "z": 4}
        for axis in PART_ORDERS[part]:
            shape[axis] //= SIZES[axis]
            share = (
                (piece * shape["z"] // 4, width)
                if splits_rows(piece)
                else (piece, width * shape["z"] // 4)
            )
            bufs.append(
                pltpu.VMEM((SIZES[axis] - 1, shape["wa"], shape["x"], *share), low_type)
            )
        if not early:
            core_bufs.append(pltpu.VMEM((2, 2, piece, width), low_type))
        outs.append(jax.ShapeDtypeStruct((2, 2, piece, width), low_type))
        lead = (1, 1) if early else (2, 2)
        given.append(grad.reshape(*lead, 2, piece, width))
    vmem = pl.BlockSpec(memory_space=pltpu.VMEM)
    size = sum(grad.size for grad in grads)
    sums = pl.pallas_call(
        grad_sum_kernel,
        out_shape=tuple(outs),
        in_specs=[vmem] * PARTS,
        out_specs=(vmem,) * PARTS,
        scratch_shapes=[
            *core_bufs,
            *bufs,
            pltpu.SemaphoreType.DMA((16 * PARTS,)),
            pltpu.SemaphoreType.DMA((16 * PARTS,)),
        ],
        compiler_params=pltpu.CompilerParams(
            collective_id=collective_id, has_side_effects=True, vmem_limit_bytes=VMEM_BYTES
        ),
        cost_estimate=pl.CostEstimate(
            flops=size * 20_000, bytes_accessed=size * 4, transcendentals=0
        ),
        name="grad_sum",
    )(*given)
    return [part.reshape(-1, part.shape[-1]) for part in sums]


def reduce_shards(grad):
    part = lax.psum_scatter(
        grad.astype(low_type), ("wa", "ctx"), scatter_dimension=0, tiled=True
    )
    return lax.all_gather(part, "ctx", axis=0, tiled=True)


def body(
    count,
    tokens,
    cotangent,
    lengths,
    block_order,
    w_query,
    b_query,
    w_key,
    w_value,
    b_value,
    w_out,
    b_out,
    gain_one,
    shift_one,
    w_up,
    b_up,
    w_down,
    b_down,
    gain_two,
    shift_two,
):
    inputs = tokens[0]
    tok_rows, width = inputs.shape
    wide = w_up.shape[1]
    half = tok_rows // 2
    shard = w_query.shape[0]
    direct = count == 16 and width == 2 * shard and shard % 64 == 0 and wide == 4 * width
    me = lax.axis_index("ctx")
    seq_ends = jnp.cumsum(lengths[0])
    own_blocks = lax.dynamic_slice(block_order, (2 * me,), (2,))
    position = (own_blocks[:, None] * half + jnp.arange(half, dtype=jnp.int32)[None, :]).reshape(-1)
    own_seg = segment_of(position, seq_ends)
    owns = jnp.any(me == jnp.arange(HEADS, dtype=jnp.int32) * count // HEADS).astype(jnp.int32)
    meta = jnp.concatenate([seq_ends.astype(jnp.int32), owns[None]])

    core = me % 2
    wa = lax.axis_index("wa")

    def fetch_half(shard_block, after=None):
        if not direct:
            return None
        if after is not None:
            shard_block, _ = lax.optimization_barrier((shard_block, after))
        size, columns = shard_block.shape
        part = lax.dynamic_slice(shard_block, (core * (size // 2), 0), (size // 2, columns))
        return lax.ppermute(part, "wa", [(0, 1), (1, 0)])

    def gather_rows(shard_block, fetched):
        if not direct:
            return lax.all_gather(shard_block, "wa", axis=0, tiled=True)
        size, columns = shard_block.shape
        swapped = lax.ppermute(fetched, "ctx", [(k, k ^ 1) for k in range(count)])
        other = (1 - wa) * size
        whole = jnp.zeros((2 * size, columns), shard_block.dtype)
        whole = lax.dynamic_update_slice(whole, shard_block, (wa * size, 0))
        whole = lax.dynamic_update_slice(whole, fetched, (other + core * (size // 2), 0))
        return lax.dynamic_update_slice(whole, swapped, (other + (1 - core) * (size // 2), 0))

    pair = jnp.stack(
        [
            w_key.astype(low_type).reshape(shard, HEADS, HEAD_DIM),
            w_value.astype(low_type).reshape(shard, HEADS, HEAD_DIM),
        ],
        axis=2,
    ).reshape(shard, 2 * width)
    own_vectors = jnp.concatenate(
        [
            jnp.stack(
                [b_query, b_value, b_out, gain_one, shift_one, gain_two, shift_two, b_down]
            ),
            b_up.reshape(4, shard),
            jnp.zeros((4, shard), jnp.float32),
        ],
        axis=0,
    ).astype(low_type)
    if direct:
        other_vectors = lax.ppermute(own_vectors, "wa", [(0, 1), (1, 0)])
        vector_rows = jnp.where(
            wa == 0,
            jnp.concatenate([own_vectors, other_vectors], axis=1),
            jnp.concatenate([other_vectors, own_vectors], axis=1),
        ).astype(jnp.float32)
    else:
        vector_rows = (
            lax.all_gather(own_vectors, "wa", axis=1, tiled=True)
        ).astype(jnp.float32)

    first_shard = jnp.concatenate([w_query.astype(low_type), pair], axis=1)
    fetched = fetch_half(first_shard)
    later_shards = (
        w_out.astype(low_type),
        w_up.astype(low_type),
        w_down.astype(low_type),
    )
    later_fetched = tuple(fetch_half(block, fetched) for block in later_shards)
    first_pack = gather_rows(first_shard, fetched)
    query_weight = first_pack[:, :width]
    pair_weight = first_pack[:, width : 3 * width]
    out_bias, gain_first, shift_first, gain_second, shift_second, down_bias = (
        vector_rows[index] for index in range(2, 8)
    )
    up_bias = (
        vector_rows[8:12].reshape(4, width // shard, shard).transpose(1, 0, 2).reshape(-1)
    )

    packed = project(inputs, first_pack, vector_rows)
    at_head = to_heads(packed, count, 0)
    context_out, qa, ka, va, sums = attend(meta, block_order, at_head)
    context_out, later_fetched = lax.optimization_barrier((context_out, later_fetched))
    out_weight, up_weight, down_weight = (
        gather_rows(block, half_block) for block, half_block in zip(later_shards, later_fetched)
    )
    context_in = to_rows(context_out, count, 1)
    context_low = (
        context_in.reshape(HEADS, half, 2, HEAD_DIM).transpose(2, 1, 0, 3).reshape(tok_rows, width)
    )

    attn_out = jnp.dot(context_low, out_weight, preferred_element_type=jnp.float32) + out_bias
    h_one = inputs.astype(jnp.float32) + attn_out
    norm_one, norm_one_back = jax.vjp(layer_norm, h_one, gain_first, shift_first)
    norm_low = norm_one.astype(low_type)
    up_pre = jnp.dot(norm_low, up_weight, preferred_element_type=jnp.float32) + up_bias
    gelu_out, gelu_back = jax.vjp(partial(jax.nn.gelu, approximate=False), up_pre)
    gelu_low = gelu_out.astype(low_type)
    down_out = jnp.dot(gelu_low, down_weight, preferred_element_type=jnp.float32) + down_bias
    h_two = norm_one + down_out
    result, norm_two_back = jax.vjp(layer_norm, h_two, gain_second, shift_second)
    activations = result.astype(low_type)[None]
    valid = (own_seg < 3).astype(jnp.float32)
    g_out = cotangent[0].astype(jnp.float32) * valid[:, None]
    d_htwo, grad_gain_second, grad_shift_second = norm_two_back(g_out)
    d_down = d_htwo.astype(low_type)
    d_gelu = jnp.einsum("td,fd->tf", d_down, down_weight, preferred_element_type=jnp.float32)
    (d_uppre,) = gelu_back(d_gelu)
    d_up = d_uppre.astype(low_type)
    d_yone = d_htwo + jnp.einsum("tf,df->td", d_up, up_weight, preferred_element_type=jnp.float32)
    d_hone, grad_gain_first, grad_shift_first = norm_one_back(d_yone)
    d_attn = d_hone.astype(low_type)
    d_context = jnp.einsum("td,cd->tc", d_attn, out_weight, preferred_element_type=jnp.float32)
    context_back = (
        d_context.astype(low_type)
        .reshape(2, half, HEADS, HEAD_DIM)
        .transpose(2, 1, 0, 3)
        .reshape(HEADS, half, LANES)
    )

    grad_wdown = jnp.einsum("tf,td->fd", gelu_low, d_down, preferred_element_type=jnp.float32)
    grad_wup = jnp.einsum("td,tf->df", norm_low, d_up, preferred_element_type=jnp.float32)
    grad_wout = jnp.einsum("tc,td->cd", context_low, d_attn, preferred_element_type=jnp.float32)
    up_bias_sums = jnp.sum(d_up.astype(jnp.float32), axis=0)
    lanes = 2 * LANES
    vec_block = jnp.concatenate(
        [
            jnp.stack(
                [
                    jnp.sum(d_attn.astype(jnp.float32), axis=0),
                    grad_gain_first,
                    grad_shift_first,
                    jnp.sum(d_down.astype(jnp.float32), axis=0),
                    grad_gain_second,
                    grad_shift_second,
                ],
                axis=1,
            ),
            up_bias_sums.reshape(width // shard, 4, shard).transpose(0, 2, 1).reshape(width, 4),
        ],
        axis=1,
    ).astype(low_type)
    out_block = jnp.concatenate(
        [grad_wout.astype(low_type), jnp.pad(vec_block, ((0, 0), (0, lanes - 10)))], axis=1
    )
    up_block = grad_wup.astype(low_type)
    down_block = grad_wdown.astype(low_type)
    def add_low(mine, given):
        return (mine.astype(jnp.float32) + given.astype(jnp.float32)).astype(low_type)

    def core_halves(block):
        view = block.reshape(2, 2, -1, block.shape[1])
        keep = jnp.where(core == 0, view[:, 0], view[:, 1])
        give = jnp.where(core == 0, view[:, 1], view[:, 0])
        return keep, lax.ppermute(give, "ctx", [(k, k ^ 1) for k in range(count)])

    def wa_halves(block):
        keep = jnp.where(wa == 0, block[0], block[1])
        give = jnp.where(wa == 0, block[1], block[0])
        return keep, lax.ppermute(give, "wa", [(0, 1), (1, 0)])

    context_back, down_block, out_block, up_block = lax.optimization_barrier(
        (context_back, down_block, out_block, up_block)
    )
    if direct:
        halves = [core_halves(block) for block in (up_block, down_block)]
        back_at_head = to_heads(context_back, count, 2)
        back_at_head, halves = lax.optimization_barrier((back_at_head, halves))
        halves = [wa_halves(add_low(*pair)) for pair in halves]
        grads_out = attend_back(meta, block_order, back_at_head, qa, ka, va, sums)
        grads_out, halves = lax.optimization_barrier((grads_out, halves))
        early = [add_low(*pair) for pair in halves]
    else:
        back_at_head = to_heads(context_back, count, 2)
        grads_out = attend_back(meta, block_order, back_at_head, qa, ka, va, sums)
    grads_in = to_rows(grads_out, count, 3)

    d_all, d_pair, bias_sums = unpack(grads_in, width)
    d_queries = d_all[:, :width]
    grad_all = jnp.einsum("tc,td->cd", inputs, d_all, preferred_element_type=jnp.float32)
    last_block = lax.dynamic_update_slice(
        grad_all.astype(low_type), bias_sums, (0, 3 * width)
    )
    if direct:
        up_sum, down_sum, last_sum, out_sum = grad_sum((*early, last_block, out_block), 4)
    else:
        up_sum, down_sum, last_sum, out_sum = (
            reduce_shards(block) for block in (up_block, down_block, last_block, out_block)
        )
    d_input = (
        d_hone
        + jnp.einsum("td,cd->tc", d_queries, query_weight, preferred_element_type=jnp.float32)
        + jnp.einsum("td,cd->tc", d_pair, pair_weight, preferred_element_type=jnp.float32)
    )
    input_grad = d_input.astype(low_type)[None]

    wide_grad = last_sum.astype(jnp.float32)
    out_grad = out_sum.astype(jnp.float32)
    return (
        activations,
        input_grad,
        wide_grad[:, :width],
        wide_grad[:, 3 * width],
        wide_grad[:, width : 2 * width],
        wide_grad[:, 2 * width : 3 * width],
        wide_grad[:, 3 * width + 1],
        out_grad[:, :width],
        out_grad[:, width],
        out_grad[:, width + 1],
        out_grad[:, width + 2],
        up_sum.astype(jnp.float32),
        out_grad[:, width + 6 : width + 10].T.reshape(-1),
        down_sum.astype(jnp.float32),
        out_grad[:, width + 3],
        out_grad[:, width + 4],
        out_grad[:, width + 5],
    )


def solution(mesh):
    placed = (
        P("wa", "ctx", None),
        P("wa", "ctx", None),
        P("wa", None),
        P(),
        P("wa", None),
        P("wa"),
        P("wa", None),
        P("wa", None),
        P("wa"),
        P("wa", None),
        P("wa"),
        P("wa"),
        P("wa"),
        P("wa", None),
        P("wa"),
        P("wa", None),
        P("wa"),
        P("wa"),
        P("wa"),
    )
    return jax.shard_map(
        partial(body, mesh.shape["ctx"]),
        mesh=mesh,
        in_specs=placed,
        out_specs=(
            P("wa", "ctx", None),
            P("wa", "ctx", None),
            P("wa", None),
            P("wa"),
            P("wa", None),
            P("wa", None),
            P("wa"),
            P("wa", None),
            P("wa"),
            P("wa"),
            P("wa"),
            P("wa", None),
            P("wa"),
            P("wa", None),
            P("wa"),
            P("wa"),
            P("wa"),
        ),
        check_vma=False,
    )
```
